32 devices in a mesh: gx: 4 (over y, x), gy: 2 (over core), gz: 4 (over z).
Axes of the slice: x: 2, y: 2, z: 4, core: 2. Of those that a mesh axis runs over, the one named last changes fastest.
Arguments:
- right_side: float32 [81, 16, 16, 512], P(None, 'gx', 'gy', 'gz'), may hold values from -18 to 18
- cell_coef: float32 [16, 16, 128], P('gx', 'gy', 'gz'), may hold values from 0.5 to 2
- cell_matrix: float32 [81, 81], replicated, may hold values from -2 to 16, as said below
- face_coupling: float32 [3, 81, 81], replicated, may hold values from -0.18 to 0.18
- patch_inverse: bfloat16 [648, 648], replicated, may hold values from -0.01 to 0.1, as said below
Outputs:
- solution: float32 [81, 16, 16, 512], P(None, 'gx', 'gy', 'gz')
- residual: float32 [81, 16, 16, 512], P(None, 'gx', 'gy', 'gz')
The draws below stay inside these ranges and needn't reach their ends.
Inputs may be any that keep to these rules, and one draw needn't show every extreme that they name: `cell_matrix`: symmetric. `patch_inverse`: symmetric.
All inputs are finite; a program needn't handle non-finite values.
Results may differ from the reference program's by a relative error of at most 0.035.
Values may be sent and summed in bfloat16 or wider, within the bound.
No kernel may reach another device: no remote copies, remote signals or barrier semaphores. Data moves between devices by JAX's collectives and lax.ppermute only.
A program may use at most 192 MiB of HBM per device.

```python
import math
import jax
import jax.numpy as jnp
from jax import lax

Q = 81
PATCH = 648
RHS = 4
NX = 16
NY = 16
NZ = 128


def symmetric_part(key, matrix_order):
    sampled = jnp.clip(jax.random.normal(key, (matrix_order, matrix_order), jnp.float32), -4.0, 4.0)
    return (sampled + sampled.T) * 0.7071


def draw_cell_matrix(key, part):
    key_diag = jax.random.fold_in(key, 11)
    key_rest = jax.random.fold_in(key, 12)
    diagonal = jax.random.uniform(key_diag, (Q,), jnp.float32, 10.8, 13.2)
    return jnp.diag(diagonal) + 0.35 * symmetric_part(key_rest, Q)


def draw_patch_inverse(key, part):
    key_diag = jax.random.fold_in(key, 21)
    key_rest = jax.random.fold_in(key, 22)
    diagonal = jax.random.uniform(key_diag, (PATCH,), jnp.float32, 0.9, 1.1)
    values = (jnp.diag(diagonal) + 0.012 * symmetric_part(key_rest, PATCH)) / 12.0
    return values.astype(jnp.bfloat16)


def shard_levels(stream_key, extent, split, low, largest):
    gain, own = 1.0, jax.random.fold_in(stream_key, 6)
    for position, parts in split:
        draws = jnp.exp(jax.random.uniform(jax.random.fold_in(own, position), (parts,), jnp.float32, low / len(split), largest / len(split)))
        gain = gain * jnp.repeat(draws, extent[position] // parts).reshape([-1 if axis == position else 1 for axis in range(len(extent))])
    return gain


def normal_values(key, dims, scale, limit, cuts=(), dtype=jnp.bfloat16):
    values = scale * jax.random.normal(key, dims, jnp.float32)
    if cuts:
        values = values * shard_levels(key, dims, cuts, -0.22, 0.18)
    return jnp.clip(values, -limit, limit).astype(dtype)


def setup_inputs(seed: int = 0) -> dict:
    keys = jax.random.split(jax.random.key(seed), 6)
    return {
        "right_side": normal_values(keys[0], (Q, NX, NY, NZ * RHS), 3.0, 18.0, ((1, 4), (2, 2), (3, 4)), jnp.float32),
        "cell_coef": jnp.clip(jnp.exp(math.log(2.0) - 1.3862944 * jax.random.uniform(keys[1], (NX, NY, NZ), jnp.float32) ** shard_levels(keys[1], (NX, NY, NZ), ((0, 4), (1, 2), (2, 4)), -0.2, 0.2)), 0.5, 2.0),
        "cell_matrix": draw_cell_matrix(jax.random.fold_in(keys[5], 71), 0),
        "face_coupling": normal_values(keys[3], (3, Q, Q), 0.03, 0.18, (), jnp.float32),
        "patch_inverse": draw_patch_inverse(jax.random.fold_in(keys[5], 71), 0),
    }


HIGH = lax.Precision.HIGHEST

def operator(values, cell_coef, cell_matrix, face_coupling):
    result = cell_coef[None, :, :, :, None] * jnp.einsum('pq,qxyzr->pxyzr', cell_matrix, values, precision=HIGH)
    for direction in range(3):
        forward = jnp.roll(values, -1, direction + 1)
        behind = jnp.roll(values, 1, direction + 1)
        result = result - jnp.einsum('pq,qxyzr->pxyzr', face_coupling[direction], forward, precision=HIGH)
        result = result - jnp.einsum('qp,qxyzr->pxyzr', face_coupling[direction], behind, precision=HIGH)
    return result

def reference(right_side, cell_coef, cell_matrix, face_coupling, patch_inverse):
    dof_count = cell_matrix.shape[0]
    residual = right_side.reshape(dof_count, NX, NY, NZ, RHS)
    solution = jnp.zeros_like(residual)
    scaling = lax.rsqrt(cell_coef)[None, :, :, :, None]
    blocks = patch_inverse.astype(jnp.float32).reshape(dof_count, 2, 2, 2, dof_count, 2, 2, 2)
    for colour in range(8):
        shifts = (1 - colour // 4, 1 - colour // 2 % 2, 1 - colour % 2)
        scaled = (scaling * residual).astype(jnp.bfloat16)
        scaled = lax.optimization_barrier(scaled).astype(jnp.float32)
        rolled = jnp.roll(scaled, shifts, axis=(1, 2, 3))
        blocked = rolled.reshape(dof_count, NX // 2, 2, NY // 2, 2, NZ // 2, 2, RHS)
        solved = jnp.einsum('qijkplmn,pXlYmZnr->qXiYjZkr', blocks, blocked, precision=HIGH)
        solved = solved.reshape(dof_count, NX, NY, NZ, RHS)
        solved = jnp.roll(solved, (-shifts[0], -shifts[1], -shifts[2]), axis=(1, 2, 3))
        correction = scaling * solved
        solution = solution + correction
        residual = residual - operator(correction, cell_coef, cell_matrix, face_coupling)
    return (solution.reshape(right_side.shape), residual.reshape(right_side.shape))
```

```python
import jax
import jax.numpy as jnp
from jax import lax
from jax.experimental import pallas as pl
from jax.experimental.pallas import tpu as pltpu
from jax.sharding import PartitionSpec as P

F32 = jnp.float32
BF16 = jnp.bfloat16
LANES = 128
VMEM_LIMIT = 28 * 1024 * 1024


class Block:
    def __init__(self, dofs, extent_x, extent_y, extent_z, rhs):
        assert extent_x % 2 == 0 and extent_y % 4 == 0 and extent_z * rhs == LANES
        self.q, self.ex, self.ey, self.ez, self.rhs = dofs, extent_x, extent_y, extent_z, rhs
        self.rows = -(-(dofs + 2) // 16) * 16
        self.nx, self.ny = extent_x // 2, extent_y // 2
        self.tiles = extent_x * extent_y * 2
        self.own = LANES // 4
        self.half = LANES // 2
        self.faces_x = 2 * extent_y
        self.faces_y = 2 * extent_x

    def tile(self, x, y, pz):
        px, py = x % 2, y % 2
        sx, sy = (x // 2) % self.nx, (y // 2) % self.ny
        return (((px * 2 + py) * 2 + pz) * self.nx + sx) * self.ny + sy

    def span(self, parity, extent):
        return range(parity - 1, parity - 1 + extent)

    def face_x(self, x, b):
        return [self.tile(x, y, pz) for y in self.span(b, self.ey) for pz in range(2)]

    def face_y(self, y, a):
        return [self.tile(x, y, pz) for x in self.span(a, self.ex) for pz in range(2)]


def lane_iota(rows):
    return lax.broadcasted_iota(jnp.int32, (rows, LANES), 1)


def roll(v, by):
    by = by % LANES
    return pltpu.roll(v, by, 1) if by else v


def dot(a, b):
    return jnp.dot(a, b, preferred_element_type=F32)


def call(body, ins, outs, aliases=None, scratch=(), flops=0, hbm_out=False):
    space = pl.BlockSpec(memory_space=pltpu.VMEM)
    if hbm_out:
        shapes = [jax.ShapeDtypeStruct(s, d) for s, d in outs]
    else:
        shapes = [pltpu.VMEM(s, d) for s, d in outs]
    return pl.pallas_call(
        body,
        in_specs=[space] * len(ins),
        out_specs=[space] * len(outs),
        out_shape=shapes,
        scratch_shapes=[pltpu.VMEM(s, d) for s, d in scratch],
        input_output_aliases=aliases or {},
        compiler_params=pltpu.CompilerParams(vmem_limit_bytes=VMEM_LIMIT),
        cost_estimate=pl.CostEstimate(flops=flops, bytes_accessed=0, transcendentals=0) if flops else None,
    )(*ins)


def coef_row(bk, r_ref, t):
    return r_ref[t, bk.q : bk.q + 1, :] + r_ref[t, bk.q + 1 : bk.q + 2, :]


def shift(v, axis, distance):
    n = lax.axis_size(axis)
    return lax.ppermute(v, axis, [((i - distance) % n, i) for i in range(n)])


def shift2(v, first, d1, second, d2):
    n1, n2 = lax.axis_size(first), lax.axis_size(second)
    route = [
        (((i - d1) % n1) * n2 + (j - d2) % n2, i * n2 + j) for i in range(n1) for j in range(n2)
    ]
    return lax.ppermute(v, (first, second), route)


def pack(bk, r_ref, tiles, lanes_from, count, out_ref, parts):
    lane = lane_iota(bk.rows)
    for n in range(0, len(tiles), parts):
        total = None
        for k, t in enumerate(tiles[n : n + parts]):
            moved = roll(r_ref[t], k * count - lanes_from)
            total = moved if total is None else jnp.where(lane < k * count, total, moved)
        out_ref[n // parts] = total.astype(BF16)


def unpack(bk, msg_ref, n, lanes_to, count, parts):
    k = n % parts
    return roll(msg_ref[n // parts].astype(F32), lanes_to - k * count)


def prep_inverse(bk):
    def body(p_ref, o_ref):
        n = p_ref.shape[0]
        row = lax.broadcasted_iota(jnp.int32, (8 * bk.rows, n), 0)
        col = lax.broadcasted_iota(jnp.int32, (8 * bk.rows, n), 1)
        o, d = row // bk.rows, row % bk.rows
        pick = jnp.where((col == d * 8 + o) & (d < bk.q), 1.0, 0.0).astype(BF16)
        left = dot(pick, p_ref[...]).astype(BF16)
        o_ref[...] = lax.dot_general(
            left, pick, (((1,), (1,)), ((), ())), preferred_element_type=F32
        ).astype(BF16)

    return body


def prep_state(bk):
    def body(rs_ref, cc_ref, r_ref, y_ref, scr):
        rows = rs_ref.reshape(bk.q * bk.ex * bk.ey, LANES)
        src = lax.broadcasted_iota(jnp.int32, (2 * LANES, 2 * LANES), 0) % LANES
        dst = lax.broadcasted_iota(jnp.int32, (2 * LANES, 2 * LANES), 1)
        pz, lane = dst // LANES, dst % LANES - bk.own
        z = 2 * (lane // bk.rhs) + pz
        inside = (lane >= 0) & (lane < bk.half)
        split = jnp.where(inside & (src == z * bk.rhs + lane % bk.rhs), 1.0, 0.0).astype(BF16)
        zz = lax.broadcasted_iota(jnp.int32, (bk.ez, LANES), 0)
        ll = lax.broadcasted_iota(jnp.int32, (bk.ez, LANES), 1)
        spread = jnp.where(ll // bk.rhs == zz, 1.0, 0.0).astype(BF16)
        coef = cc_ref[...]
        high = coef.astype(BF16)
        low = (coef - high.astype(F32)).astype(BF16)
        high, low = dot(high, spread), dot(low, spread)
        scr[...] = jnp.zeros_like(scr)
        for x in range(bk.ex):
            for y in range(bk.ey):
                n = x * bk.ey + y
                scr[n % 4, : bk.q, :] = rows[pl.ds(n, bk.q, stride=bk.ex * bk.ey), :]
                scr[n % 4, bk.q : bk.q + 1, :] = high[n : n + 1]
                scr[n % 4, bk.q + 1 : bk.q + 2, :] = low[n : n + 1]
                raw = scr[n % 4]
                top = raw.astype(BF16)
                rest = (raw - top.astype(F32)).astype(BF16)
                out = dot(jnp.concatenate([top, rest], axis=1), split)
                r_ref[bk.tile(x, y, 0)] = out[:, :LANES]
                r_ref[bk.tile(x, y, 1)] = out[:, LANES:]
        tiles = [bk.tile(x, bk.ey - 1, pz) for x in range(bk.ex) for pz in range(2)]
        pack(bk, r_ref, tiles, bk.own, bk.half, y_ref, 2)

    return body


def halo_cells(bk):
    return [
        bk.tile(x, y, pz)
        for x in range(bk.ex - 1)
        for y in bk.span(0, bk.ey)
        for pz in range(2)
    ]


def prep_halo(bk):
    def body(r_in, y_ref, r_ref, zl_ref, zh_ref, x_ref, xl_ref, xh_ref):
        n = 0
        for x in range(bk.ex):
            for pz in range(2):
                r_ref[bk.tile(x, -1, pz)] = unpack(bk, y_ref, n, bk.own, bk.half, 2)
                n += 1
        cells = halo_cells(bk)
        pack(bk, r_ref, cells, bk.own, bk.own, zl_ref, 4)
        pack(bk, r_ref, cells, 2 * bk.own, bk.own, zh_ref, 4)
        edge = bk.face_x(bk.ex - 1, 0)
        pack(bk, r_ref, edge, bk.own, bk.half, x_ref, 2)
        pack(bk, r_ref, edge, bk.own, bk.own, xl_ref, 4)
        pack(bk, r_ref, edge, 2 * bk.own, bk.own, xh_ref, 4)

    return body


def fill_halo(bk, r_ref, zl_ref, zh_ref, x_ref, xl_ref, xh_ref):
    lane = lane_iota(bk.rows)
    below, above = lane < bk.own, lane >= 3 * bk.own

    def joined(own, low_ref, high_ref, n):
        low = unpack(bk, low_ref, n, 0, bk.own, 4)
        high = unpack(bk, high_ref, n, 3 * bk.own, bk.own, 4)
        return jnp.where(below, low, jnp.where(above, high, own))

    for n, t in enumerate(halo_cells(bk)):
        r_ref[t] = joined(r_ref[t], zl_ref, zh_ref, n)
    for n, t in enumerate(bk.face_x(-1, 0)):
        r_ref[t] = joined(unpack(bk, x_ref, n, bk.own, bk.half, 2), xl_ref, xh_ref, n)


def solve(bk, colour, r_ref, p_ref, c_ref, xl_ref, xh_ref, y_ref, xs_ref):
    a, b, g = colour
    back = bk.rhs
    n = 0
    for px in range(bk.nx):
        for py in range(0, bk.ny, 2):
            cells = []
            for half in range(2):
                for o in range(8):
                    x = a - 1 + 2 * px + o // 4
                    y = b - 1 + 2 * (py + half) + o // 2 % 2
                    pz = o % 2 if g else 1 - o % 2
                    t = bk.tile(x, y, pz)
                    scale = lax.rsqrt(coef_row(bk, r_ref, t))
                    scaled = r_ref[t] * scale
                    if g == 0 and pz == 1:
                        scaled = roll(scaled, back)
                    lanes = slice(half * LANES, (half + 1) * LANES)
                    xs_ref[n, o * bk.rows : (o + 1) * bk.rows, lanes] = scaled.astype(BF16)
                    cells.append((half, o, t, scale, g == 0 and pz == 1))
            solved = dot(p_ref[...], xs_ref[n])
            for half, o, t, scale, moved in cells:
                v = solved[o * bk.rows : (o + 1) * bk.rows, half * LANES : (half + 1) * LANES]
                if moved:
                    v = roll(v, -back)
                c_ref[t] = (v * scale).astype(BF16)
            n += 1
    for m, t in enumerate(bk.face_x(a - 1, b)):
        xl_ref[m] = c_ref[t]
    for m, t in enumerate(bk.face_x(a - 2 + bk.ex, b)):
        xh_ref[m] = c_ref[t]
    for m, t in enumerate(bk.face_y(b - 1, a) + bk.face_y(b - 2 + bk.ey, a)):
        y_ref[m] = c_ref[t]


def ghosts(bk, colour, r_ref, sol_ref, g_ref, from_below, from_above, y_ref):
    a, b, g = colour

    def add(matrix, tiles, ghost_ref, base):
        for m in range(0, len(tiles), 2):
            two = jnp.concatenate([ghost_ref[base + m], ghost_ref[base + m + 1]], axis=1)
            change = dot(g_ref[matrix], two)
            r_ref[tiles[m]] += change[:, :LANES]
            r_ref[tiles[m + 1]] += change[:, LANES:]

    add(0, bk.face_x(a - 2 + bk.ex, b), from_above, 0)
    add(1, bk.face_x(a - 1, b), from_below, 0)
    add(2, bk.face_y(b - 2 + bk.ey, a), y_ref, 0)
    add(3, bk.face_y(b - 1, a), y_ref, bk.faces_y)
    if a == 0:
        for m, t in enumerate(bk.face_x(bk.ex - 1, b)):
            sol_ref[t] += from_above[m].astype(F32)
    if b == 0:
        m = 0
        for x in bk.span(a, bk.ex):
            for pz in range(2):
                if x >= 0:
                    sol_ref[bk.tile(x, bk.ey - 1, pz)] += y_ref[m].astype(F32)
                m += 1


def own_change(bk, colour, first):
    a, b, g = colour

    def body(*refs):
        if first:
            r_in, c_ref, w_ref, r_ref, sol_ref, cm_ref, cz_ref = refs
        else:
            r_in, sol_in, c_ref, w_ref, r_ref, sol_ref, cm_ref, cz_ref = refs
        xs, ys = bk.span(a, bk.ex), bk.span(b, bk.ey)
        for x in xs:
            for y in ys:
                for pz in range(2):
                    t = bk.tile(x, y, pz)
                    c = c_ref[t].astype(F32)
                    cm_ref[t] = (c * coef_row(bk, r_ref, t)).astype(BF16)
                    cz_ref[t] = roll(c_ref[t], bk.rhs if pz else -bk.rhs)
                    if x >= 0 and y >= 0:
                        sol_ref[t] = c if first else sol_ref[t] + c
                    elif first:
                        sol_ref[t] = jnp.zeros_like(c)
        nothing = jnp.zeros((bk.rows, LANES), BF16)

        def at(x, y, pz):
            return c_ref[bk.tile(x, y, pz)] if x in xs and y in ys else nothing

        def stack(x, y, pz):
            other = bk.tile(x, y, 1 - pz)
            near, far = c_ref[other], cz_ref[other]
            return jnp.concatenate(
                [
                    cm_ref[bk.tile(x, y, pz)],
                    at(x + 1, y, pz),
                    at(x - 1, y, pz),
                    at(x, y + 1, pz),
                    at(x, y - 1, pz),
                    far if pz else near,
                    near if pz else far,
                ],
                axis=0,
            )

        for x in xs:
            for y in ys:
                both = jnp.concatenate([stack(x, y, 0), stack(x, y, 1)], axis=1)
                change = dot(w_ref[...], both)
                for pz in range(2):
                    r_ref[bk.tile(x, y, pz)] -= change[:, pz * LANES : (pz + 1) * LANES]

    return body


def leave(bk, ref):
    def body(tile_ref, out_ref):
        rows = out_ref.reshape(bk.q * bk.ex * bk.ey, LANES)
        src = lax.broadcasted_iota(jnp.int32, (2 * LANES, LANES), 0)
        dst = lax.broadcasted_iota(jnp.int32, (2 * LANES, LANES), 1)
        pz, lane = src // LANES, src % LANES - bk.own
        z = 2 * (lane // bk.rhs) + pz
        inside = (lane >= 0) & (lane < bk.half)
        join = jnp.where(inside & (dst == z * bk.rhs + lane % bk.rhs), 1.0, 0.0).astype(BF16)
        for x in range(bk.ex):
            for y in range(bk.ey):
                both = jnp.concatenate(
                    [tile_ref[bk.tile(x, y, 0)], tile_ref[bk.tile(x, y, 1)]], axis=1
                )
                top = both.astype(BF16)
                rest = (both - top.astype(F32)).astype(BF16)
                out = dot(top, join) + dot(rest, join)
                rows[pl.ds(x * bk.ey + y, bk.q, stride=bk.ex * bk.ey), :] = out[: bk.q]

    return body


def on_device(right_side, cell_coef, cell_matrix, face_coupling, patch_inverse):
    dofs = cell_matrix.shape[0]
    ex, ey, ez = cell_coef.shape
    bk = Block(dofs, ex, ey, ez, right_side.shape[3] // ez)
    rows, tiles = bk.rows, bk.tiles
    grown = [(0, rows - dofs), (0, rows - dofs)]
    square = (rows, LANES)

    state = ((tiles,) + square, F32)
    coarse = ((tiles,) + square, BF16)
    face_x, face_y = ((bk.faces_x,) + square, BF16), ((2 * bk.faces_y,) + square, BF16)

    def msg(n):
        return ((n,) + square, BF16)

    r, ymsg = call(
        prep_state(bk), [right_side, cell_coef.reshape(ex * ey, ez)], [state, msg(ex)],
        scratch=[((4,) + square, F32)],
    )
    ymsg = shift(ymsg, "gy", 1)
    edge = 2 * ey
    inner = len(halo_cells(bk))
    r, zl, zh, xm, xl, xh = call(
        prep_halo(bk), [r, ymsg],
        [state, msg(inner // 4), msg(inner // 4), msg(edge // 2), msg(edge // 4), msg(edge // 4)],
        aliases={0: 0},
    )
    halo = (
        shift(zh, "gz", 1),
        shift(zl, "gz", -1),
        shift(xm, "gx", 1),
        shift2(xh, "gx", 1, "gz", 1),
        shift2(xl, "gx", 1, "gz", -1),
    )
    (inverse,) = call(prep_inverse(bk), [patch_inverse], [((8 * rows, 8 * rows), BF16)])
    padded = jnp.pad(face_coupling, [(0, 0)] + grown)
    flipped = jnp.swapaxes(padded, 1, 2)
    pairs = [padded[0], flipped[0], padded[1], flipped[1], padded[2], flipped[2]]
    couple = jnp.stack(pairs[:4]).astype(BF16)
    weights = jnp.concatenate([jnp.pad(cell_matrix, grown)] + [-m for m in pairs], axis=1)
    weights = weights.astype(BF16)

    solve_scratch = [((bk.nx * bk.ny // 2, 8 * rows, 2 * LANES), BF16)]
    solve_outs = [coarse, face_x, face_x, face_y]
    flops = 1 << 27
    sol = None
    pending = None
    for colour in range(8):
        par = (colour // 4, colour // 2 % 2, colour % 2)
        if colour == 0:

            def body(r_in, zl, zh, xm, xl, xh, p, r_ref, c, fl, fh, fy, xs):
                fill_halo(bk, r_ref, zl, zh, xm, xl, xh)
                solve(bk, (0, 0, 0), r_ref, p, c, fl, fh, fy, xs)

            r, c, fl, fh, fy = call(
                body, [r, *halo, inverse], [state] + solve_outs,
                aliases={0: 0}, scratch=solve_scratch, flops=flops,
            )
        else:
            before = ((colour - 1) // 4, (colour - 1) // 2 % 2, (colour - 1) % 2)
            if par[1] == before[1]:

                def body(r_in, s_in, lo, hi, yy, gm, p, r_ref, s_ref, c, fl, fh, fy, xs, par=par, before=before):
                    ghosts(bk, before, r_ref, s_ref, gm, lo, hi, yy)
                    solve(bk, par, r_ref, p, c, fl, fh, fy, xs)

                r, sol, c, fl, fh, fy = call(
                    body, [r, sol, *pending, couple, inverse], [state, state] + solve_outs,
                    aliases={0: 0, 1: 1}, scratch=solve_scratch, flops=flops,
                )
            else:
                r, sol = move_region(bk, before, par, r, sol, pending, couple, msg, state)

                def body(r_in, p, r_ref, c, fl, fh, fy, xs, par=par):
                    solve(bk, par, r_ref, p, c, fl, fh, fy, xs)

                r, c, fl, fh, fy = call(
                    body, [r, inverse], [state] + solve_outs,
                    aliases={0: 0}, scratch=solve_scratch, flops=flops,
                )
        pending = exchange(fl, fh, fy, bk)
        if colour == 0:
            r, sol = call(
                own_change(bk, par, True), [r, c, weights], [state, state],
                aliases={0: 0}, scratch=[coarse, coarse], flops=flops,
            )
        else:
            r, sol = call(
                own_change(bk, par, False), [r, sol, c, weights], [state, state],
                aliases={0: 0, 1: 1}, scratch=[coarse, coarse], flops=flops,
            )
    whole = (right_side.shape, F32)
    (solution_out,) = call(leave(bk, None), [sol], [whole], hbm_out=True, flops=flops)

    def last(r_in, lo, hi, yy, gm, r_ref):
        ghosts(bk, (1, 1, 1), r_ref, None, gm, lo, hi, yy)

    (r,) = call(last, [r, *pending, couple], [state], aliases={0: 0})
    (residual_out,) = call(leave(bk, None), [r], [whole], hbm_out=True)
    return solution_out, residual_out


def exchange(fl, fh, fy, bk):
    below, above = shift(fh, "gx", 1), shift(fl, "gx", -1)
    if lax.axis_size("gy") == 2:
        ys = shift(fy, "gy", 1)
    else:
        n = bk.faces_y
        ys = jnp.concatenate([shift(fy[:n], "gy", -1), shift(fy[n:], "gy", 1)])
    return below, above, ys


def move_region(bk, before, par, r, sol, pending, couple, msg, state):
    to_home_y = before[1] == 0
    to_home_x = before[0] == 0 and par[0] == 1
    with_sol = before == (0, 0, 1)
    x_send = bk.face_x(-1, 1)
    x_home = bk.face_x(bk.ex - 1, 1)
    a = par[0]
    y_cells = bk.face_y(-1, a)
    sol_cells = [bk.tile(bk.ex - 1, bk.ey - 1, pz) for pz in range(2)]
    n_y = len(y_cells) + (2 if with_sol else 0)

    def finish(r_in, s_in, lo, hi, yy, gm, r_ref, s_ref, m_ref):
        ghosts(bk, before, r_ref, s_ref, gm, lo, hi, yy)
        if to_home_x:
            for m, t in enumerate(x_send):
                m_ref[m] = r_ref[t].astype(BF16)
        else:
            for m, t in enumerate(y_cells):
                m_ref[m] = r_ref[t].astype(BF16)
            if with_sol:
                for m, t in enumerate(sol_cells):
                    m_ref[len(y_cells) + m] = s_ref[t].astype(BF16)

    n_first = len(x_send) if to_home_x else n_y
    r, sol, m = call(
        finish, [r, sol, *pending, couple], [state, state, msg(n_first)], aliases={0: 0, 1: 1}
    )
    if to_home_x:
        m = shift(m, "gx", -1)

        def turn(r_in, m_in, r_ref, y_ref):
            for i, t in enumerate(x_home):
                r_ref[t] = m_in[i].astype(F32)
            for i, t in enumerate(y_cells):
                y_ref[i] = r_ref[t].astype(BF16)

        r, m = call(turn, [r, m], [state, msg(n_y)], aliases={0: 0})
    m = shift(m, "gy", -1 if to_home_y else 1)

    def place(r_in, s_in, m_in, r_ref, s_ref):
        for i, t in enumerate(y_cells):
            r_ref[t] = m_in[i].astype(F32)
        if with_sol:
            for i, t in enumerate(sol_cells):
                s_ref[t] = m_in[len(y_cells) + i].astype(F32)

    r, sol = call(place, [r, sol, m], [state, state], aliases={0: 0, 1: 1})
    return r, sol


def solution(mesh):
    placed = (P(None, "gx", "gy", "gz"), P("gx", "gy", "gz"), P(), P(), P())
    return jax.shard_map(
        on_device,
        mesh=mesh,
        in_specs=placed,
        out_specs=(P(None, "gx", "gy", "gz"), P(None, "gx", "gy", "gz")),
        check_vma=False,
    )
```

```python
import jax
import jax.numpy as jnp
from jax import lax
from jax.experimental import pallas as pl
from jax.experimental.pallas import tpu as pltpu
from jax.sharding import PartitionSpec as P

F32 = jnp.float32
BF16 = jnp.bfloat16
LANES = 128
VMEM_LIMIT = 28 * 1024 * 1024


class Block:
    def __init__(self, dofs, extent_x, extent_y, extent_z, rhs):
        assert extent_x % 2 == 0 and extent_y % 4 == 0 and extent_z * rhs == LANES
        self.q, self.ex, self.ey, self.ez, self.rhs = dofs, extent_x, extent_y, extent_z, rhs
        self.rows = -(-(dofs + 2) // 16) * 16
        self.nx, self.ny = extent_x // 2, extent_y // 2
        self.tiles = extent_x * extent_y * 2
        self.own = LANES // 4
        self.half = LANES // 2
        self.faces_x = 2 * extent_y
        self.faces_y = 2 * extent_x

    def tile(self, x, y, pz):
        px, py = x % 2, y % 2
        sx, sy = (x // 2) % self.nx, (y // 2) % self.ny
        return (((px * 2 + py) * 2 + pz) * self.nx + sx) * self.ny + sy

    def span(self, parity, extent):
        return range(parity - 1, parity - 1 + extent)

    def face_x(self, x, b):
        return [self.tile(x, y, pz) for y in self.span(b, self.ey) for pz in range(2)]

    def face_y(self, y, a):
        return [self.tile(x, y, pz) for x in self.span(a, self.ex) for pz in range(2)]


def lane_iota(rows):
    return lax.broadcasted_iota(jnp.int32, (rows, LANES), 1)


def roll(v, by):
    by = by % LANES
    return pltpu.roll(v, by, 1) if by else v


def dot(a, b):
    return jnp.dot(a, b, preferred_element_type=F32)


def call(body, ins, outs, aliases=None, scratch=(), flops=0, hbm_out=False, scalars=0):
    space = pl.BlockSpec(memory_space=pltpu.VMEM)
    table = pl.BlockSpec(memory_space=pltpu.SMEM)
    if hbm_out:
        shapes = [jax.ShapeDtypeStruct(s, d) for s, d in outs]
    else:
        shapes = [pltpu.VMEM(s, d) for s, d in outs]
    return pl.pallas_call(
        body,
        in_specs=[table] * scalars + [space] * (len(ins) - scalars),
        out_specs=[space] * len(outs),
        out_shape=shapes,
        scratch_shapes=[pltpu.VMEM(s, d) for s, d in scratch],
        input_output_aliases=aliases or {},
        compiler_params=pltpu.CompilerParams(vmem_limit_bytes=VMEM_LIMIT),
        cost_estimate=pl.CostEstimate(flops=flops, bytes_accessed=0, transcendentals=0) if flops else None,
    )(*ins)


def coef_row(bk, r_ref, t):
    return r_ref[t, bk.q : bk.q + 1, :] + r_ref[t, bk.q + 1 : bk.q + 2, :]


def shift(v, axis, distance):
    n = lax.axis_size(axis)
    return lax.ppermute(v, axis, [((i - distance) % n, i) for i in range(n)])


def shift2(v, first, d1, second, d2):
    n1, n2 = lax.axis_size(first), lax.axis_size(second)
    route = [
        (((i - d1) % n1) * n2 + (j - d2) % n2, i * n2 + j) for i in range(n1) for j in range(n2)
    ]
    return lax.ppermute(v, (first, second), route)


def pack(bk, r_ref, tiles, lanes_from, count, out_ref, parts):
    lane = lane_iota(bk.rows)
    for n in range(0, len(tiles), parts):
        total = None
        for k, t in enumerate(tiles[n : n + parts]):
            moved = roll(r_ref[t], k * count - lanes_from)
            total = moved if total is None else jnp.where(lane < k * count, total, moved)
        out_ref[n // parts] = total.astype(BF16)


def unpack(bk, msg_ref, n, lanes_to, count, parts):
    k = n % parts
    return roll(msg_ref[n // parts].astype(F32), lanes_to - k * count)


def prep_inverse(bk):
    def body(p_ref, o_ref):
        n = p_ref.shape[0]
        row = lax.broadcasted_iota(jnp.int32, (8 * bk.rows, n), 0)
        col = lax.broadcasted_iota(jnp.int32, (8 * bk.rows, n), 1)
        o, d = row // bk.rows, row % bk.rows
        pick = jnp.where((col == d * 8 + o) & (d < bk.q), 1.0, 0.0).astype(BF16)
        left = dot(pick, p_ref[...]).astype(BF16)
        o_ref[...] = lax.dot_general(
            left, pick, (((1,), (1,)), ((), ())), preferred_element_type=F32
        ).astype(BF16)

    return body


def prep_state(bk):
    def body(rs_ref, cc_ref, r_ref, y_ref, scr):
        rows = rs_ref.reshape(bk.q * bk.ex * bk.ey, LANES)
        src = lax.broadcasted_iota(jnp.int32, (2 * LANES, 2 * LANES), 0) % LANES
        dst = lax.broadcasted_iota(jnp.int32, (2 * LANES, 2 * LANES), 1)
        pz, lane = dst // LANES, dst % LANES - bk.own
        z = 2 * (lane // bk.rhs) + pz
        inside = (lane >= 0) & (lane < bk.half)
        split = jnp.where(inside & (src == z * bk.rhs + lane % bk.rhs), 1.0, 0.0).astype(BF16)
        zz = lax.broadcasted_iota(jnp.int32, (bk.ez, LANES), 0)
        ll = lax.broadcasted_iota(jnp.int32, (bk.ez, LANES), 1)
        spread = jnp.where(ll // bk.rhs == zz, 1.0, 0.0).astype(BF16)
        coef = cc_ref[...]
        high = coef.astype(BF16)
        low = (coef - high.astype(F32)).astype(BF16)
        high, low = dot(high, spread), dot(low, spread)
        scr[...] = jnp.zeros_like(scr)
        for x in range(bk.ex):
            for y in range(bk.ey):
                n = x * bk.ey + y
                scr[n % 4, : bk.q, :] = rows[pl.ds(n, bk.q, stride=bk.ex * bk.ey), :]
                scr[n % 4, bk.q : bk.q + 1, :] = high[n : n + 1]
                scr[n % 4, bk.q + 1 : bk.q + 2, :] = low[n : n + 1]
                raw = scr[n % 4]
                top = raw.astype(BF16)
                rest = (raw - top.astype(F32)).astype(BF16)
                out = dot(jnp.concatenate([top, rest], axis=1), split)
                r_ref[bk.tile(x, y, 0)] = out[:, :LANES]
                r_ref[bk.tile(x, y, 1)] = out[:, LANES:]
        tiles = [bk.tile(x, bk.ey - 1, pz) for x in range(bk.ex) for pz in range(2)]
        pack(bk, r_ref, tiles, bk.own, bk.half, y_ref, 2)

    return body


def halo_cells(bk):
    return [
        bk.tile(x, y, pz)
        for x in range(bk.ex - 1)
        for y in bk.span(0, bk.ey)
        for pz in range(2)
    ]


def prep_halo(bk):
    def body(r_in, y_ref, r_ref, zl_ref, zh_ref, x_ref, xl_ref, xh_ref):
        n = 0
        for x in range(bk.ex):
            for pz in range(2):
                r_ref[bk.tile(x, -1, pz)] = unpack(bk, y_ref, n, bk.own, bk.half, 2)
                n += 1
        cells = halo_cells(bk)
        pack(bk, r_ref, cells, bk.own, bk.own, zl_ref, 4)
        pack(bk, r_ref, cells, 2 * bk.own, bk.own, zh_ref, 4)
        edge = bk.face_x(bk.ex - 1, 0)
        pack(bk, r_ref, edge, bk.own, bk.half, x_ref, 2)
        pack(bk, r_ref, edge, bk.own, bk.own, xl_ref, 4)
        pack(bk, r_ref, edge, 2 * bk.own, bk.own, xh_ref, 4)

    return body


def fill_halo(bk, r_ref, zl_ref, zh_ref, x_ref, xl_ref, xh_ref):
    lane = lane_iota(bk.rows)
    below, above = lane < bk.own, lane >= 3 * bk.own

    def joined(own, low_ref, high_ref, n):
        low = unpack(bk, low_ref, n, 0, bk.own, 4)
        high = unpack(bk, high_ref, n, 3 * bk.own, bk.own, 4)
        return jnp.where(below, low, jnp.where(above, high, own))

    for n, t in enumerate(halo_cells(bk)):
        r_ref[t] = joined(r_ref[t], zl_ref, zh_ref, n)
    for n, t in enumerate(bk.face_x(-1, 0)):
        r_ref[t] = joined(unpack(bk, x_ref, n, bk.own, bk.half, 2), xl_ref, xh_ref, n)


def solve(bk, colour, r_ref, p_ref, c_ref, xl_ref, xh_ref, y_ref, xs_ref):
    a, b, g = colour
    back = bk.rhs
    n = 0
    for px in range(bk.nx):
        for py in range(0, bk.ny, 2):
            cells = []
            for half in range(2):
                for o in range(8):
                    x = a - 1 + 2 * px + o // 4
                    y = b - 1 + 2 * (py + half) + o // 2 % 2
                    pz = o % 2 if g else 1 - o % 2
                    t = bk.tile(x, y, pz)
                    scale = lax.rsqrt(coef_row(bk, r_ref, t))
                    scaled = r_ref[t] * scale
                    if g == 0 and pz == 1:
                        scaled = roll(scaled, back)
                    lanes = slice(half * LANES, (half + 1) * LANES)
                    xs_ref[n, o * bk.rows : (o + 1) * bk.rows, lanes] = scaled.astype(BF16)
                    cells.append((half, o, t, scale, g == 0 and pz == 1))
            solved = dot(p_ref[...], xs_ref[n])
            for half, o, t, scale, moved in cells:
                v = solved[o * bk.rows : (o + 1) * bk.rows, half * LANES : (half + 1) * LANES]
                if moved:
                    v = roll(v, -back)
                c_ref[t] = (v * scale).astype(BF16)
            n += 1
    for m, t in enumerate(bk.face_x(a - 1, b)):
        xl_ref[m] = c_ref[t]
    for m, t in enumerate(bk.face_x(a - 2 + bk.ex, b)):
        xh_ref[m] = c_ref[t]
    for m, t in enumerate(bk.face_y(b - 1, a) + bk.face_y(b - 2 + bk.ey, a)):
        y_ref[m] = c_ref[t]


def ghosts(bk, colour, r_ref, sol_ref, g_ref, from_below, from_above, y_ref):
    a, b, g = colour

    def add(matrix, tiles, ghost_ref, base):
        for m in range(0, len(tiles), 2):
            two = jnp.concatenate([ghost_ref[base + m], ghost_ref[base + m + 1]], axis=1)
            change = dot(g_ref[matrix], two)
            r_ref[tiles[m]] += change[:, :LANES]
            r_ref[tiles[m + 1]] += change[:, LANES:]

    add(0, bk.face_x(a - 2 + bk.ex, b), from_above, 0)
    add(1, bk.face_x(a - 1, b), from_below, 0)
    add(2, bk.face_y(b - 2 + bk.ey, a), y_ref, 0)
    add(3, bk.face_y(b - 1, a), y_ref, bk.faces_y)
    if a == 0:
        for m, t in enumerate(bk.face_x(bk.ex - 1, b)):
            sol_ref[t] += from_above[m].astype(F32)
    if b == 0:
        m = 0
        for x in bk.span(a, bk.ex):
            for pz in range(2):
                if x >= 0:
                    sol_ref[bk.tile(x, bk.ey - 1, pz)] += y_ref[m].astype(F32)
                m += 1


def own_change(bk, colour, first):
    a, b, g = colour

    def body(*refs):
        if first:
            r_in, c_ref, w_ref, r_ref, sol_ref, cm_ref, cz_ref = refs
        else:
            r_in, sol_in, c_ref, w_ref, r_ref, sol_ref, cm_ref, cz_ref = refs
        xs, ys = bk.span(a, bk.ex), bk.span(b, bk.ey)
        for x in xs:
            for y in ys:
                for pz in range(2):
                    t = bk.tile(x, y, pz)
                    c = c_ref[t].astype(F32)
                    cm_ref[t] = (c * coef_row(bk, r_ref, t)).astype(BF16)
                    cz_ref[t] = roll(c_ref[t], bk.rhs if pz else -bk.rhs)
                    if x >= 0 and y >= 0:
                        sol_ref[t] = c if first else sol_ref[t] + c
                    elif first:
                        sol_ref[t] = jnp.zeros_like(c)
        nothing = jnp.zeros((bk.rows, LANES), BF16)

        def at(x, y, pz):
            return c_ref[bk.tile(x, y, pz)] if x in xs and y in ys else nothing

        def stack(x, y, pz):
            other = bk.tile(x, y, 1 - pz)
            near, far = c_ref[other], cz_ref[other]
            return jnp.concatenate(
                [
                    cm_ref[bk.tile(x, y, pz)],
                    at(x + 1, y, pz),
                    at(x - 1, y, pz),
                    at(x, y + 1, pz),
                    at(x, y - 1, pz),
                    far if pz else near,
                    near if pz else far,
                ],
                axis=0,
            )

        for x in xs:
            for y in ys:
                both = jnp.concatenate([stack(x, y, 0), stack(x, y, 1)], axis=1)
                change = dot(w_ref[...], both)
                for pz in range(2):
                    r_ref[bk.tile(x, y, pz)] -= change[:, pz * LANES : (pz + 1) * LANES]

    return body


def leave(bk, ref):
    def body(tile_ref, out_ref):
        rows = out_ref.reshape(bk.q * bk.ex * bk.ey, LANES)
        src = lax.broadcasted_iota(jnp.int32, (2 * LANES, LANES), 0)
        dst = lax.broadcasted_iota(jnp.int32, (2 * LANES, LANES), 1)
        pz, lane = src // LANES, src % LANES - bk.own
        z = 2 * (lane // bk.rhs) + pz
        inside = (lane >= 0) & (lane < bk.half)
        join = jnp.where(inside & (dst == z * bk.rhs + lane % bk.rhs), 1.0, 0.0).astype(BF16)
        for x in range(bk.ex):
            for y in range(bk.ey):
                both = jnp.concatenate(
                    [tile_ref[bk.tile(x, y, 0)], tile_ref[bk.tile(x, y, 1)]], axis=1
                )
                top = both.astype(BF16)
                rest = (both - top.astype(F32)).astype(BF16)
                out = dot(top, join) + dot(rest, join)
                rows[pl.ds(x * bk.ey + y, bk.q, stride=bk.ex * bk.ey), :] = out[: bk.q]

    return body


class Slab:
    def __init__(self, bk, count):
        self.bk, self.count = bk, count
        self.q, self.rhs, self.rows, self.ny = bk.q, bk.rhs, bk.rows, bk.ny
        self.ey = bk.ey
        self.groups = count
        self.width = LANES // count
        self.depth = bk.ez // count
        self.halo = 2 * bk.rhs
        self.tiles = bk.tiles

    @staticmethod
    def fits(bk, count):
        depth = bk.ez // count
        return (
            bk.ez % count == 0
            and depth % 2 == 0
            and bk.nx == 2
            and (depth // 2 + 4) * bk.rhs * count == LANES
            and bk.tiles % 16 == 0
        )

    def tile(self, px, x2, y, pz):
        return (((px * 2 + y % 2) * 2 + pz) * 2 + x2) * self.ny + (y // 2) % self.ny

    def face_y(self, y):
        return [self.tile(px, x2, y, pz) for px in range(2) for x2 in range(2) for pz in range(2)]

    def order(self):
        return [0, 1, 3, 2] if self.count == 4 else list(range(self.count))


def home_prep(bk):
    def body(rs_ref, cc_ref, h_ref, up_ref, down_ref, scr):
        rows = rs_ref.reshape(bk.q * bk.ex * bk.ey, LANES)
        src = lax.broadcasted_iota(jnp.int32, (LANES, 2 * LANES), 0)
        dst = lax.broadcasted_iota(jnp.int32, (LANES, 2 * LANES), 1)
        pz, lane = dst // LANES, dst % LANES - bk.own
        z = 2 * (lane // bk.rhs) + pz
        inside = (lane >= 0) & (lane < bk.half)
        split = jnp.where(inside & (src == z * bk.rhs + lane % bk.rhs), 1.0, 0.0).astype(BF16)
        zz = lax.broadcasted_iota(jnp.int32, (bk.ez, LANES), 0)
        ll = lax.broadcasted_iota(jnp.int32, (bk.ez, LANES), 1)
        spread = jnp.where(ll // bk.rhs == zz, 1.0, 0.0).astype(BF16)
        coef = cc_ref[...]
        high = coef.astype(BF16)
        low = (coef - high.astype(F32)).astype(BF16)
        high, low = dot(high, spread), dot(low, spread)
        scr[...] = jnp.zeros_like(scr)
        for x in range(bk.ex):
            for y in range(bk.ey):
                n = x * bk.ey + y
                scr[n % 4, : bk.q, :] = rows[pl.ds(n, bk.q, stride=bk.ex * bk.ey), :]
                scr[n % 4, bk.q : bk.q + 1, :] = high[n : n + 1]
                scr[n % 4, bk.q + 1 : bk.q + 2, :] = low[n : n + 1]
                out = dot(scr[n % 4].astype(BF16), split)
                h_ref[bk.tile(x, y, 0)] = out[:, :LANES].astype(BF16)
                h_ref[bk.tile(x, y, 1)] = out[:, LANES:].astype(BF16)
        width = 2 * bk.rhs
        pack(bk, h_ref, list(range(bk.tiles)), bk.own + bk.half - width, width, up_ref, LANES // width)
        pack(bk, h_ref, list(range(bk.tiles)), bk.own, width, down_ref, LANES // width)

    return body


def scatter(sb):
    bk, parts = sb.bk, sb.groups
    width = 2 * bk.rhs
    per = LANES // width

    def body(me_ref, h_ref, below_ref, above_ref, *outs):
        lane = lane_iota(sb.rows)
        low = (lane >= bk.own - width) & (lane < bk.own)
        high = (lane >= bk.own + bk.half) & (lane < bk.own + bk.half + width)
        me = me_ref[0]
        for n in range(0, sb.tiles, parts):
            filled = []
            for t in range(n, n + parts):
                k = t % per
                from_low = roll(below_ref[t // per].astype(F32), bk.own - width - k * width)
                from_high = roll(above_ref[t // per].astype(F32), bk.own + bk.half - k * width)
                v = jnp.where(low, from_low, h_ref[t].astype(F32))
                filled.append(jnp.where(high, from_high, v))
            for d, out in enumerate(outs):
                start = me_ref[1 + d]
                total = filled[0]
                for k, v in enumerate(filled):
                    place = (me + k) % parts
                    by = (place * sb.width - start + LANES) % LANES
                    moved = pltpu.roll(v, by, 1)
                    total = moved if k == 0 else jnp.where(lane // sb.width == place, moved, total)
                out[n // parts] = total.astype(BF16)

    return body


def gather_state(sb, me_ref, parts_refs, r_ref):
    lane = lane_iota(sb.rows) // sb.width
    parts = sb.groups
    me = me_ref[0]
    for t in range(sb.tiles):
        k = t % parts
        total = parts_refs[0][t // parts].astype(F32)
        for d in range(1, parts):
            source = (me - d + parts) % parts
            total = jnp.where(lane == (source + k) % parts, parts_refs[d][t // parts].astype(F32), total)
        r_ref[t] = roll(total, -k * sb.width)


def slab_solve(sb, colour, r_ref, p_ref, c_ref, y_ref, xs_ref):
    a, b, g = colour
    rows = sb.rows
    n = 0
    for x2 in range(2):
        for py in range(0, sb.ny, 2):
            cells = []
            for half in range(2):
                for o in range(8):
                    xo, y = o // 4, b - 1 + 2 * (py + half) + o // 2 % 2
                    pz = o % 2 if g else 1 - o % 2
                    moved = sb.rhs if g == 0 and pz == 1 else 0
                    if a or xo == 1:
                        t = sb.tile(xo if a else 0, x2, y, pz)
                    else:
                        t = sb.tile(1, 1 - x2, y, pz)
                        moved += 0 if x2 else sb.width
                    scale = lax.rsqrt(coef_row(sb, r_ref, t))
                    lanes = slice(half * LANES, (half + 1) * LANES)
                    xs_ref[n, o * rows : (o + 1) * rows, lanes] = roll(
                        r_ref[t] * scale, moved
                    ).astype(BF16)
                    cells.append((half, o, t, scale, moved))
            solved = dot(p_ref[...], xs_ref[n])
            for half, o, t, scale, moved in cells:
                v = solved[o * rows : (o + 1) * rows, half * LANES : (half + 1) * LANES]
                c_ref[t] = (roll(v, -moved) * scale).astype(BF16)
            n += 1
    for m, t in enumerate(sb.face_y(b - 1) + sb.face_y(b - 2 + sb.ey)):
        y_ref[m] = c_ref[t]


def slab_ghosts(sb, colour, r_ref, sol_ref, g_ref, y_ref):
    a, b, g = colour
    count = len(sb.face_y(0))
    for matrix, y, base in ((0, b - 2 + sb.ey, 0), (1, b - 1, count)):
        tiles = sb.face_y(y)
        for m in range(0, count, 2):
            two = jnp.concatenate([y_ref[base + m], y_ref[base + m + 1]], axis=1)
            change = dot(g_ref[matrix], two)
            r_ref[tiles[m]] += change[:, :LANES]
            r_ref[tiles[m + 1]] += change[:, LANES:]
    if b == 0:
        for m, t in enumerate(sb.face_y(sb.ey - 1)):
            sol_ref[t] += y_ref[m].astype(F32)


def slab_change(sb, colour, first):
    a, b, g = colour

    def body(*refs):
        if first:
            r_in, c_ref, w_ref, r_ref, sol_ref, cm_ref, cz_ref, cx_ref = refs
        else:
            r_in, sol_in, c_ref, w_ref, r_ref, sol_ref, cm_ref, cz_ref, cx_ref = refs
        ys = sb.bk.span(b, sb.ey)
        cells = [(px, x2, y) for px in range(2) for x2 in range(2) for y in ys]
        for px, x2, y in cells:
            for pz in range(2):
                t = sb.tile(px, x2, y, pz)
                c = c_ref[t].astype(F32)
                cm_ref[t] = (c * coef_row(sb, r_ref, t)).astype(BF16)
                cz_ref[t] = roll(c_ref[t], sb.rhs if pz else -sb.rhs)
                if px == x2:
                    cx_ref[t] = roll(c_ref[t], sb.width if px else -sb.width)
                if y >= 0:
                    sol_ref[t] = c if first else sol_ref[t] + c
                elif first:
                    sol_ref[t] = jnp.zeros_like(c)
        nothing = jnp.zeros((sb.rows, LANES), BF16)

        def stack(px, x2, y, pz):
            beside = c_ref[sb.tile(1 - px, x2, y, pz)]
            across = (cx_ref if px == x2 else c_ref)[sb.tile(1 - px, 1 - x2, y, pz)]
            other = sb.tile(px, x2, y, 1 - pz)
            near, far = c_ref[other], cz_ref[other]
            return jnp.concatenate(
                [
                    cm_ref[sb.tile(px, x2, y, pz)],
                    across if px else beside,
                    beside if px else across,
                    c_ref[sb.tile(px, x2, y + 1, pz)] if y + 1 in ys else nothing,
                    c_ref[sb.tile(px, x2, y - 1, pz)] if y - 1 in ys else nothing,
                    far if pz else near,
                    near if pz else far,
                ],
                axis=0,
            )

        for px, x2, y in cells:
            both = jnp.concatenate([stack(px, x2, y, 0), stack(px, x2, y, 1)], axis=1)
            change = dot(w_ref[...], both)
            for pz in range(2):
                r_ref[sb.tile(px, x2, y, pz)] -= change[:, pz * LANES : (pz + 1) * LANES]

    return body


def emit_halo(sb, r_ref, up_ref, down_ref):
    lane = lane_iota(sb.rows) % sb.width
    top = sb.width - 2 * sb.halo
    parts = sb.width // sb.halo
    for ref, start in ((up_ref, top), (down_ref, sb.halo)):
        for n in range(0, sb.tiles, parts):
            total = None
            for k in range(parts):
                moved = roll(r_ref[n + k], k * sb.halo - start)
                total = moved if k == 0 else jnp.where(lane < k * sb.halo, total, moved)
            ref[n // parts] = total.astype(BF16)


def fill_slab_halo(sb, r_ref, below_ref, above_ref):
    lane = lane_iota(sb.rows) % sb.width
    parts = sb.width // sb.halo
    for t in range(sb.tiles):
        k = t % parts
        low = roll(below_ref[t // parts].astype(F32), -k * sb.halo)
        high = roll(above_ref[t // parts].astype(F32), sb.width - sb.halo - k * sb.halo)
        own = jnp.where(lane < sb.halo, low, r_ref[t])
        r_ref[t] = jnp.where(lane >= sb.width - sb.halo, high, own)


def collect(sb):
    width = sb.width - 2 * sb.halo
    parts = LANES // width

    def body(me_ref, r_ref, s_ref, *outs):
        lane = lane_iota(sb.rows) // width
        slab = me_ref[0]
        for source, base in ((s_ref, 0), (r_ref, sb.tiles // parts)):
            for n in range(0, sb.tiles, parts):
                for d, out in enumerate(outs):
                    start = me_ref[1 + d]
                    total = None
                    for k in range(parts):
                        place = (slab + k) % parts
                        moved = pltpu.roll(source[n + k], (place * width - start + LANES) % LANES, 1)
                        total = moved if k == 0 else jnp.where(lane == place, moved, total)
                    out[base + n // parts] = total.astype(BF16)

    return body


def deliver(sb):
    bk = sb.bk
    width = sb.width - 2 * sb.halo
    parts = LANES // width

    def body(me_ref, *refs):
        ins, outs = refs[: sb.groups], refs[sb.groups :]
        lane = lane_iota(sb.rows) // width
        src = lax.broadcasted_iota(jnp.int32, (2 * LANES, LANES), 0)
        dst = lax.broadcasted_iota(jnp.int32, (2 * LANES, LANES), 1)
        pz, at = src // LANES, src % LANES
        z = 2 * (at // bk.rhs) + pz
        join = jnp.where((at < bk.half) & (dst == z * bk.rhs + at % bk.rhs), 1.0, 0.0).astype(BF16)
        for index, out_ref in enumerate(outs):
            rows = out_ref.reshape(bk.q * bk.ex * bk.ey, LANES)
            base = index * (sb.tiles // parts)

            def home(t):
                k = t % parts
                total = ins[0][base + t // parts].astype(F32)
                for d in range(1, sb.groups):
                    place = (me_ref[d] + k) % parts
                    total = jnp.where(lane == place, ins[d][base + t // parts].astype(F32), total)
                return roll(total, -k * width).astype(BF16)

            for x in range(bk.ex):
                for y in range(bk.ey):
                    both = jnp.concatenate([home(bk.tile(x, y, 0)), home(bk.tile(x, y, 1))], axis=1)
                    out = dot(both, join)
                    rows[pl.ds(x * bk.ey + y, bk.q, stride=bk.ex * bk.ey), :] = out[: bk.q]

    return body


def in_slabs(bk, sb, right_side, cell_coef, inverse, couple, weights):
    count, order = sb.count, sb.order()
    square = (sb.rows, LANES)
    state = ((sb.tiles,) + square, F32)
    coarse = ((sb.tiles,) + square, BF16)
    faces = ((2 * len(sb.face_y(0)),) + square, BF16)
    one_face = (((len(sb.face_y(0)),) + square), BF16)

    def msg(n):
        return ((n,) + square, BF16)

    me = lax.axis_index("gx")
    slab_of = jnp.array([order.index(i) for i in range(count)], jnp.int32)
    others = (me + jnp.arange(count)) % count
    sources = (me - jnp.arange(count)) % count
    depth = sb.depth // 2 * sb.rhs
    send = jnp.concatenate([me[None], bk.own - sb.halo + depth * slab_of[others]]).astype(jnp.int32)
    back = jnp.concatenate([slab_of[me][None], sb.halo + sb.width * others]).astype(jnp.int32)
    arrive = slab_of[sources].astype(jnp.int32)

    layers = msg(sb.tiles * 2 * bk.rhs // LANES)
    home, up, down = call(
        home_prep(bk), [right_side, cell_coef.reshape(bk.ex * bk.ey, bk.ez)], [coarse, layers, layers],
        scratch=[((4,) + square, F32)],
    )
    below, above = shift(up, "gz", 1), shift(down, "gz", -1)
    pieces = call(
        scatter(sb), [send, home, below, above], [msg(sb.tiles // count)] * count, scalars=1
    )
    pieces = [shift(p, "gx", d) if d else p for d, p in enumerate(pieces)]

    def chain(v, step):
        n = lax.axis_size("gz")
        route = []
        for z in range(n):
            for s in range(count):
                total = (z * count + s + step) % (n * count)
                route.append((order[s] * n + z, order[total % count] * n + total // count))
        return lax.ppermute(v, ("gx", "gz"), route)

    def swap(v, step):
        return shift(v, "gy", step)

    edge = sb.face_y(-1)

    def assemble(me_ref, *refs):
        r_ref, y_ref = refs[count:]
        gather_state(sb, me_ref, refs[:count], r_ref)
        for m, t in enumerate(edge):
            y_ref[m] = r_ref[t].astype(BF16)

    r, moved = call(assemble, [send, *pieces], [state, one_face], scalars=1)
    moved = swap(moved, 1)
    sol = halos = pending = None
    flops = 1 << 27
    solve_scratch = [((sb.ny, 8 * sb.rows, 2 * LANES), BF16)]
    halo_msg = msg(sb.tiles * sb.halo // sb.width)
    refresh = (1, 4)

    for colour in range(8):
        par = (colour // 4, colour // 2 % 2, colour % 2)
        before = ((colour - 1) // 4, (colour - 1) // 2 % 2, (colour - 1) % 2)
        fresh = (colour - 1) in refresh
        turn = colour > 0 and par[1] != before[1]
        if turn or fresh:

            def finish(r_in, s_in, yy, gm, r_ref, s_ref, *outs, before=before, turn=turn):
                slab_ghosts(sb, before, r_ref, s_ref, gm, yy)
                if turn:
                    for m, t in enumerate(edge):
                        outs[0][m] = r_ref[t].astype(BF16)
                else:
                    emit_halo(sb, r_ref, *outs)

            outs = [one_face] if turn else [halo_msg, halo_msg]
            r, sol, *out = call(
                finish, [r, sol, pending, couple], [state, state] + outs, aliases={0: 0, 1: 1}
            )
            if turn:
                moved = swap(out[0], -1 if before[1] == 0 else 1)
            if turn and fresh:

                def turned(r_in, m_in, r_ref, u_ref, d_ref):
                    for m, t in enumerate(edge):
                        r_ref[t] = m_in[m].astype(F32)
                    emit_halo(sb, r_ref, u_ref, d_ref)

                r, *out = call(turned, [r, moved], [state, halo_msg, halo_msg], aliases={0: 0})
            if fresh:
                halos = (chain(out[0], 1), chain(out[1], -1))

                def solve_fresh(r_in, lo, hi, p, r_ref, c, fy, xs, par=par):
                    fill_slab_halo(sb, r_ref, lo, hi)
                    slab_solve(sb, par, r_ref, p, c, fy, xs)

                args = [r, *halos, inverse]
                body = solve_fresh
            else:
                args = [r, moved, inverse]
                body = None
        elif colour == 0:
            args, body = [r, moved, inverse], None
        else:

            def solve_next(r_in, s_in, yy, gm, p, r_ref, s_ref, c, fy, xs, par=par, before=before):
                slab_ghosts(sb, before, r_ref, s_ref, gm, yy)
                slab_solve(sb, par, r_ref, p, c, fy, xs)

            args, body = [r, sol, pending, couple, inverse], solve_next
        if body is None:

            def body(r_in, m_in, p, r_ref, c, fy, xs, par=par):
                for m, t in enumerate(edge):
                    r_ref[t] = m_in[m].astype(F32)
                slab_solve(sb, par, r_ref, p, c, fy, xs)

        with_sol = len(args) == 5
        kept = [state, state] if with_sol else [state]
        got = call(
            body, args, kept + [coarse, faces], scratch=solve_scratch, flops=flops,
            aliases={0: 0, 1: 1} if with_sol else {0: 0},
        )
        if with_sol:
            r, sol, c, fy = got
        else:
            r, c, fy = got
        if lax.axis_size("gy") == 2:
            pending = swap(fy, 1)
        else:
            n = len(edge)
            pending = jnp.concatenate([swap(fy[:n], -1), swap(fy[n:], 1)])
        ins = [r, c, weights] if colour == 0 else [r, sol, c, weights]
        r, sol = call(
            slab_change(sb, par, colour == 0), ins, [state, state], flops=flops,
            aliases={0: 0} if colour == 0 else {0: 0, 1: 1}, scratch=[coarse, coarse, coarse],
        )

    half = sb.tiles * depth // LANES

    def last(me_ref, r_in, s_in, yy, gm, r_ref, s_ref, *outs):
        slab_ghosts(sb, (1, 1, 1), r_ref, s_ref, gm, yy)
        collect(sb)(me_ref, r_ref, s_ref, *outs)

    r, sol, *parts = call(
        last, [back, r, sol, pending, couple], [state, state] + [msg(2 * half)] * count,
        aliases={1: 0, 2: 1}, scalars=1,
    )
    parts = [shift(p, "gx", d) if d else p for d, p in enumerate(parts)]
    whole = (right_side.shape, F32)
    return tuple(call(deliver(sb), [arrive, *parts], [whole, whole], hbm_out=True, scalars=1))


def on_device(right_side, cell_coef, cell_matrix, face_coupling, patch_inverse):
    dofs = cell_matrix.shape[0]
    ex, ey, ez = cell_coef.shape
    bk = Block(dofs, ex, ey, ez, right_side.shape[3] // ez)
    rows, tiles = bk.rows, bk.tiles
    grown = [(0, rows - dofs), (0, rows - dofs)]
    square = (rows, LANES)

    state = ((tiles,) + square, F32)
    coarse = ((tiles,) + square, BF16)
    face_x, face_y = ((bk.faces_x,) + square, BF16), ((2 * bk.faces_y,) + square, BF16)

    def msg(n):
        return ((n,) + square, BF16)

    (inverse,) = call(prep_inverse(bk), [patch_inverse], [((8 * rows, 8 * rows), BF16)])
    padded = jnp.pad(face_coupling, [(0, 0)] + grown)
    flipped = jnp.swapaxes(padded, 1, 2)
    pairs = [padded[0], flipped[0], padded[1], flipped[1], padded[2], flipped[2]]
    couple = jnp.stack(pairs[:4]).astype(BF16)
    weights = jnp.concatenate([jnp.pad(cell_matrix, grown)] + [-m for m in pairs], axis=1)
    weights = weights.astype(BF16)
    if Slab.fits(bk, lax.axis_size("gx")):
        sb = Slab(bk, lax.axis_size("gx"))
        return in_slabs(bk, sb, right_side, cell_coef, inverse, couple[2:], weights)

    r, ymsg = call(
        prep_state(bk), [right_side, cell_coef.reshape(ex * ey, ez)], [state, msg(ex)],
        scratch=[((4,) + square, F32)],
    )
    ymsg = shift(ymsg, "gy", 1)
    edge = 2 * ey
    inner = len(halo_cells(bk))
    r, zl, zh, xm, xl, xh = call(
        prep_halo(bk), [r, ymsg],
        [state, msg(inner // 4), msg(inner // 4), msg(edge // 2), msg(edge // 4), msg(edge // 4)],
        aliases={0: 0},
    )
    halo = (
        shift(zh, "gz", 1),
        shift(zl, "gz", -1),
        shift(xm, "gx", 1),
        shift2(xh, "gx", 1, "gz", 1),
        shift2(xl, "gx", 1, "gz", -1),
    )
    solve_scratch = [((bk.nx * bk.ny // 2, 8 * rows, 2 * LANES), BF16)]
    solve_outs = [coarse, face_x, face_x, face_y]
    flops = 1 << 27
    sol = None
    pending = None
    for colour in range(8):
        par = (colour // 4, colour // 2 % 2, colour % 2)
        if colour == 0:

            def body(r_in, zl, zh, xm, xl, xh, p, r_ref, c, fl, fh, fy, xs):
                fill_halo(bk, r_ref, zl, zh, xm, xl, xh)
                solve(bk, (0, 0, 0), r_ref, p, c, fl, fh, fy, xs)

            r, c, fl, fh, fy = call(
                body, [r, *halo, inverse], [state] + solve_outs,
                aliases={0: 0}, scratch=solve_scratch, flops=flops,
            )
        else:
            before = ((colour - 1) // 4, (colour - 1) // 2 % 2, (colour - 1) % 2)
            if par[1] == before[1]:

                def body(r_in, s_in, lo, hi, yy, gm, p, r_ref, s_ref, c, fl, fh, fy, xs, par=par, before=before):
                    ghosts(bk, before, r_ref, s_ref, gm, lo, hi, yy)
                    solve(bk, par, r_ref, p, c, fl, fh, fy, xs)

                r, sol, c, fl, fh, fy = call(
                    body, [r, sol, *pending, couple, inverse], [state, state] + solve_outs,
                    aliases={0: 0, 1: 1}, scratch=solve_scratch, flops=flops,
                )
            else:
                r, sol = move_region(bk, before, par, r, sol, pending, couple, msg, state)

                def body(r_in, p, r_ref, c, fl, fh, fy, xs, par=par):
                    solve(bk, par, r_ref, p, c, fl, fh, fy, xs)

                r, c, fl, fh, fy = call(
                    body, [r, inverse], [state] + solve_outs,
                    aliases={0: 0}, scratch=solve_scratch, flops=flops,
                )
        pending = exchange(fl, fh, fy, bk)
        if colour == 0:
            r, sol = call(
                own_change(bk, par, True), [r, c, weights], [state, state],
                aliases={0: 0}, scratch=[coarse, coarse], flops=flops,
            )
        else:
            r, sol = call(
                own_change(bk, par, False), [r, sol, c, weights], [state, state],
                aliases={0: 0, 1: 1}, scratch=[coarse, coarse], flops=flops,
            )
    whole = (right_side.shape, F32)
    (solution_out,) = call(leave(bk, None), [sol], [whole], hbm_out=True, flops=flops)

    def last(r_in, lo, hi, yy, gm, r_ref):
        ghosts(bk, (1, 1, 1), r_ref, None, gm, lo, hi, yy)

    (r,) = call(last, [r, *pending, couple], [state], aliases={0: 0})
    (residual_out,) = call(leave(bk, None), [r], [whole], hbm_out=True)
    return solution_out, residual_out


def exchange(fl, fh, fy, bk):
    below, above = shift(fh, "gx", 1), shift(fl, "gx", -1)
    if lax.axis_size("gy") == 2:
        ys = shift(fy, "gy", 1)
    else:
        n = bk.faces_y
        ys = jnp.concatenate([shift(fy[:n], "gy", -1), shift(fy[n:], "gy", 1)])
    return below, above, ys


def move_region(bk, before, par, r, sol, pending, couple, msg, state):
    to_home_y = before[1] == 0
    to_home_x = before[0] == 0 and par[0] == 1
    with_sol = before == (0, 0, 1)
    x_send = bk.face_x(-1, 1)
    x_home = bk.face_x(bk.ex - 1, 1)
    a = par[0]
    y_cells = bk.face_y(-1, a)
    sol_cells = [bk.tile(bk.ex - 1, bk.ey - 1, pz) for pz in range(2)]
    n_y = len(y_cells) + (2 if with_sol else 0)

    def finish(r_in, s_in, lo, hi, yy, gm, r_ref, s_ref, m_ref):
        ghosts(bk, before, r_ref, s_ref, gm, lo, hi, yy)
        if to_home_x:
            for m, t in enumerate(x_send):
                m_ref[m] = r_ref[t].astype(BF16)
        else:
            for m, t in enumerate(y_cells):
                m_ref[m] = r_ref[t].astype(BF16)
            if with_sol:
                for m, t in enumerate(sol_cells):
                    m_ref[len(y_cells) + m] = s_ref[t].astype(BF16)

    n_first = len(x_send) if to_home_x else n_y
    r, sol, m = call(
        finish, [r, sol, *pending, couple], [state, state, msg(n_first)], aliases={0: 0, 1: 1}
    )
    if to_home_x:
        m = shift(m, "gx", -1)

        def turn(r_in, m_in, r_ref, y_ref):
            for i, t in enumerate(x_home):
                r_ref[t] = m_in[i].astype(F32)
            for i, t in enumerate(y_cells):
                y_ref[i] = r_ref[t].astype(BF16)

        r, m = call(turn, [r, m], [state, msg(n_y)], aliases={0: 0})
    m = shift(m, "gy", -1 if to_home_y else 1)

    def place(r_in, s_in, m_in, r_ref, s_ref):
        for i, t in enumerate(y_cells):
            r_ref[t] = m_in[i].astype(F32)
        if with_sol:
            for i, t in enumerate(sol_cells):
                s_ref[t] = m_in[len(y_cells) + i].astype(F32)

    r, sol = call(place, [r, sol, m], [state, state], aliases={0: 0, 1: 1})
    return r, sol


def solution(mesh):
    placed = (P(None, "gx", "gy", "gz"), P("gx", "gy", "gz"), P(), P(), P())
    return jax.shard_map(
        on_device,
        mesh=mesh,
        in_specs=placed,
        out_specs=(P(None, "gx", "gy", "gz"), P(None, "gx", "gy", "gz")),
        check_vma=False,
    )
```

```python
import jax
import jax.numpy as jnp
from jax import lax
from jax.experimental import pallas as pl
from jax.experimental.pallas import tpu as pltpu
from jax.sharding import PartitionSpec as P

F32 = jnp.float32
BF16 = jnp.bfloat16
LANES = 128
VMEM_LIMIT = 28 * 1024 * 1024


class Block:
    def __init__(self, dofs, extent_x, extent_y, extent_z, rhs):
        assert extent_x % 2 == 0 and extent_y % 4 == 0 and extent_z * rhs == LANES
        self.q, self.ex, self.ey, self.ez, self.rhs = dofs, extent_x, extent_y, extent_z, rhs
        self.rows = -(-(dofs + 2) // 16) * 16
        self.nx, self.ny = extent_x // 2, extent_y // 2
        self.tiles = extent_x * extent_y * 2
        self.own = LANES // 4
        self.half = LANES // 2
        self.faces_x = 2 * extent_y
        self.faces_y = 2 * extent_x

    def tile(self, x, y, pz):
        px, py = x % 2, y % 2
        sx, sy = (x // 2) % self.nx, (y // 2) % self.ny
        return (((px * 2 + py) * 2 + pz) * self.nx + sx) * self.ny + sy

    def span(self, parity, extent):
        return range(parity - 1, parity - 1 + extent)

    def face_x(self, x, b):
        return [self.tile(x, y, pz) for y in self.span(b, self.ey) for pz in range(2)]

    def face_y(self, y, a):
        return [self.tile(x, y, pz) for x in self.span(a, self.ex) for pz in range(2)]


def lane_iota(rows):
    return lax.broadcasted_iota(jnp.int32, (rows, LANES), 1)


def roll(v, by):
    by = by % LANES
    return pltpu.roll(v, by, 1) if by else v


def dot(a, b):
    return jnp.dot(a, b, preferred_element_type=F32)


def call(body, ins, outs, aliases=None, scratch=(), flops=0, hbm_out=False, scalars=0):
    space = pl.BlockSpec(memory_space=pltpu.VMEM)
    table = pl.BlockSpec(memory_space=pltpu.SMEM)
    if hbm_out:
        shapes = [jax.ShapeDtypeStruct(s, d) for s, d in outs]
    else:
        shapes = [pltpu.VMEM(s, d) for s, d in outs]
    return pl.pallas_call(
        body,
        in_specs=[table] * scalars + [space] * (len(ins) - scalars),
        out_specs=[space] * len(outs),
        out_shape=shapes,
        scratch_shapes=[pltpu.VMEM(s, d) for s, d in scratch],
        input_output_aliases=aliases or {},
        compiler_params=pltpu.CompilerParams(vmem_limit_bytes=VMEM_LIMIT),
        cost_estimate=pl.CostEstimate(flops=flops, bytes_accessed=0, transcendentals=0) if flops else None,
    )(*ins)


def coef_row(bk, r_ref, t):
    return r_ref[t, bk.q : bk.q + 1, :] + r_ref[t, bk.q + 1 : bk.q + 2, :]


def shift(v, axis, distance):
    n = lax.axis_size(axis)
    return lax.ppermute(v, axis, [((i - distance) % n, i) for i in range(n)])


def shift2(v, first, d1, second, d2):
    n1, n2 = lax.axis_size(first), lax.axis_size(second)
    route = [
        (((i - d1) % n1) * n2 + (j - d2) % n2, i * n2 + j) for i in range(n1) for j in range(n2)
    ]
    return lax.ppermute(v, (first, second), route)


def pack(bk, r_ref, tiles, lanes_from, count, out_ref, parts):
    lane = lane_iota(bk.rows)
    for n in range(0, len(tiles), parts):
        total = None
        for k, t in enumerate(tiles[n : n + parts]):
            moved = roll(r_ref[t], k * count - lanes_from)
            total = moved if total is None else jnp.where(lane < k * count, total, moved)
        out_ref[n // parts] = total.astype(BF16)


def unpack(bk, msg_ref, n, lanes_to, count, parts):
    k = n % parts
    return roll(msg_ref[n // parts].astype(F32), lanes_to - k * count)


def prep_tables(bk):
    q, rows = bk.q, bk.rows

    def body(p_ref, m_ref, f_ref, o_ref, w_ref, g_ref):
        n = p_ref.shape[0]
        row = lax.broadcasted_iota(jnp.int32, (8 * rows, n), 0)
        col = lax.broadcasted_iota(jnp.int32, (8 * rows, n), 1)
        o, d = row // rows, row % rows
        pick = jnp.where((col == d * 8 + o) & (d < q), 1.0, 0.0).astype(BF16)
        left = dot(pick, p_ref[...]).astype(BF16)
        o_ref[...] = lax.dot_general(
            left, pick, (((1,), (1,)), ((), ())), preferred_element_type=F32
        ).astype(BF16)
        row = lax.broadcasted_iota(jnp.int32, (q, 7 * rows), 0)
        col = lax.broadcasted_iota(jnp.int32, (q, 7 * rows), 1)
        total = dot(m_ref[...].astype(BF16), jnp.where(col == row, 1.0, 0.0).astype(BF16))
        g_ref[...] = jnp.zeros_like(g_ref)
        w_ref[...] = jnp.zeros_like(w_ref)
        one = jnp.where(
            lax.broadcasted_iota(jnp.int32, (q, rows), 0) == lax.broadcasted_iota(jnp.int32, (q, rows), 1),
            1.0, 0.0,
        ).astype(BF16)
        for direction in range(3):
            face = f_ref[direction].astype(BF16)
            for side in range(2):
                at = rows * (1 + 2 * direction + side)
                place = jnp.where(col == row + at, 1.0, 0.0).astype(BF16)
                dims = (((1 - side,), (0,)), ((), ()))
                total = total - lax.dot_general(face, place, dims, preferred_element_type=F32)
                if direction < 2:
                    g_ref[2 * direction + side, :q, :] = lax.dot_general(
                        face, one, dims, preferred_element_type=F32
                    ).astype(BF16)
        w_ref[:q, :] = total.astype(BF16)

    return body


def prep_state(bk):
    def body(rs_ref, cc_ref, r_ref, y_ref, scr):
        rows = rs_ref.reshape(bk.q * bk.ex * bk.ey, LANES)
        src = lax.broadcasted_iota(jnp.int32, (2 * LANES, 2 * LANES), 0) % LANES
        dst = lax.broadcasted_iota(jnp.int32, (2 * LANES, 2 * LANES), 1)
        pz, lane = dst // LANES, dst % LANES - bk.own
        z = 2 * (lane // bk.rhs) + pz
        inside = (lane >= 0) & (lane < bk.half)
        split = jnp.where(inside & (src == z * bk.rhs + lane % bk.rhs), 1.0, 0.0).astype(BF16)
        zz = lax.broadcasted_iota(jnp.int32, (bk.ez, LANES), 0)
        ll = lax.broadcasted_iota(jnp.int32, (bk.ez, LANES), 1)
        spread = jnp.where(ll // bk.rhs == zz, 1.0, 0.0).astype(BF16)
        coef = cc_ref[...]
        high = coef.astype(BF16)
        low = (coef - high.astype(F32)).astype(BF16)
        high, low = dot(high, spread), dot(low, spread)
        scr[...] = jnp.zeros_like(scr)
        for x in range(bk.ex):
            for y in range(bk.ey):
                n = x * bk.ey + y
                scr[n % 4, : bk.q, :] = rows[pl.ds(n, bk.q, stride=bk.ex * bk.ey), :]
                scr[n % 4, bk.q : bk.q + 1, :] = high[n : n + 1]
                scr[n % 4, bk.q + 1 : bk.q + 2, :] = low[n : n + 1]
                raw = scr[n % 4]
                top = raw.astype(BF16)
                rest = (raw - top.astype(F32)).astype(BF16)
                out = dot(jnp.concatenate([top, rest], axis=1), split)
                r_ref[bk.tile(x, y, 0)] = out[:, :LANES]
                r_ref[bk.tile(x, y, 1)] = out[:, LANES:]
        tiles = [bk.tile(x, bk.ey - 1, pz) for x in range(bk.ex) for pz in range(2)]
        pack(bk, r_ref, tiles, bk.own, bk.half, y_ref, 2)

    return body


def halo_cells(bk):
    return [
        bk.tile(x, y, pz)
        for x in range(bk.ex - 1)
        for y in bk.span(0, bk.ey)
        for pz in range(2)
    ]


def prep_halo(bk):
    def body(r_in, y_ref, r_ref, zl_ref, zh_ref, x_ref, xl_ref, xh_ref):
        n = 0
        for x in range(bk.ex):
            for pz in range(2):
                r_ref[bk.tile(x, -1, pz)] = unpack(bk, y_ref, n, bk.own, bk.half, 2)
                n += 1
        cells = halo_cells(bk)
        pack(bk, r_ref, cells, bk.own, bk.own, zl_ref, 4)
        pack(bk, r_ref, cells, 2 * bk.own, bk.own, zh_ref, 4)
        edge = bk.face_x(bk.ex - 1, 0)
        pack(bk, r_ref, edge, bk.own, bk.half, x_ref, 2)
        pack(bk, r_ref, edge, bk.own, bk.own, xl_ref, 4)
        pack(bk, r_ref, edge, 2 * bk.own, bk.own, xh_ref, 4)

    return body


def fill_halo(bk, r_ref, zl_ref, zh_ref, x_ref, xl_ref, xh_ref):
    lane = lane_iota(bk.rows)
    below, above = lane < bk.own, lane >= 3 * bk.own

    def joined(own, low_ref, high_ref, n):
        low = unpack(bk, low_ref, n, 0, bk.own, 4)
        high = unpack(bk, high_ref, n, 3 * bk.own, bk.own, 4)
        return jnp.where(below, low, jnp.where(above, high, own))

    for n, t in enumerate(halo_cells(bk)):
        r_ref[t] = joined(r_ref[t], zl_ref, zh_ref, n)
    for n, t in enumerate(bk.face_x(-1, 0)):
        r_ref[t] = joined(unpack(bk, x_ref, n, bk.own, bk.half, 2), xl_ref, xh_ref, n)


def solve(bk, colour, r_ref, p_ref, c_ref, xl_ref, xh_ref, y_ref, xs_ref):
    a, b, g = colour
    back = bk.rhs
    n = 0
    for px in range(bk.nx):
        for py in range(0, bk.ny, 2):
            cells = []
            for half in range(2):
                for o in range(8):
                    x = a - 1 + 2 * px + o // 4
                    y = b - 1 + 2 * (py + half) + o // 2 % 2
                    pz = o % 2 if g else 1 - o % 2
                    t = bk.tile(x, y, pz)
                    scale = lax.rsqrt(coef_row(bk, r_ref, t))
                    scaled = r_ref[t] * scale
                    if g == 0 and pz == 1:
                        scaled = roll(scaled, back)
                    lanes = slice(half * LANES, (half + 1) * LANES)
                    xs_ref[n, o * bk.rows : (o + 1) * bk.rows, lanes] = scaled.astype(BF16)
                    cells.append((half, o, t, scale, g == 0 and pz == 1))
            solved = dot(p_ref[...], xs_ref[n])
            for half, o, t, scale, moved in cells:
                v = solved[o * bk.rows : (o + 1) * bk.rows, half * LANES : (half + 1) * LANES]
                if moved:
                    v = roll(v, -back)
                c_ref[t] = (v * scale).astype(BF16)
            n += 1
    for m, t in enumerate(bk.face_x(a - 1, b)):
        xl_ref[m] = c_ref[t]
    for m, t in enumerate(bk.face_x(a - 2 + bk.ex, b)):
        xh_ref[m] = c_ref[t]
    for m, t in enumerate(bk.face_y(b - 1, a) + bk.face_y(b - 2 + bk.ey, a)):
        y_ref[m] = c_ref[t]


def ghosts(bk, colour, r_ref, sol_ref, g_ref, from_below, from_above, y_ref):
    a, b, g = colour

    def add(matrix, tiles, ghost_ref, base):
        for m in range(0, len(tiles), 2):
            two = jnp.concatenate([ghost_ref[base + m], ghost_ref[base + m + 1]], axis=1)
            change = dot(g_ref[matrix], two)
            r_ref[tiles[m]] += change[:, :LANES]
            r_ref[tiles[m + 1]] += change[:, LANES:]

    add(0, bk.face_x(a - 2 + bk.ex, b), from_above, 0)
    add(1, bk.face_x(a - 1, b), from_below, 0)
    add(2, bk.face_y(b - 2 + bk.ey, a), y_ref, 0)
    add(3, bk.face_y(b - 1, a), y_ref, bk.faces_y)
    if a == 0:
        for m, t in enumerate(bk.face_x(bk.ex - 1, b)):
            sol_ref[t] += from_above[m].astype(F32)
    if b == 0:
        m = 0
        for x in bk.span(a, bk.ex):
            for pz in range(2):
                if x >= 0:
                    sol_ref[bk.tile(x, bk.ey - 1, pz)] += y_ref[m].astype(F32)
                m += 1


def own_change(bk, colour, first):
    a, b, g = colour

    def body(*refs):
        if first:
            r_in, c_ref, w_ref, r_ref, sol_ref, cm_ref, cz_ref = refs
        else:
            r_in, sol_in, c_ref, w_ref, r_ref, sol_ref, cm_ref, cz_ref = refs
        xs, ys = bk.span(a, bk.ex), bk.span(b, bk.ey)
        for x in xs:
            for y in ys:
                for pz in range(2):
                    t = bk.tile(x, y, pz)
                    c = c_ref[t].astype(F32)
                    cm_ref[t] = (c * coef_row(bk, r_ref, t)).astype(BF16)
                    cz_ref[t] = roll(c_ref[t], bk.rhs if pz else -bk.rhs)
                    if x >= 0 and y >= 0:
                        sol_ref[t] = c if first else sol_ref[t] + c
                    elif first:
                        sol_ref[t] = jnp.zeros_like(c)
        nothing = jnp.zeros((bk.rows, LANES), BF16)

        def at(x, y, pz):
            return c_ref[bk.tile(x, y, pz)] if x in xs and y in ys else nothing

        def stack(x, y, pz):
            other = bk.tile(x, y, 1 - pz)
            near, far = c_ref[other], cz_ref[other]
            return jnp.concatenate(
                [
                    cm_ref[bk.tile(x, y, pz)],
                    at(x + 1, y, pz),
                    at(x - 1, y, pz),
                    at(x, y + 1, pz),
                    at(x, y - 1, pz),
                    far if pz else near,
                    near if pz else far,
                ],
                axis=0,
            )

        for x in xs:
            for y in ys:
                both = jnp.concatenate([stack(x, y, 0), stack(x, y, 1)], axis=1)
                change = dot(w_ref[...], both)
                for pz in range(2):
                    r_ref[bk.tile(x, y, pz)] -= change[:, pz * LANES : (pz + 1) * LANES]

    return body


def leave(bk, ref):
    def body(tile_ref, out_ref):
        rows = out_ref.reshape(bk.q * bk.ex * bk.ey, LANES)
        src = lax.broadcasted_iota(jnp.int32, (2 * LANES, LANES), 0)
        dst = lax.broadcasted_iota(jnp.int32, (2 * LANES, LANES), 1)
        pz, lane = src // LANES, src % LANES - bk.own
        z = 2 * (lane // bk.rhs) + pz
        inside = (lane >= 0) & (lane < bk.half)
        join = jnp.where(inside & (dst == z * bk.rhs + lane % bk.rhs), 1.0, 0.0).astype(BF16)
        for x in range(bk.ex):
            for y in range(bk.ey):
                both = jnp.concatenate(
                    [tile_ref[bk.tile(x, y, 0)], tile_ref[bk.tile(x, y, 1)]], axis=1
                )
                top = both.astype(BF16)
                rest = (both - top.astype(F32)).astype(BF16)
                out = dot(top, join) + dot(rest, join)
                rows[pl.ds(x * bk.ey + y, bk.q, stride=bk.ex * bk.ey), :] = out[: bk.q]

    return body


class Slab:
    def __init__(self, bk, count):
        self.bk, self.count = bk, count
        self.q, self.rhs, self.rows, self.ny = bk.q, bk.rhs, bk.rows, bk.ny
        self.ey = bk.ey
        self.groups = count
        self.width = LANES // count
        self.depth = bk.ez // count
        self.halo = 2 * bk.rhs
        self.tiles = bk.tiles

    @staticmethod
    def fits(bk, count):
        depth = bk.ez // count
        return (
            bk.ez % count == 0
            and depth % 2 == 0
            and bk.nx == 2
            and (depth // 2 + 4) * bk.rhs * count == LANES
            and bk.tiles % 16 == 0
        )

    def tile(self, px, x2, y, pz):
        return (((px * 2 + y % 2) * 2 + pz) * 2 + x2) * self.ny + (y // 2) % self.ny

    def face_y(self, y):
        return [self.tile(px, x2, y, pz) for px in range(2) for x2 in range(2) for pz in range(2)]

    def place(self, device):
        slab = device * 0
        for s, d in enumerate(self.order()):
            slab = jnp.where(device == d, s, slab)
        return slab

    def order(self):
        return [0, 1, 3, 2] if self.count == 4 else list(range(self.count))


def home_prep(bk):
    def body(rs_ref, cc_ref, h_ref, up_ref, down_ref, scr):
        rows = rs_ref.reshape(bk.q * bk.ex * bk.ey, LANES)
        src = lax.broadcasted_iota(jnp.int32, (LANES, 2 * LANES), 0)
        dst = lax.broadcasted_iota(jnp.int32, (LANES, 2 * LANES), 1)
        pz, lane = dst // LANES, dst % LANES - bk.own
        z = 2 * (lane // bk.rhs) + pz
        inside = (lane >= 0) & (lane < bk.half)
        split = jnp.where(inside & (src == z * bk.rhs + lane % bk.rhs), 1.0, 0.0).astype(BF16)
        zz = lax.broadcasted_iota(jnp.int32, (bk.ez, LANES), 0)
        ll = lax.broadcasted_iota(jnp.int32, (bk.ez, LANES), 1)
        spread = jnp.where(ll // bk.rhs == zz, 1.0, 0.0).astype(BF16)
        coef = cc_ref[...]
        high = coef.astype(BF16)
        low = (coef - high.astype(F32)).astype(BF16)
        high, low = dot(high, spread), dot(low, spread)
        scr[...] = jnp.zeros_like(scr)
        for x in range(bk.ex):
            for y in range(bk.ey):
                n = x * bk.ey + y
                scr[n % 4, : bk.q, :] = rows[pl.ds(n, bk.q, stride=bk.ex * bk.ey), :]
                scr[n % 4, bk.q : bk.q + 1, :] = high[n : n + 1]
                scr[n % 4, bk.q + 1 : bk.q + 2, :] = low[n : n + 1]
                out = dot(scr[n % 4].astype(BF16), split)
                h_ref[bk.tile(x, y, 0)] = out[:, :LANES].astype(BF16)
                h_ref[bk.tile(x, y, 1)] = out[:, LANES:].astype(BF16)
        width = 2 * bk.rhs
        cells = list(range(bk.tiles))
        pack(bk, h_ref, cells, bk.own + bk.half - width, width, up_ref, LANES // width)
        pack(bk, h_ref, cells, bk.own, 2 * width, down_ref, LANES // (2 * width))

    return body


def scatter(sb):
    bk, parts = sb.bk, sb.groups
    width = 2 * bk.rhs
    per = LANES // width

    def body(h_ref, below_ref, above_ref, *outs):
        lane = lane_iota(sb.rows)
        low = (lane >= bk.own - width) & (lane < bk.own)
        high = (lane >= bk.own + bk.half) & (lane < bk.own + bk.half + 2 * width)
        me = lax.axis_index("gx")
        step = bk.half // parts
        groups = []
        for d in range(parts):
            slab = sb.place((me + d) % parts)
            groups.append((lane - slab * step + LANES) % LANES // sb.width)
        for n in range(0, sb.tiles, parts):
            totals = [None] * parts
            for k in range(parts):
                t = n + k
                pz = t // (2 * sb.ny) % 2
                from_low = roll(below_ref[t // per], bk.own - width - t % per * width)
                m = t % (per // 2)
                from_high = roll(above_ref[t // (per // 2)], bk.own + bk.half - m * 2 * width)
                v = jnp.where(low, from_low, h_ref[t])
                v = jnp.where(high, from_high, v)
                start = bk.own - (2 if pz else 1) * bk.rhs
                place = (me + k) % parts
                v = pltpu.roll(v, (place * sb.width - start + LANES) % LANES, 1)
                for d in range(parts):
                    totals[d] = v if k == 0 else jnp.where(groups[d] == place, v, totals[d])
            for d, out in enumerate(outs):
                out[n // parts] = totals[d]

    return body


def gather_state(sb, parts_refs, r_ref):
    parts = sb.groups
    me = lax.axis_index("gx")
    by = sb.place(me) * (sb.bk.half // parts)
    group = (lane_iota(sb.rows) - by + LANES) % LANES // sb.width
    for t in range(sb.tiles):
        k = t % parts
        total = parts_refs[0][t // parts]
        for d in range(1, parts):
            source = (me - d + parts) % parts
            total = jnp.where(group == (source + k) % parts, parts_refs[d][t // parts], total)
        r_ref[t] = pltpu.roll(total, (2 * LANES - k * sb.width - by) % LANES, 1).astype(F32)


def slab_solve(sb, colour, r_ref, p_ref, c_ref, y_ref, xs_ref):
    a, b, g = colour
    rows = sb.rows
    n = 0
    for x2 in range(2):
        for py in range(0, sb.ny, 2):
            cells = []
            for half in range(2):
                for o in range(8):
                    xo, y = o // 4, b - 1 + 2 * (py + half) + o // 2 % 2
                    pz = o % 2 if g else 1 - o % 2
                    moved = -sb.rhs if g == 1 and pz == 1 else 0
                    if a or xo == 1:
                        t = sb.tile(xo if a else 0, x2, y, pz)
                    else:
                        t = sb.tile(1, 1 - x2, y, pz)
                        moved += 0 if x2 else sb.width
                    scale = lax.rsqrt(coef_row(sb, r_ref, t))
                    lanes = slice(half * LANES, (half + 1) * LANES)
                    xs_ref[n, o * rows : (o + 1) * rows, lanes] = roll(
                        r_ref[t] * scale, moved
                    ).astype(BF16)
                    cells.append((half, o, t, scale, moved))
            solved = dot(p_ref[...], xs_ref[n])
            for half, o, t, scale, moved in cells:
                v = solved[o * rows : (o + 1) * rows, half * LANES : (half + 1) * LANES]
                c_ref[t] = (roll(v, -moved) * scale).astype(BF16)
            n += 1
    for m, t in enumerate(sb.face_y(b - 1) + sb.face_y(b - 2 + sb.ey)):
        y_ref[m] = c_ref[t]


def slab_ghosts(sb, colour, r_ref, sol_ref, g_ref, y_ref):
    a, b, g = colour
    count = len(sb.face_y(0))
    for matrix, y, base in ((2, b - 2 + sb.ey, 0), (3, b - 1, count)):
        tiles = sb.face_y(y)
        for m in range(0, count, 2):
            two = jnp.concatenate([y_ref[base + m], y_ref[base + m + 1]], axis=1)
            change = dot(g_ref[matrix], two)
            r_ref[tiles[m]] += change[:, :LANES]
            r_ref[tiles[m + 1]] += change[:, LANES:]
    if b == 0:
        for m, t in enumerate(sb.face_y(sb.ey - 1)):
            sol_ref[t] += y_ref[m].astype(F32)


def slab_change(sb, colour, first):
    a, b, g = colour

    def body(*refs):
        if first:
            r_in, c_ref, w_ref, r_ref, sol_ref, cm_ref, cz_ref, cx_ref = refs
        else:
            r_in, sol_in, c_ref, w_ref, r_ref, sol_ref, cm_ref, cz_ref, cx_ref = refs
        ys = sb.bk.span(b, sb.ey)
        cells = [(px, x2, y) for px in range(2) for x2 in range(2) for y in ys]
        for px, x2, y in cells:
            for pz in range(2):
                t = sb.tile(px, x2, y, pz)
                c = c_ref[t].astype(F32)
                cm_ref[t] = (c * coef_row(sb, r_ref, t)).astype(BF16)
                cz_ref[t] = roll(c_ref[t], -sb.rhs if pz else sb.rhs)
                if px == x2:
                    cx_ref[t] = roll(c_ref[t], sb.width if px else -sb.width)
                if y >= 0:
                    sol_ref[t] = c if first else sol_ref[t] + c
                elif first:
                    sol_ref[t] = jnp.zeros_like(c)
        nothing = jnp.zeros((sb.rows, LANES), BF16)

        def stack(px, x2, y, pz):
            beside = c_ref[sb.tile(1 - px, x2, y, pz)]
            across = (cx_ref if px == x2 else c_ref)[sb.tile(1 - px, 1 - x2, y, pz)]
            other = sb.tile(px, x2, y, 1 - pz)
            near, far = c_ref[other], cz_ref[other]
            return jnp.concatenate(
                [
                    cm_ref[sb.tile(px, x2, y, pz)],
                    across if px else beside,
                    beside if px else across,
                    c_ref[sb.tile(px, x2, y + 1, pz)] if y + 1 in ys else nothing,
                    c_ref[sb.tile(px, x2, y - 1, pz)] if y - 1 in ys else nothing,
                    near if pz else far,
                    far if pz else near,
                ],
                axis=0,
            )

        for px, x2, y in cells:
            both = jnp.concatenate([stack(px, x2, y, 0), stack(px, x2, y, 1)], axis=1)
            change = dot(w_ref[...], both)
            for pz in range(2):
                r_ref[sb.tile(px, x2, y, pz)] -= change[:, pz * LANES : (pz + 1) * LANES]

    return body


def emit_halo(sb, r_ref, up_ref, down_ref):
    lane = lane_iota(sb.rows) % sb.width
    top = sb.width - 2 * sb.halo
    parts = sb.width // sb.halo
    for ref, start in ((up_ref, top), (down_ref, sb.halo)):
        for n in range(0, sb.tiles, parts):
            total = None
            for k in range(parts):
                moved = roll(r_ref[n + k], k * sb.halo - start)
                total = moved if k == 0 else jnp.where(lane < k * sb.halo, total, moved)
            ref[n // parts] = total.astype(BF16)


def fill_slab_halo(sb, r_ref, below_ref, above_ref):
    lane = lane_iota(sb.rows) % sb.width
    parts = sb.width // sb.halo
    for t in range(sb.tiles):
        k = t % parts
        low = roll(below_ref[t // parts].astype(F32), -k * sb.halo)
        high = roll(above_ref[t // parts].astype(F32), sb.width - sb.halo - k * sb.halo)
        own = jnp.where(lane < sb.halo, low, r_ref[t])
        r_ref[t] = jnp.where(lane >= sb.width - sb.halo, high, own)


def collect(sb, source, base, outs, extras, extra_at):
    width = sb.width - 2 * sb.halo
    parts = LANES // width
    lane = lane_iota(sb.rows)
    piece = lane // width
    me = lax.axis_index("gx")
    slab = sb.place(me)
    offset = sb.bk.own // width
    for n in range(0, sb.tiles, parts):
        totals = [None] * len(outs)
        for k in range(parts):
            by = (offset + slab + k) * width - sb.halo
            v = pltpu.roll(source[n + k].astype(BF16), by % LANES, 1)
            for d in range(len(outs)):
                place = (offset + slab + k + 2 * ((me + d) % sb.groups)) % parts
                totals[d] = v if k == 0 else jnp.where(piece == place, v, totals[d])
        for d, out in enumerate(outs):
            out[base + n // parts] = totals[d]
    per = sb.width // sb.rhs
    evens = even_tiles(sb)
    joined = []
    for m in range(sb.groups):
        total = None
        for k, t in enumerate(evens[m * per : (m + 1) * per]):
            v = roll(source[t].astype(BF16), k * sb.rhs - (sb.width - sb.halo - sb.rhs))
            total = v if k == 0 else jnp.where(lane % sb.width < k * sb.rhs, total, v)
        joined.append(roll(total, m * sb.width))
    for u, out in enumerate(extras):
        total = joined[0]
        for m in range(1, sb.groups):
            total = jnp.where(lane // sb.width == (u + m) % sb.groups, joined[m], total)
        out[extra_at] = total


def even_tiles(sb):
    return [t for t in range(sb.tiles) if t // (2 * sb.ny) % 2 == 0]


def deliver(sb):
    bk = sb.bk
    width = sb.width - 2 * sb.halo
    parts = LANES // width
    per = sb.width // sb.rhs

    def body(*refs):
        ins, extras, outs = refs[: sb.groups], refs[sb.groups : 2 * sb.groups], refs[2 * sb.groups :]
        lane = lane_iota(sb.rows)
        piece = lane // width
        first = (lane >= bk.own) & (lane < bk.own + bk.rhs)
        src = lax.broadcasted_iota(jnp.int32, (2 * LANES, LANES), 0)
        dst = lax.broadcasted_iota(jnp.int32, (2 * LANES, LANES), 1)
        pz, at = src // LANES, src % LANES - bk.own
        z = 2 * (at // bk.rhs) + pz
        inside = (at >= 0) & (at < bk.half)
        join = jnp.where(inside & (dst == z * bk.rhs + at % bk.rhs), 1.0, 0.0).astype(BF16)
        me = lax.axis_index("gx")
        slabs = [sb.place((me - d + sb.groups) % sb.groups) for d in range(sb.groups)]
        evens = even_tiles(sb)
        for index, out_ref in enumerate(outs):
            rows = out_ref.reshape(bk.q * bk.ex * bk.ey, LANES)
            base = index * (sb.tiles // parts)
            layer = extras[0][index]
            for e in extras[1:]:
                layer = layer + e[index]

            def home(t, even):
                k = t % parts
                total = ins[0][base + t // parts]
                for d in range(1, sb.groups):
                    place = (bk.own // width + slabs[d] + k + 2 * me) % parts
                    total = jnp.where(piece == place, ins[d][base + t // parts], total)
                by = (3 * LANES - (k + 2 * me) * width + (bk.rhs if even else 0)) % LANES
                total = pltpu.roll(total, by, 1)
                if not even:
                    return total
                n = evens.index(t)
                by = (bk.own + 3 * LANES - (me + n // per) * sb.width - n % per * sb.rhs) % LANES
                return jnp.where(first, pltpu.roll(layer, by, 1), total)

            for x in range(bk.ex):
                for y in range(bk.ey):
                    both = jnp.concatenate(
                        [home(bk.tile(x, y, 0), True), home(bk.tile(x, y, 1), False)], axis=1
                    )
                    out = dot(both, join)
                    rows[pl.ds(x * bk.ey + y, bk.q, stride=bk.ex * bk.ey), :] = out[: bk.q]

    return body


def in_slabs(bk, sb, right_side, cell_coef, inverse, couple, weights):
    count, order = sb.count, sb.order()
    square = (sb.rows, LANES)
    state = ((sb.tiles,) + square, F32)
    coarse = ((sb.tiles,) + square, BF16)
    faces = ((2 * len(sb.face_y(0)),) + square, BF16)
    one_face = (((len(sb.face_y(0)),) + square), BF16)

    def msg(n):
        return ((n,) + square, BF16)

    width = 2 * bk.rhs
    up_layers, down_layers = msg(sb.tiles * width // LANES), msg(sb.tiles * 2 * width // LANES)
    home, up, down = call(
        home_prep(bk), [right_side, cell_coef.reshape(bk.ex * bk.ey, bk.ez)],
        [coarse, up_layers, down_layers], scratch=[((4,) + square, F32)],
    )
    below, above = shift(up, "gz", 1), shift(down, "gz", -1)
    pieces = call(scatter(sb), [home, below, above], [msg(sb.tiles // count)] * count)
    pieces = [shift(p, "gx", d) if d else p for d, p in enumerate(pieces)]

    def chain(v, step):
        n = lax.axis_size("gz")
        route = []
        for z in range(n):
            for s in range(count):
                total = (z * count + s + step) % (n * count)
                route.append((order[s] * n + z, order[total % count] * n + total // count))
        return lax.ppermute(v, ("gx", "gz"), route)

    def swap(v, step):
        return shift(v, "gy", step)

    edge = sb.face_y(-1)

    def assemble(*refs):
        r_ref, y_ref = refs[count:]
        gather_state(sb, refs[:count], r_ref)
        for m, t in enumerate(edge):
            y_ref[m] = r_ref[t].astype(BF16)

    r, moved = call(assemble, pieces, [state, one_face])
    moved = swap(moved, 1)
    sol = halos = pending = None
    flops = 1 << 27
    solve_scratch = [((sb.ny, 8 * sb.rows, 2 * LANES), BF16)]
    halo_msg = msg(sb.tiles * sb.halo // sb.width)
    refresh = (3,)

    for colour in range(8):
        par = (colour // 4, colour // 2 % 2, colour % 2)
        before = ((colour - 1) // 4, (colour - 1) // 2 % 2, (colour - 1) % 2)
        fresh = (colour - 1) in refresh
        turn = colour > 0 and par[1] != before[1]
        if turn or fresh:

            def finish(r_in, s_in, yy, gm, r_ref, s_ref, *outs, before=before, turn=turn):
                slab_ghosts(sb, before, r_ref, s_ref, gm, yy)
                if turn:
                    for m, t in enumerate(edge):
                        outs[0][m] = r_ref[t].astype(BF16)
                else:
                    emit_halo(sb, r_ref, *outs)

            outs = [one_face] if turn else [halo_msg, halo_msg]
            r, sol, *out = call(
                finish, [r, sol, pending, couple], [state, state] + outs, aliases={0: 0, 1: 1}
            )
            if turn:
                moved = swap(out[0], -1 if before[1] == 0 else 1)
            if turn and fresh:

                def turned(r_in, m_in, r_ref, u_ref, d_ref):
                    for m, t in enumerate(edge):
                        r_ref[t] = m_in[m].astype(F32)
                    emit_halo(sb, r_ref, u_ref, d_ref)

                r, *out = call(turned, [r, moved], [state, halo_msg, halo_msg], aliases={0: 0})
            if fresh:
                halos = (chain(out[0], 1), chain(out[1], -1))

                def solve_fresh(r_in, lo, hi, p, r_ref, c, fy, xs, par=par):
                    fill_slab_halo(sb, r_ref, lo, hi)
                    slab_solve(sb, par, r_ref, p, c, fy, xs)

                args = [r, *halos, inverse]
                body = solve_fresh
            else:
                args = [r, moved, inverse]
                body = None
        elif colour == 0:
            args, body = [r, moved, inverse], None
        else:

            def solve_next(r_in, s_in, yy, gm, p, r_ref, s_ref, c, fy, xs, par=par, before=before):
                slab_ghosts(sb, before, r_ref, s_ref, gm, yy)
                slab_solve(sb, par, r_ref, p, c, fy, xs)

            args, body = [r, sol, pending, couple, inverse], solve_next
        if body is None:

            def body(r_in, m_in, p, r_ref, c, fy, xs, par=par):
                for m, t in enumerate(edge):
                    r_ref[t] = m_in[m].astype(F32)
                slab_solve(sb, par, r_ref, p, c, fy, xs)

        with_sol = len(args) == 5
        kept = [state, state] if with_sol else [state]
        got = call(
            body, args, kept + [coarse, faces], scratch=solve_scratch, flops=flops,
            aliases={0: 0, 1: 1} if with_sol else {0: 0},
        )
        if with_sol:
            r, sol, c, fy = got
        else:
            r, c, fy = got
        if lax.axis_size("gy") == 2:
            pending = swap(fy, 1)
        else:
            n = len(edge)
            pending = jnp.concatenate([swap(fy[:n], -1), swap(fy[n:], 1)])
        ins = [r, c, weights] if colour == 0 else [r, sol, c, weights]
        r, sol = call(
            slab_change(sb, par, colour == 0), ins, [state, state], flops=flops,
            aliases={0: 0} if colour == 0 else {0: 0, 1: 1}, scratch=[coarse, coarse, coarse],
        )

    each = sb.tiles * (sb.depth // 2 * sb.rhs) // LANES

    def last(r_in, s_in, yy, gm, r_ref, s_ref, *outs):
        slab_ghosts(sb, (1, 1, 1), r_ref, s_ref, gm, yy)
        collect(sb, s_ref, 0, outs[:count], outs[count:], 0)
        collect(sb, r_ref, each, outs[:count], outs[count:], 1)

    r, sol, *parts = call(
        last, [r, sol, pending, couple], [state, state] + [msg(2 * each)] * count + [msg(2)] * count,
        aliases={0: 0, 1: 1},
    )

    def next_block(v, to):
        n = lax.axis_size("gz")
        return lax.ppermute(
            v, ("gx", "gz"), [(order[-1] * n + z, to * n + (z + 1) % n) for z in range(n)]
        )

    extras = [next_block(v, u) for u, v in enumerate(parts[count:])]
    parts = [shift(p, "gx", d) if d else p for d, p in enumerate(parts[:count])]
    whole = (right_side.shape, F32)
    return tuple(call(deliver(sb), parts + extras, [whole, whole], hbm_out=True))


def on_device(right_side, cell_coef, cell_matrix, face_coupling, patch_inverse):
    dofs = cell_matrix.shape[0]
    ex, ey, ez = cell_coef.shape
    bk = Block(dofs, ex, ey, ez, right_side.shape[3] // ez)
    rows, tiles = bk.rows, bk.tiles
    square = (rows, LANES)

    state = ((tiles,) + square, F32)
    coarse = ((tiles,) + square, BF16)
    face_x, face_y = ((bk.faces_x,) + square, BF16), ((2 * bk.faces_y,) + square, BF16)

    def msg(n):
        return ((n,) + square, BF16)

    inverse, weights, couple = call(
        prep_tables(bk), [patch_inverse, cell_matrix, face_coupling],
        [((8 * rows, 8 * rows), BF16), ((rows, 7 * rows), BF16), ((4, rows, rows), BF16)],
    )
    if Slab.fits(bk, lax.axis_size("gx")):
        sb = Slab(bk, lax.axis_size("gx"))
        return in_slabs(bk, sb, right_side, cell_coef, inverse, couple, weights)

    r, ymsg = call(
        prep_state(bk), [right_side, cell_coef.reshape(ex * ey, ez)], [state, msg(ex)],
        scratch=[((4,) + square, F32)],
    )
    ymsg = shift(ymsg, "gy", 1)
    edge = 2 * ey
    inner = len(halo_cells(bk))
    r, zl, zh, xm, xl, xh = call(
        prep_halo(bk), [r, ymsg],
        [state, msg(inner // 4), msg(inner // 4), msg(edge // 2), msg(edge // 4), msg(edge // 4)],
        aliases={0: 0},
    )
    halo = (
        shift(zh, "gz", 1),
        shift(zl, "gz", -1),
        shift(xm, "gx", 1),
        shift2(xh, "gx", 1, "gz", 1),
        shift2(xl, "gx", 1, "gz", -1),
    )
    solve_scratch = [((bk.nx * bk.ny // 2, 8 * rows, 2 * LANES), BF16)]
    solve_outs = [coarse, face_x, face_x, face_y]
    flops = 1 << 27
    sol = None
    pending = None
    for colour in range(8):
        par = (colour // 4, colour // 2 % 2, colour % 2)
        if colour == 0:

            def body(r_in, zl, zh, xm, xl, xh, p, r_ref, c, fl, fh, fy, xs):
                fill_halo(bk, r_ref, zl, zh, xm, xl, xh)
                solve(bk, (0, 0, 0), r_ref, p, c, fl, fh, fy, xs)

            r, c, fl, fh, fy = call(
                body, [r, *halo, inverse], [state] + solve_outs,
                aliases={0: 0}, scratch=solve_scratch, flops=flops,
            )
        else:
            before = ((colour - 1) // 4, (colour - 1) // 2 % 2, (colour - 1) % 2)
            if par[1] == before[1]:

                def body(r_in, s_in, lo, hi, yy, gm, p, r_ref, s_ref, c, fl, fh, fy, xs, par=par, before=before):
                    ghosts(bk, before, r_ref, s_ref, gm, lo, hi, yy)
                    solve(bk, par, r_ref, p, c, fl, fh, fy, xs)

                r, sol, c, fl, fh, fy = call(
                    body, [r, sol, *pending, couple, inverse], [state, state] + solve_outs,
                    aliases={0: 0, 1: 1}, scratch=solve_scratch, flops=flops,
                )
            else:
                r, sol = move_region(bk, before, par, r, sol, pending, couple, msg, state)

                def body(r_in, p, r_ref, c, fl, fh, fy, xs, par=par):
                    solve(bk, par, r_ref, p, c, fl, fh, fy, xs)

                r, c, fl, fh, fy = call(
                    body, [r, inverse], [state] + solve_outs,
                    aliases={0: 0}, scratch=solve_scratch, flops=flops,
                )
        pending = exchange(fl, fh, fy, bk)
        if colour == 0:
            r, sol = call(
                own_change(bk, par, True), [r, c, weights], [state, state],
                aliases={0: 0}, scratch=[coarse, coarse], flops=flops,
            )
        else:
            r, sol = call(
                own_change(bk, par, False), [r, sol, c, weights], [state, state],
                aliases={0: 0, 1: 1}, scratch=[coarse, coarse], flops=flops,
            )
    whole = (right_side.shape, F32)
    (solution_out,) = call(leave(bk, None), [sol], [whole], hbm_out=True, flops=flops)

    def last(r_in, lo, hi, yy, gm, r_ref):
        ghosts(bk, (1, 1, 1), r_ref, None, gm, lo, hi, yy)

    (r,) = call(last, [r, *pending, couple], [state], aliases={0: 0})
    (residual_out,) = call(leave(bk, None), [r], [whole], hbm_out=True)
    return solution_out, residual_out


def exchange(fl, fh, fy, bk):
    below, above = shift(fh, "gx", 1), shift(fl, "gx", -1)
    if lax.axis_size("gy") == 2:
        ys = shift(fy, "gy", 1)
    else:
        n = bk.faces_y
        ys = jnp.concatenate([shift(fy[:n], "gy", -1), shift(fy[n:], "gy", 1)])
    return below, above, ys


def move_region(bk, before, par, r, sol, pending, couple, msg, state):
    to_home_y = before[1] == 0
    to_home_x = before[0] == 0 and par[0] == 1
    with_sol = before == (0, 0, 1)
    x_send = bk.face_x(-1, 1)
    x_home = bk.face_x(bk.ex - 1, 1)
    a = par[0]
    y_cells = bk.face_y(-1, a)
    sol_cells = [bk.tile(bk.ex - 1, bk.ey - 1, pz) for pz in range(2)]
    n_y = len(y_cells) + (2 if with_sol else 0)

    def finish(r_in, s_in, lo, hi, yy, gm, r_ref, s_ref, m_ref):
        ghosts(bk, before, r_ref, s_ref, gm, lo, hi, yy)
        if to_home_x:
            for m, t in enumerate(x_send):
                m_ref[m] = r_ref[t].astype(BF16)
        else:
            for m, t in enumerate(y_cells):
                m_ref[m] = r_ref[t].astype(BF16)
            if with_sol:
                for m, t in enumerate(sol_cells):
                    m_ref[len(y_cells) + m] = s_ref[t].astype(BF16)

    n_first = len(x_send) if to_home_x else n_y
    r, sol, m = call(
        finish, [r, sol, *pending, couple], [state, state, msg(n_first)], aliases={0: 0, 1: 1}
    )
    if to_home_x:
        m = shift(m, "gx", -1)

        def turn(r_in, m_in, r_ref, y_ref):
            for i, t in enumerate(x_home):
                r_ref[t] = m_in[i].astype(F32)
            for i, t in enumerate(y_cells):
                y_ref[i] = r_ref[t].astype(BF16)

        r, m = call(turn, [r, m], [state, msg(n_y)], aliases={0: 0})
    m = shift(m, "gy", -1 if to_home_y else 1)

    def place(r_in, s_in, m_in, r_ref, s_ref):
        for i, t in enumerate(y_cells):
            r_ref[t] = m_in[i].astype(F32)
        if with_sol:
            for i, t in enumerate(sol_cells):
                s_ref[t] = m_in[len(y_cells) + i].astype(F32)

    r, sol = call(place, [r, sol, m], [state, state], aliases={0: 0, 1: 1})
    return r, sol


def solution(mesh):
    placed = (P(None, "gx", "gy", "gz"), P("gx", "gy", "gz"), P(), P(), P())
    return jax.shard_map(
        on_device,
        mesh=mesh,
        in_specs=placed,
        out_specs=(P(None, "gx", "gy", "gz"), P(None, "gx", "gy", "gz")),
        check_vma=False,
    )
```

```python
import jax
import jax.numpy as jnp
from jax import lax
from jax.experimental import pallas as pl
from jax.experimental.pallas import tpu as pltpu
from jax.sharding import PartitionSpec as P

F32 = jnp.float32
BF16 = jnp.bfloat16
LANES = 128
VMEM_LIMIT = 28 * 1024 * 1024


class Block:
    def __init__(self, dofs, extent_x, extent_y, extent_z, rhs):
        assert extent_x % 2 == 0 and extent_y % 4 == 0 and extent_z * rhs == LANES
        self.q, self.ex, self.ey, self.ez, self.rhs = dofs, extent_x, extent_y, extent_z, rhs
        self.rows = -(-(dofs + 2) // 16) * 16
        self.sent = -(-(dofs + 2) // 8) * 8
        self.nx, self.ny = extent_x // 2, extent_y // 2
        self.tiles = extent_x * extent_y * 2
        self.own = LANES // 4
        self.half = LANES // 2
        self.faces_x = 2 * extent_y
        self.faces_y = 2 * extent_x

    def tile(self, x, y, pz):
        px, py = x % 2, y % 2
        sx, sy = (x // 2) % self.nx, (y // 2) % self.ny
        return (((px * 2 + py) * 2 + pz) * self.nx + sx) * self.ny + sy

    def span(self, parity, extent):
        return range(parity - 1, parity - 1 + extent)

    def face_x(self, x, b):
        return [self.tile(x, y, pz) for y in self.span(b, self.ey) for pz in range(2)]

    def face_y(self, y, a):
        return [self.tile(x, y, pz) for x in self.span(a, self.ex) for pz in range(2)]


def lane_iota(rows):
    return lax.broadcasted_iota(jnp.int32, (rows, LANES), 1)


def in_steps(count, page, each=4):
    def step(i, carry):
        for n in range(each):
            page(i * each + n)
        return carry

    lax.fori_loop(0, count // each, step, 0)


def weight(inside, rows):
    return jnp.broadcast_to(jnp.where(inside, 1.0, 0.0).astype(BF16), (rows, LANES))


def roll(v, by):
    by = by % LANES
    return pltpu.roll(v, by, 1) if by else v


def turned(v, by):
    return roll(v, by) if isinstance(by, int) else pltpu.roll(v, (by + LANES) % LANES, 1)


def dot(a, b):
    return jnp.dot(a, b, preferred_element_type=F32)


def call(body, ins, outs, aliases=None, scratch=(), flops=0, hbm_out=False, far_in=0, copies=0, vmem=VMEM_LIMIT):
    space = pl.BlockSpec(memory_space=pltpu.VMEM)
    far = pl.BlockSpec(memory_space=pltpu.HBM)
    if hbm_out:
        shapes = [jax.ShapeDtypeStruct(s, d) for s, d in outs]
    else:
        shapes = [pltpu.VMEM(s, d) for s, d in outs]
    return pl.pallas_call(
        body,
        in_specs=[far] * far_in + [space] * (len(ins) - far_in),
        out_specs=[far if hbm_out and copies else space] * len(outs),
        out_shape=shapes,
        scratch_shapes=[pltpu.VMEM(s, d) for s, d in scratch]
        + ([pltpu.SemaphoreType.DMA((copies,))] if copies else []),
        input_output_aliases=aliases or {},
        compiler_params=pltpu.CompilerParams(vmem_limit_bytes=vmem),
        cost_estimate=pl.CostEstimate(flops=flops, bytes_accessed=0, transcendentals=0) if flops else None,
    )(*ins)


def coef_row(bk, r_ref, t):
    return r_ref[t, bk.q : bk.q + 1, :] + r_ref[t, bk.q + 1 : bk.q + 2, :]


def shift(v, axis, distance):
    n = lax.axis_size(axis)
    return lax.ppermute(v, axis, [((i - distance) % n, i) for i in range(n)])


def shift2(v, first, d1, second, d2):
    n1, n2 = lax.axis_size(first), lax.axis_size(second)
    route = [
        (((i - d1) % n1) * n2 + (j - d2) % n2, i * n2 + j) for i in range(n1) for j in range(n2)
    ]
    return lax.ppermute(v, (first, second), route)


def pack(bk, r_ref, tiles, lanes_from, count, out_ref, parts):
    lane = lane_iota(bk.rows)
    for n in range(0, len(tiles), parts):
        total = None
        for k, t in enumerate(tiles[n : n + parts]):
            moved = roll(r_ref[t], k * count - lanes_from)
            total = moved if total is None else jnp.where(lane < k * count, total, moved)
        out_ref[n // parts] = total.astype(BF16)


def unpack(bk, msg_ref, n, lanes_to, count, parts):
    k = n % parts
    return roll(msg_ref[n // parts].astype(F32), lanes_to - k * count)


def prep_tables(bk):
    q, rows = bk.q, bk.rows

    def body(p_ref, m_ref, f_ref, o_ref, w_ref, g_ref, pick_ref):
        n = p_ref.shape[0]
        row = lax.broadcasted_iota(jnp.int32, (rows, n), 0)
        col = lax.broadcasted_iota(jnp.int32, (rows, n), 1)

        def build(o, carry):
            pick = jnp.where((col == row * 8 + o) & (row < q), 1.0, 0.0).astype(BF16)
            pick_ref[pl.ds(o * rows, rows), :] = pick
            return carry

        lax.fori_loop(0, 8, build, 0)

        def move(o, carry):
            at = pl.ds(o * rows, rows)
            left = dot(pick_ref[at, :], p_ref[...]).astype(BF16)
            o_ref[at, :] = lax.dot_general(
                left, pick_ref[...], (((1,), (1,)), ((), ())), preferred_element_type=F32
            ).astype(BF16)
            return carry

        lax.fori_loop(0, 8, move, 0)
        row = lax.broadcasted_iota(jnp.int32, (q, 7 * rows), 0)
        col = lax.broadcasted_iota(jnp.int32, (q, 7 * rows), 1)
        total = dot(m_ref[...].astype(BF16), jnp.where(col == row, 1.0, 0.0).astype(BF16))
        g_ref[...] = jnp.zeros_like(g_ref)
        w_ref[...] = jnp.zeros_like(w_ref)
        one = jnp.where(
            lax.broadcasted_iota(jnp.int32, (q, rows), 0) == lax.broadcasted_iota(jnp.int32, (q, rows), 1),
            1.0, 0.0,
        ).astype(BF16)
        for direction in range(3):
            face = f_ref[direction].astype(BF16)
            for side in range(2):
                at = rows * (1 + 2 * direction + side)
                place = jnp.where(col == row + at, 1.0, 0.0).astype(BF16)
                dims = (((1 - side,), (0,)), ((), ()))
                total = total - lax.dot_general(face, place, dims, preferred_element_type=F32)
                if direction < 2:
                    g_ref[2 * direction + side, :q, :] = lax.dot_general(
                        face, one, dims, preferred_element_type=F32
                    ).astype(BF16)
        w_ref[:q, :] = total.astype(BF16)

    return body


def prep_state(bk):
    def body(rs_ref, cc_ref, r_ref, y_ref, scr):
        rows = rs_ref.reshape(bk.q * bk.ex * bk.ey, LANES)
        src = lax.broadcasted_iota(jnp.int32, (2 * LANES, 2 * LANES), 0) % LANES
        dst = lax.broadcasted_iota(jnp.int32, (2 * LANES, 2 * LANES), 1)
        pz, lane = dst // LANES, dst % LANES - bk.own
        z = 2 * (lane // bk.rhs) + pz
        inside = (lane >= 0) & (lane < bk.half)
        split = jnp.where(inside & (src == z * bk.rhs + lane % bk.rhs), 1.0, 0.0).astype(BF16)
        zz = lax.broadcasted_iota(jnp.int32, (bk.ez, LANES), 0)
        ll = lax.broadcasted_iota(jnp.int32, (bk.ez, LANES), 1)
        spread = jnp.where(ll // bk.rhs == zz, 1.0, 0.0).astype(BF16)
        coef = cc_ref[...]
        high = coef.astype(BF16)
        low = (coef - high.astype(F32)).astype(BF16)
        high, low = dot(high, spread), dot(low, spread)
        scr[...] = jnp.zeros_like(scr)
        for x in range(bk.ex):
            for y in range(bk.ey):
                n = x * bk.ey + y
                scr[n % 4, : bk.q, :] = rows[pl.ds(n, bk.q, stride=bk.ex * bk.ey), :]
                scr[n % 4, bk.q : bk.q + 1, :] = high[n : n + 1]
                scr[n % 4, bk.q + 1 : bk.q + 2, :] = low[n : n + 1]
                raw = scr[n % 4]
                top = raw.astype(BF16)
                rest = (raw - top.astype(F32)).astype(BF16)
                out = dot(jnp.concatenate([top, rest], axis=1), split)
                r_ref[bk.tile(x, y, 0)] = out[:, :LANES]
                r_ref[bk.tile(x, y, 1)] = out[:, LANES:]
        tiles = [bk.tile(x, bk.ey - 1, pz) for x in range(bk.ex) for pz in range(2)]
        pack(bk, r_ref, tiles, bk.own, bk.half, y_ref, 2)

    return body


def halo_cells(bk):
    return [
        bk.tile(x, y, pz)
        for x in range(bk.ex - 1)
        for y in bk.span(0, bk.ey)
        for pz in range(2)
    ]


def prep_halo(bk):
    def body(r_in, y_ref, r_ref, zl_ref, zh_ref, x_ref, xl_ref, xh_ref):
        n = 0
        for x in range(bk.ex):
            for pz in range(2):
                r_ref[bk.tile(x, -1, pz)] = unpack(bk, y_ref, n, bk.own, bk.half, 2)
                n += 1
        cells = halo_cells(bk)
        pack(bk, r_ref, cells, bk.own, bk.own, zl_ref, 4)
        pack(bk, r_ref, cells, 2 * bk.own, bk.own, zh_ref, 4)
        edge = bk.face_x(bk.ex - 1, 0)
        pack(bk, r_ref, edge, bk.own, bk.half, x_ref, 2)
        pack(bk, r_ref, edge, bk.own, bk.own, xl_ref, 4)
        pack(bk, r_ref, edge, 2 * bk.own, bk.own, xh_ref, 4)

    return body


def fill_halo(bk, r_ref, zl_ref, zh_ref, x_ref, xl_ref, xh_ref):
    lane = lane_iota(bk.rows)
    below, above = lane < bk.own, lane >= 3 * bk.own

    def joined(own, low_ref, high_ref, n):
        low = unpack(bk, low_ref, n, 0, bk.own, 4)
        high = unpack(bk, high_ref, n, 3 * bk.own, bk.own, 4)
        return jnp.where(below, low, jnp.where(above, high, own))

    for n, t in enumerate(halo_cells(bk)):
        r_ref[t] = joined(r_ref[t], zl_ref, zh_ref, n)
    for n, t in enumerate(bk.face_x(-1, 0)):
        r_ref[t] = joined(unpack(bk, x_ref, n, bk.own, bk.half, 2), xl_ref, xh_ref, n)


def solve(bk, colour, r_ref, p_ref, c_ref, xl_ref, xh_ref, y_ref, xs_ref):
    a, b, g = colour
    back = bk.rhs
    n = 0
    for px in range(bk.nx):
        for py in range(0, bk.ny, 2):
            cells = []
            for half in range(2):
                for o in range(8):
                    x = a - 1 + 2 * px + o // 4
                    y = b - 1 + 2 * (py + half) + o // 2 % 2
                    pz = o % 2 if g else 1 - o % 2
                    t = bk.tile(x, y, pz)
                    scale = lax.rsqrt(coef_row(bk, r_ref, t))
                    scaled = r_ref[t] * scale
                    if g == 0 and pz == 1:
                        scaled = roll(scaled, back)
                    lanes = slice(half * LANES, (half + 1) * LANES)
                    xs_ref[n, o * bk.rows : (o + 1) * bk.rows, lanes] = scaled.astype(BF16)
                    cells.append((half, o, t, scale, g == 0 and pz == 1))
            solved = dot(p_ref[...], xs_ref[n])
            for half, o, t, scale, moved in cells:
                v = solved[o * bk.rows : (o + 1) * bk.rows, half * LANES : (half + 1) * LANES]
                if moved:
                    v = roll(v, -back)
                c_ref[t] = (v * scale).astype(BF16)
            n += 1
    for m, t in enumerate(bk.face_x(a - 1, b)):
        xl_ref[m] = c_ref[t]
    for m, t in enumerate(bk.face_x(a - 2 + bk.ex, b)):
        xh_ref[m] = c_ref[t]
    for m, t in enumerate(bk.face_y(b - 1, a) + bk.face_y(b - 2 + bk.ey, a)):
        y_ref[m] = c_ref[t]


def ghosts(bk, colour, r_ref, sol_ref, g_ref, from_below, from_above, y_ref):
    a, b, g = colour

    def add(matrix, tiles, ghost_ref, base):
        for m in range(0, len(tiles), 2):
            two = jnp.concatenate([ghost_ref[base + m], ghost_ref[base + m + 1]], axis=1)
            change = dot(g_ref[matrix], two)
            r_ref[tiles[m]] += change[:, :LANES]
            r_ref[tiles[m + 1]] += change[:, LANES:]

    add(0, bk.face_x(a - 2 + bk.ex, b), from_above, 0)
    add(1, bk.face_x(a - 1, b), from_below, 0)
    add(2, bk.face_y(b - 2 + bk.ey, a), y_ref, 0)
    add(3, bk.face_y(b - 1, a), y_ref, bk.faces_y)
    if a == 0:
        for m, t in enumerate(bk.face_x(bk.ex - 1, b)):
            sol_ref[t] += from_above[m].astype(F32)
    if b == 0:
        m = 0
        for x in bk.span(a, bk.ex):
            for pz in range(2):
                if x >= 0:
                    sol_ref[bk.tile(x, bk.ey - 1, pz)] += y_ref[m].astype(F32)
                m += 1


def own_change(bk, colour, first):
    a, b, g = colour

    def body(*refs):
        if first:
            r_in, c_ref, w_ref, r_ref, sol_ref, cm_ref, cz_ref = refs
        else:
            r_in, sol_in, c_ref, w_ref, r_ref, sol_ref, cm_ref, cz_ref = refs
        xs, ys = bk.span(a, bk.ex), bk.span(b, bk.ey)
        for x in xs:
            for y in ys:
                for pz in range(2):
                    t = bk.tile(x, y, pz)
                    c = c_ref[t].astype(F32)
                    cm_ref[t] = (c * coef_row(bk, r_ref, t)).astype(BF16)
                    cz_ref[t] = roll(c_ref[t], bk.rhs if pz else -bk.rhs)
                    if x >= 0 and y >= 0:
                        sol_ref[t] = c if first else sol_ref[t] + c
                    elif first:
                        sol_ref[t] = jnp.zeros_like(c)
        nothing = jnp.zeros((bk.rows, LANES), BF16)

        def at(x, y, pz):
            return c_ref[bk.tile(x, y, pz)] if x in xs and y in ys else nothing

        def stack(x, y, pz):
            other = bk.tile(x, y, 1 - pz)
            near, far = c_ref[other], cz_ref[other]
            return jnp.concatenate(
                [
                    cm_ref[bk.tile(x, y, pz)],
                    at(x + 1, y, pz),
                    at(x - 1, y, pz),
                    at(x, y + 1, pz),
                    at(x, y - 1, pz),
                    far if pz else near,
                    near if pz else far,
                ],
                axis=0,
            )

        for x in xs:
            for y in ys:
                both = jnp.concatenate([stack(x, y, 0), stack(x, y, 1)], axis=1)
                change = dot(w_ref[...], both)
                for pz in range(2):
                    r_ref[bk.tile(x, y, pz)] -= change[:, pz * LANES : (pz + 1) * LANES]

    return body


def leave(bk, ref):
    def body(tile_ref, out_ref):
        rows = out_ref.reshape(bk.q * bk.ex * bk.ey, LANES)
        src = lax.broadcasted_iota(jnp.int32, (2 * LANES, LANES), 0)
        dst = lax.broadcasted_iota(jnp.int32, (2 * LANES, LANES), 1)
        pz, lane = src // LANES, src % LANES - bk.own
        z = 2 * (lane // bk.rhs) + pz
        inside = (lane >= 0) & (lane < bk.half)
        join = jnp.where(inside & (dst == z * bk.rhs + lane % bk.rhs), 1.0, 0.0).astype(BF16)
        for x in range(bk.ex):
            for y in range(bk.ey):
                both = jnp.concatenate(
                    [tile_ref[bk.tile(x, y, 0)], tile_ref[bk.tile(x, y, 1)]], axis=1
                )
                top = both.astype(BF16)
                rest = (both - top.astype(F32)).astype(BF16)
                out = dot(top, join) + dot(rest, join)
                rows[pl.ds(x * bk.ey + y, bk.q, stride=bk.ex * bk.ey), :] = out[: bk.q]

    return body


class Slab:
    def __init__(self, bk, count):
        self.bk, self.count = bk, count
        self.q, self.rhs, self.rows, self.ny = bk.q, bk.rhs, bk.rows, bk.ny
        self.sent = bk.sent
        self.ey = bk.ey
        self.groups = count
        self.width = LANES // count
        self.depth = bk.ez // count
        self.halo = 2 * bk.rhs
        self.tiles = bk.tiles

    @staticmethod
    def fits(bk, count):
        depth = bk.ez // count
        return (
            bk.ez % count == 0
            and depth % 2 == 0
            and bk.nx == 2
            and (depth // 2 + 4) * bk.rhs * count == LANES
            and bk.tiles % 16 == 0
        )

    def tile(self, px, x2, y, pz):
        return (((px * 2 + y % 2) * 2 + pz) * 2 + x2) * self.ny + (y // 2) % self.ny

    def face_y(self, y):
        return [self.tile(px, x2, y, pz) for px in range(2) for x2 in range(2) for pz in range(2)]

    def edge(self, n, low_side):
        pz = n // (2 * self.ny) % 2
        index = n // (4 * self.ny) * (2 * self.ny // self.groups) + n % (2 * self.ny) // self.groups
        pairs = (2 if pz else 3) if low_side else (2 if pz else 1)
        each = {1: 8, 2: 4, 3: 2}[pairs]
        base = 0 if pz else self.tiles // (2 * self.groups) // 4
        return base + index // each, index % each * (self.width // each), pairs * self.rhs

    def pages(self, low_side):
        return 1 + max(self.edge(n, low_side)[0] for n in range(0, self.tiles, self.groups))

    def place(self, device):
        slab = device * 0
        for s, d in enumerate(self.order()):
            slab = jnp.where(device == d, s, slab)
        return slab

    def order(self):
        return [0, 1, 3, 2] if self.count == 4 else list(range(self.count))


def home_prep(bk, sb):
    def body(rs_ref, cc_ref, h_ref, up_ref, down_ref, scr, high_ref, low_ref, in_ref, cin_ref, sems):
        copies = [
            pltpu.make_async_copy(rs_ref.at[:, x], in_ref.at[x], sems.at[x]) for x in range(bk.ex)
        ]
        coefs = pltpu.make_async_copy(cc_ref, cin_ref, sems.at[bk.ex])
        coefs.start()
        for c in copies:
            c.start()
        src = lax.broadcasted_iota(jnp.int32, (LANES, 2 * LANES), 0)
        dst = lax.broadcasted_iota(jnp.int32, (LANES, 2 * LANES), 1)
        pz, lane = dst // LANES, dst % LANES - bk.own
        z = 2 * (lane // bk.rhs) + pz
        inside = (lane >= 0) & (lane < bk.half)
        split = jnp.where(inside & (src == z * bk.rhs + lane % bk.rhs), 1.0, 0.0).astype(BF16)
        zz = lax.broadcasted_iota(jnp.int32, (bk.ez, LANES), 0)
        ll = lax.broadcasted_iota(jnp.int32, (bk.ez, LANES), 1)
        spread = jnp.where(ll // bk.rhs == zz, 1.0, 0.0).astype(BF16)
        coefs.wait()
        coef = cin_ref[...]
        high = coef.astype(BF16)
        low = (coef - high.astype(F32)).astype(BF16)
        high_ref[...], low_ref[...] = dot(high, spread), dot(low, spread)
        scr[...] = jnp.zeros_like(scr)

        for x in range(bk.ex):
            copies[x].wait()
            rows = in_ref.at[x].reshape(bk.q * bk.ey, LANES)

            def column(half, carry, x=x, rows=rows):
                for i in range(bk.ey // 2):
                    y = half + 2 * i
                    n = x * bk.ey + y
                    scr[i, : bk.q, :] = rows[pl.ds(y, bk.q, stride=bk.ey), :]
                    scr[i, bk.q : bk.q + 1, :] = high_ref[pl.ds(n, 1), :]
                    scr[i, bk.q + 1 : bk.q + 2, :] = low_ref[pl.ds(n, 1), :]
                    out = dot(scr[i].astype(BF16), split)
                    h_ref[bk.tile(x, y, 0)] = out[:, :LANES].astype(BF16)
                    h_ref[bk.tile(x, y, 1)] = out[:, LANES:].astype(BF16)
                return carry

            for half in range(2):
                column(half, 0)
        lane = lane_iota(1)
        for ref, low_side in ((up_ref, False), (down_ref, True)):
            for n in range(0, bk.tiles, sb.groups):
                page, slot, width = sb.edge(n, low_side)
                start = bk.own if low_side else bk.own + bk.half - width
                total = ref[page] if slot else None
                for k in range(sb.groups):
                    at = k * sb.width + slot
                    inside = weight((lane >= at) & (lane < at + width), sb.sent)
                    v = roll(h_ref[n + k, : sb.sent], at - start) * inside
                    total = v if total is None else total + v
                ref[page] = total

    return body


def scatter(sb):
    bk, parts, rows = sb.bk, sb.groups, sb.sent

    def body(h_ref, below_ref, above_ref, *outs):
        lane = lane_iota(1)
        me = lax.axis_index("gx")
        step = bk.half // parts
        keep, slabs = [], []
        for d in range(parts):
            slab = sb.place((me + d) % parts)
            slabs.append(slab)
            group = (lane - slab * step + LANES) % LANES // sb.width
            keep.append([weight(group == (me + k) % parts, rows) for k in range(parts)])
        ends = {}
        for pz in range(2):
            for low_side in range(2):
                pairs = sb.edge(0 if not pz else 2 * sb.ny, not low_side)[2]
                if low_side:
                    inside, end = lane % sb.width < pairs, 0
                else:
                    at = (lane - step * (parts - 1) + LANES) % LANES
                    inside, end = at % sb.width >= sb.width - pairs, parts - 1
                for d in range(parts):
                    chosen = jnp.where(inside, jnp.where(slabs[d] == end, 1, 0), 0)
                    ends[pz, low_side, d] = weight(chosen == 1, rows)
        for n in range(0, sb.tiles, parts):
            totals = [None] * parts
            pz = n // (2 * sb.ny) % 2
            for k in range(parts):
                start = bk.own - (2 if pz else 1) * bk.rhs
                by = ((me + k) % parts * sb.width - start + LANES) % LANES
                v = pltpu.roll(h_ref[n + k, :rows], by, 1)
                for d in range(parts):
                    totals[d] = v * keep[d][k] if k == 0 else totals[d] + v * keep[d][k]
            page, slot, width = sb.edge(n, False)
            low = pltpu.roll(below_ref[page], (me * sb.width - slot + LANES) % LANES, 1)
            page, slot, width = sb.edge(n, True)
            by = me * sb.width + step * (parts - 1) + sb.width - width - slot
            high = pltpu.roll(above_ref[page], (by + LANES) % LANES, 1)
            for d, out in enumerate(outs):
                out[n // parts] = totals[d] + low * ends[pz, 1, d] + high * ends[pz, 0, d]

    return body


def gather_state(sb, parts_refs, r_ref):
    parts, rows = sb.groups, sb.sent
    me = lax.axis_index("gx")
    by = sb.place(me) * (sb.bk.half // parts)
    group = (lane_iota(1) - by + LANES) % LANES // sb.width
    keep = [
        [weight(group == (me - d + parts + k) % parts, rows) for d in range(parts)]
        for k in range(parts)
    ]

    def page(n):
        for k in range(parts):
            total = parts_refs[0][n] * keep[k][0]
            for d in range(1, parts):
                total = total + parts_refs[d][n] * keep[k][d]
            total = pltpu.roll(total, (2 * LANES - k * sb.width - by) % LANES, 1)
            r_ref[n * parts + k, :rows] = total.astype(F32)
            r_ref[n * parts + k, rows:] = jnp.zeros((sb.rows - rows, LANES), F32)

    in_steps(sb.tiles // parts, page)


def slab_solve(sb, colour, r_ref, p_ref, c_ref, y_ref, xs_ref):
    a, b, g = colour
    rows = sb.rows

    def column(x2, carry):
        for n, py in enumerate(range(0, sb.ny, 2)):
            cells = []
            for half in range(2):
                for o in range(8):
                    xo, y = o // 4, b - 1 + 2 * (py + half) + o // 2 % 2
                    pz = o % 2 if g else 1 - o % 2
                    moved = -sb.rhs if g == 1 and pz == 1 else 0
                    if a or xo == 1:
                        t = sb.tile(xo if a else 0, x2, y, pz)
                    else:
                        t = sb.tile(1, 1 - x2, y, pz)
                        moved = moved + (1 - x2) * sb.width
                    scale = lax.rsqrt(coef_row(sb, r_ref, t))
                    lanes = slice(half * LANES, (half + 1) * LANES)
                    xs_ref[n, o * rows : (o + 1) * rows, lanes] = turned(
                        r_ref[t] * scale, moved
                    ).astype(BF16)
                    cells.append((half, o, t, scale, moved))
            solved = dot(p_ref[...], xs_ref[n])
            for half, o, t, scale, moved in cells:
                v = solved[o * rows : (o + 1) * rows, half * LANES : (half + 1) * LANES]
                c_ref[t] = (turned(v, -moved) * scale).astype(BF16)
        return carry

    lax.fori_loop(0, 2, column, 0)
    for m, t in enumerate(sb.face_y(b - 1) + sb.face_y(b - 2 + sb.ey)):
        y_ref[m] = c_ref[t]


def slab_ghosts(sb, colour, r_ref, sol_ref, g_ref, y_ref):
    a, b, g = colour
    count = len(sb.face_y(0))
    for matrix, y, base in ((2, b - 2 + sb.ey, 0), (3, b - 1, count)):
        tiles = sb.face_y(y)
        for m in range(0, count, 2):
            two = jnp.concatenate([y_ref[base + m], y_ref[base + m + 1]], axis=1)
            change = dot(g_ref[matrix], two)
            r_ref[tiles[m]] += change[:, :LANES]
            r_ref[tiles[m + 1]] += change[:, LANES:]
    if b == 0:
        for m, t in enumerate(sb.face_y(sb.ey - 1)):
            sol_ref[t] += y_ref[m].astype(F32)


def slab_change(sb, colour, first, last=False):
    a, b, g = colour

    def body(*refs):
        if last:
            r_in, c_ref, w_ref, r_ref, cm_ref, cz_ref, cx_ref = refs
        elif first:
            r_in, c_ref, w_ref, r_ref, sol_ref, cm_ref, cz_ref, cx_ref = refs
        else:
            r_in, sol_in, c_ref, w_ref, r_ref, sol_ref, cm_ref, cz_ref, cx_ref = refs
        ys = sb.bk.span(b, sb.ey)
        cells = [(px, x2, y) for px in range(2) for x2 in range(2) for y in ys]
        for px, x2, y in cells:
            for pz in range(2):
                t = sb.tile(px, x2, y, pz)
                c = c_ref[t].astype(F32)
                cm_ref[t] = (c * coef_row(sb, r_ref, t)).astype(BF16)
                cz_ref[t] = roll(c_ref[t], -sb.rhs if pz else sb.rhs)
                if px == x2:
                    cx_ref[t] = roll(c_ref[t], sb.width if px else -sb.width)
                if last:
                    continue
                if y >= 0:
                    sol_ref[t] = c if first else sol_ref[t] + c
                elif first:
                    sol_ref[t] = jnp.zeros_like(c)
        nothing = jnp.zeros((sb.rows, LANES), BF16)

        def stack(px, x2, y, pz):
            beside = c_ref[sb.tile(1 - px, x2, y, pz)]
            across = (cx_ref if px == x2 else c_ref)[sb.tile(1 - px, 1 - x2, y, pz)]
            other = sb.tile(px, x2, y, 1 - pz)
            near, far = c_ref[other], cz_ref[other]
            return jnp.concatenate(
                [
                    cm_ref[sb.tile(px, x2, y, pz)],
                    across if px else beside,
                    beside if px else across,
                    c_ref[sb.tile(px, x2, y + 1, pz)] if y + 1 in ys else nothing,
                    c_ref[sb.tile(px, x2, y - 1, pz)] if y - 1 in ys else nothing,
                    near if pz else far,
                    far if pz else near,
                ],
                axis=0,
            )

        for px, x2, y in cells:
            both = jnp.concatenate([stack(px, x2, y, 0), stack(px, x2, y, 1)], axis=1)
            change = dot(w_ref[...], both)
            for pz in range(2):
                r_ref[sb.tile(px, x2, y, pz)] -= change[:, pz * LANES : (pz + 1) * LANES]

    return body


def emit_halo(sb, r_ref, up_ref, down_ref):
    rows = sb.sent
    lane = lane_iota(rows) % sb.width
    top = sb.width - 2 * sb.halo
    parts = sb.width // sb.halo

    def page(n):
        for ref, start in ((up_ref, top), (down_ref, sb.halo)):
            total = None
            for k in range(parts):
                moved = roll(r_ref[n * parts + k, :rows], k * sb.halo - start)
                total = moved if k == 0 else jnp.where(lane < k * sb.halo, total, moved)
            ref[n] = total.astype(BF16)

    in_steps(sb.tiles // parts, page)


def fill_slab_halo(sb, r_ref, below_ref, above_ref):
    rows = sb.sent
    lane = lane_iota(rows) % sb.width
    parts = sb.width // sb.halo

    def page(n):
        for k in range(parts):
            t = n * parts + k
            low = roll(below_ref[n].astype(F32), -k * sb.halo)
            high = roll(above_ref[n].astype(F32), sb.width - sb.halo - k * sb.halo)
            own = jnp.where(lane < sb.halo, low, r_ref[t, :rows])
            r_ref[t, :rows] = jnp.where(lane >= sb.width - sb.halo, high, own)

    in_steps(sb.tiles // parts, page)


def collect(sb, source, outs, extras, extra_at):
    width = sb.width - 2 * sb.halo
    parts = LANES // width
    rows = sb.sent
    lane = lane_iota(rows)
    piece = lane_iota(1) // width
    me = lax.axis_index("gx")
    slab = sb.place(me)
    offset = sb.bk.own // width
    keep = [
        [
            weight(piece == (offset + slab + k + 2 * ((me + d) % sb.groups)) % parts, rows)
            for k in range(parts)
        ]
        for d in range(len(outs))
    ]
    def page(n):
        totals = [None] * len(outs)
        for k in range(parts):
            by = (offset + slab + k) * width - sb.halo
            v = pltpu.roll(source[n * parts + k, :rows].astype(BF16), by % LANES, 1)
            for d in range(len(outs)):
                totals[d] = v * keep[d][k] if k == 0 else totals[d] + v * keep[d][k]
        for d, out in enumerate(outs):
            out[n] = totals[d]

    if outs:
        in_steps(sb.tiles // parts, page)
    per = sb.width // sb.rhs
    evens = even_tiles(sb)
    joined = []
    for m in range(sb.groups if extras else 0):
        total = None
        for k, t in enumerate(evens[m * per : (m + 1) * per]):
            v = roll(source[t, :rows].astype(BF16), k * sb.rhs - (sb.width - sb.halo - sb.rhs))
            total = v if k == 0 else jnp.where(lane % sb.width < k * sb.rhs, total, v)
        joined.append(roll(total, m * sb.width))
    for u, out in enumerate(extras):
        total = joined[0]
        for m in range(1, sb.groups):
            total = jnp.where(lane // sb.width == (u + m) % sb.groups, joined[m], total)
        out[extra_at] = total


def even_tiles(sb):
    return [t for t in range(sb.tiles) if t // (2 * sb.ny) % 2 == 0]


def deliver(sb):
    bk = sb.bk
    width = sb.width - 2 * sb.halo
    parts = LANES // width
    per = sb.width // sb.rhs

    def body(*refs):
        count = sb.groups
        both_ins = (refs[:count], refs[count : 2 * count])
        extras, outs = refs[2 * count : 3 * count], refs[3 * count : 3 * count + 2]
        buffer, sems = refs[3 * count + 2 :]
        rows_sent = sb.sent
        lane = lane_iota(1)
        piece = lane // width
        first = weight((lane >= bk.own) & (lane < bk.own + bk.rhs), rows_sent)
        later = 1 - first
        src = lax.broadcasted_iota(jnp.int32, (2 * LANES, LANES), 0)
        dst = lax.broadcasted_iota(jnp.int32, (2 * LANES, LANES), 1)
        pz, at = src // LANES, src % LANES - bk.own
        z = 2 * (at // bk.rhs) + pz
        inside = (at >= 0) & (at < bk.half)
        join = jnp.where(inside & (dst == z * bk.rhs + at % bk.rhs), 1.0, 0.0).astype(BF16)
        me = lax.axis_index("gx")
        slabs = [sb.place((me - d + sb.groups) % sb.groups) for d in range(sb.groups)]
        keep = [
            [weight(piece == (bk.own // width + s + k + 2 * me) % parts, rows_sent) for s in slabs]
            for k in range(parts)
        ]
        evens = even_tiles(sb)
        def copy_of(index, x):
            return pltpu.make_async_copy(
                buffer.at[index, x], outs[index].at[:, x], sems.at[index * bk.ex + x]
            )

        for index in range(2):
            ins = both_ins[index]
            layer = extras[0][index]
            for e in extras[1:]:
                layer = layer + e[index]

            def home(t, k, even, ins=ins, layer=layer):
                page = t // parts
                total = ins[0][page] * keep[k][0]
                for d in range(1, sb.groups):
                    total = total + ins[d][page] * keep[k][d]
                by = (3 * LANES - (k + 2 * me) * width + (bk.rhs if even else 0)) % LANES
                total = pltpu.roll(total, by, 1)
                if not even:
                    return total
                n = t // (2 * parts) * parts + k
                by = (bk.own + 3 * LANES - (me + n // per) * sb.width - n % per * sb.rhs) % LANES
                return first * pltpu.roll(layer, by, 1) + later * total

            def columns(px, carry, index=index, home=home):
                for sx in range(bk.nx):
                    x = 2 * sx + px
                    rows = buffer.at[index, x].reshape(bk.q * bk.ey, LANES)
                    for y in range(bk.ey):
                        t = bk.tile(x, y, 0)
                        k = sx * bk.ny + y // 2
                        both = jnp.concatenate(
                            [home(t, k, True), home(t + parts, k, False)], axis=1
                        )
                        out = dot(both, join)
                        rows[pl.ds(y, bk.q, stride=bk.ey), :] = out[: bk.q]
                return carry

            lax.fori_loop(0, 2, columns, 0)
            for x in range(bk.ex):
                copy_of(index, x).start()
        for index in range(2):
            for x in range(bk.ex):
                copy_of(index, x).wait()

    return body


def in_slabs(bk, sb, right_side, cell_coef, inverse, couple, weights):
    count, order = sb.count, sb.order()
    square = (sb.rows, LANES)
    state = ((sb.tiles,) + square, F32)
    coarse = ((sb.tiles,) + square, BF16)
    faces = ((2 * len(sb.face_y(0)),) + square, BF16)
    one_face = (((len(sb.face_y(0)),) + square), BF16)

    def msg(n):
        return ((n,) + square, BF16)

    def sent(n):
        return ((n, sb.sent, LANES), BF16)

    spread = ((bk.ex * bk.ey, LANES), F32)
    home, up, down = call(
        home_prep(bk, sb), [right_side, cell_coef.reshape(bk.ex * bk.ey, bk.ez)],
        [coarse, sent(sb.pages(False)), sent(sb.pages(True))],
        scratch=[
            ((bk.ey // 2,) + square, F32), spread, spread,
            ((bk.ex, bk.q, bk.ey, LANES), F32), ((bk.ex * bk.ey, bk.ez), F32),
        ],
        far_in=2, copies=bk.ex + 1, vmem=64_600_000,
    )
    below, above = shift(up, "gz", 1), shift(down, "gz", -1)
    pieces = call(scatter(sb), [home, below, above], [sent(sb.tiles // count)] * count)
    pieces = [shift(p, "gx", d) if d else p for d, p in enumerate(pieces)]

    def chain(v, step):
        n = lax.axis_size("gz")
        route = []
        for z in range(n):
            for s in range(count):
                total = (z * count + s + step) % (n * count)
                route.append((order[s] * n + z, order[total % count] * n + total // count))
        return lax.ppermute(v, ("gx", "gz"), route)

    def swap(v, step):
        return shift(v, "gy", step)

    edge = sb.face_y(-1)

    def assemble(*refs):
        r_ref, y_ref = refs[count + 1 :]
        gather_state(sb, refs[:count], r_ref)
        for m, t in enumerate(edge):
            y_ref[m] = r_ref[t].astype(BF16)

    r, moved = call(assemble, pieces + [inverse], [state, one_face])
    moved = swap(moved, 1)
    sol = halos = pending = None
    flops = 1 << 27
    solve_scratch = [((sb.ny // 2, 8 * sb.rows, 2 * LANES), BF16)]
    halo_msg = sent(sb.tiles * sb.halo // sb.width)
    refresh = (3,)

    for colour in range(8):
        par = (colour // 4, colour // 2 % 2, colour % 2)
        before = ((colour - 1) // 4, (colour - 1) // 2 % 2, (colour - 1) % 2)
        fresh = (colour - 1) in refresh
        turn = colour > 0 and par[1] != before[1]
        if turn or fresh:

            def finish(r_in, s_in, yy, gm, r_ref, s_ref, *outs, before=before, turn=turn):
                slab_ghosts(sb, before, r_ref, s_ref, gm, yy)
                if turn:
                    for m, t in enumerate(edge):
                        outs[0][m] = r_ref[t].astype(BF16)
                else:
                    emit_halo(sb, r_ref, *outs)

            outs = [one_face] if turn else [halo_msg, halo_msg]
            r, sol, *out = call(
                finish, [r, sol, pending, couple], [state, state] + outs, aliases={0: 0, 1: 1}
            )
            if turn:
                moved = swap(out[0], -1 if before[1] == 0 else 1)
            if turn and fresh:

                def turned(r_in, m_in, r_ref, u_ref, d_ref):
                    for m, t in enumerate(edge):
                        r_ref[t] = m_in[m].astype(F32)
                    emit_halo(sb, r_ref, u_ref, d_ref)

                r, *out = call(turned, [r, moved], [state, halo_msg, halo_msg], aliases={0: 0})
            if fresh:
                halos = (chain(out[0], 1), chain(out[1], -1))

                def solve_fresh(r_in, lo, hi, p, r_ref, c, fy, xs, par=par):
                    fill_slab_halo(sb, r_ref, lo, hi)
                    slab_solve(sb, par, r_ref, p, c, fy, xs)

                args = [r, *halos, inverse]
                body = solve_fresh
            else:
                args = [r, moved, inverse]
                body = None
        elif colour == 0:
            args, body = [r, moved, inverse], None
        else:

            def solve_next(r_in, s_in, yy, gm, p, r_ref, s_ref, c, fy, xs, par=par, before=before):
                slab_ghosts(sb, before, r_ref, s_ref, gm, yy)
                slab_solve(sb, par, r_ref, p, c, fy, xs)

            args, body = [r, sol, pending, couple, inverse], solve_next
        if body is None:

            def body(r_in, m_in, p, r_ref, c, fy, xs, par=par):
                for m, t in enumerate(edge):
                    r_ref[t] = m_in[m].astype(F32)
                slab_solve(sb, par, r_ref, p, c, fy, xs)

        with_sol = len(args) == 5
        kept = [state, state] if with_sol else [state]
        got = call(
            body, args, kept + [coarse, faces], scratch=solve_scratch, flops=flops,
            aliases={0: 0, 1: 1} if with_sol else {0: 0},
        )
        if with_sol:
            r, sol, c, fy = got
        else:
            r, c, fy = got
        if lax.axis_size("gy") == 2:
            pending = swap(fy, 1)
        else:
            n = len(edge)
            pending = jnp.concatenate([swap(fy[:n], -1), swap(fy[n:], 1)])
        if colour == 7:

            def finished(s_in, c_ref, s_ref, *outs):

                def page(t):
                    s_ref[t] += c_ref[t].astype(F32)

                in_steps(sb.tiles, page, 16)
                collect(sb, s_ref, outs, [], 0)

            each = sent(sb.tiles * (sb.depth // 2 * sb.rhs) // LANES)
            sol, *sol_parts = call(finished, [sol, c], [state] + [each] * count, aliases={0: 0}, flops=flops)
            sol_parts = [shift(p, "gx", d) if d else p for d, p in enumerate(sol_parts)]
            (r,) = call(
                slab_change(sb, par, False, True), [r, c, weights], [state], flops=flops,
                aliases={0: 0}, scratch=[coarse, coarse, coarse],
            )
            continue
        ins = [r, c, weights] if colour == 0 else [r, sol, c, weights]
        r, sol = call(
            slab_change(sb, par, colour == 0), ins, [state, state], flops=flops,
            aliases={0: 0} if colour == 0 else {0: 0, 1: 1}, scratch=[coarse, coarse, coarse],
        )

    def last(r_in, sol_ref, yy, gm, r_ref, *outs):
        slab_ghosts(sb, (1, 1, 1), r_ref, None, gm, yy)
        collect(sb, sol_ref, [], outs[count:], 0)
        collect(sb, r_ref, outs[:count], outs[count:], 1)

    r, *parts = call(
        last, [r, sol, pending, couple], [state] + [each] * count + [sent(2)] * count, aliases={0: 0}
    )

    def next_block(v, to):
        n = lax.axis_size("gz")
        return lax.ppermute(
            v, ("gx", "gz"), [(order[-1] * n + z, to * n + (z + 1) % n) for z in range(n)]
        )

    extras = [next_block(v, u) for u, v in enumerate(parts[count:])]
    parts = [shift(p, "gx", d) if d else p for d, p in enumerate(parts[:count])]
    whole = (right_side.shape, F32)
    return tuple(
        call(
            deliver(sb), sol_parts + parts + extras, [whole, whole], hbm_out=True,
            scratch=[((2, bk.ex, bk.q, bk.ey, LANES), F32)], copies=2 * bk.ex,
        )
    )


def on_device(right_side, cell_coef, cell_matrix, face_coupling, patch_inverse):
    dofs = cell_matrix.shape[0]
    ex, ey, ez = cell_coef.shape
    bk = Block(dofs, ex, ey, ez, right_side.shape[3] // ez)
    rows, tiles = bk.rows, bk.tiles
    square = (rows, LANES)

    state = ((tiles,) + square, F32)
    coarse = ((tiles,) + square, BF16)
    face_x, face_y = ((bk.faces_x,) + square, BF16), ((2 * bk.faces_y,) + square, BF16)

    def msg(n):
        return ((n,) + square, BF16)

    inverse, weights, couple = call(
        prep_tables(bk), [patch_inverse, cell_matrix, face_coupling],
        [((8 * rows, 8 * rows), BF16), ((rows, 7 * rows), BF16), ((4, rows, rows), BF16)],
        scratch=[((8 * rows, patch_inverse.shape[0]), BF16)], flops=1 << 30,
    )
    if Slab.fits(bk, lax.axis_size("gx")):
        sb = Slab(bk, lax.axis_size("gx"))
        return in_slabs(bk, sb, right_side, cell_coef, inverse, couple, weights)

    r, ymsg = call(
        prep_state(bk), [right_side, cell_coef.reshape(ex * ey, ez)], [state, msg(ex)],
        scratch=[((4,) + square, F32)],
    )
    ymsg = shift(ymsg, "gy", 1)
    edge = 2 * ey
    inner = len(halo_cells(bk))
    r, zl, zh, xm, xl, xh = call(
        prep_halo(bk), [r, ymsg],
        [state, msg(inner // 4), msg(inner // 4), msg(edge // 2), msg(edge // 4), msg(edge // 4)],
        aliases={0: 0},
    )
    halo = (
        shift(zh, "gz", 1),
        shift(zl, "gz", -1),
        shift(xm, "gx", 1),
        shift2(xh, "gx", 1, "gz", 1),
        shift2(xl, "gx", 1, "gz", -1),
    )
    solve_scratch = [((bk.nx * bk.ny // 2, 8 * rows, 2 * LANES), BF16)]
    solve_outs = [coarse, face_x, face_x, face_y]
    flops = 1 << 27
    sol = None
    pending = None
    for colour in range(8):
        par = (colour // 4, colour // 2 % 2, colour % 2)
        if colour == 0:

            def body(r_in, zl, zh, xm, xl, xh, p, r_ref, c, fl, fh, fy, xs):
                fill_halo(bk, r_ref, zl, zh, xm, xl, xh)
                solve(bk, (0, 0, 0), r_ref, p, c, fl, fh, fy, xs)

            r, c, fl, fh, fy = call(
                body, [r, *halo, inverse], [state] + solve_outs,
                aliases={0: 0}, scratch=solve_scratch, flops=flops,
            )
        else:
            before = ((colour - 1) // 4, (colour - 1) // 2 % 2, (colour - 1) % 2)
            if par[1] == before[1]:

                def body(r_in, s_in, lo, hi, yy, gm, p, r_ref, s_ref, c, fl, fh, fy, xs, par=par, before=before):
                    ghosts(bk, before, r_ref, s_ref, gm, lo, hi, yy)
                    solve(bk, par, r_ref, p, c, fl, fh, fy, xs)

                r, sol, c, fl, fh, fy = call(
                    body, [r, sol, *pending, couple, inverse], [state, state] + solve_outs,
                    aliases={0: 0, 1: 1}, scratch=solve_scratch, flops=flops,
                )
            else:
                r, sol = move_region(bk, before, par, r, sol, pending, couple, msg, state)

                def body(r_in, p, r_ref, c, fl, fh, fy, xs, par=par):
                    solve(bk, par, r_ref, p, c, fl, fh, fy, xs)

                r, c, fl, fh, fy = call(
                    body, [r, inverse], [state] + solve_outs,
                    aliases={0: 0}, scratch=solve_scratch, flops=flops,
                )
        pending = exchange(fl, fh, fy, bk)
        if colour == 0:
            r, sol = call(
                own_change(bk, par, True), [r, c, weights], [state, state],
                aliases={0: 0}, scratch=[coarse, coarse], flops=flops,
            )
        else:
            r, sol = call(
                own_change(bk, par, False), [r, sol, c, weights], [state, state],
                aliases={0: 0, 1: 1}, scratch=[coarse, coarse], flops=flops,
            )
    whole = (right_side.shape, F32)
    (solution_out,) = call(leave(bk, None), [sol], [whole], hbm_out=True, flops=flops)

    def last(r_in, lo, hi, yy, gm, r_ref):
        ghosts(bk, (1, 1, 1), r_ref, None, gm, lo, hi, yy)

    (r,) = call(last, [r, *pending, couple], [state], aliases={0: 0})
    (residual_out,) = call(leave(bk, None), [r], [whole], hbm_out=True)
    return solution_out, residual_out


def exchange(fl, fh, fy, bk):
    below, above = shift(fh, "gx", 1), shift(fl, "gx", -1)
    if lax.axis_size("gy") == 2:
        ys = shift(fy, "gy", 1)
    else:
        n = bk.faces_y
        ys = jnp.concatenate([shift(fy[:n], "gy", -1), shift(fy[n:], "gy", 1)])
    return below, above, ys


def move_region(bk, before, par, r, sol, pending, couple, msg, state):
    to_home_y = before[1] == 0
    to_home_x = before[0] == 0 and par[0] == 1
    with_sol = before == (0, 0, 1)
    x_send = bk.face_x(-1, 1)
    x_home = bk.face_x(bk.ex - 1, 1)
    a = par[0]
    y_cells = bk.face_y(-1, a)
    sol_cells = [bk.tile(bk.ex - 1, bk.ey - 1, pz) for pz in range(2)]
    n_y = len(y_cells) + (2 if with_sol else 0)

    def finish(r_in, s_in, lo, hi, yy, gm, r_ref, s_ref, m_ref):
        ghosts(bk, before, r_ref, s_ref, gm, lo, hi, yy)
        if to_home_x:
            for m, t in enumerate(x_send):
                m_ref[m] = r_ref[t].astype(BF16)
        else:
            for m, t in enumerate(y_cells):
                m_ref[m] = r_ref[t].astype(BF16)
            if with_sol:
                for m, t in enumerate(sol_cells):
                    m_ref[len(y_cells) + m] = s_ref[t].astype(BF16)

    n_first = len(x_send) if to_home_x else n_y
    r, sol, m = call(
        finish, [r, sol, *pending, couple], [state, state, msg(n_first)], aliases={0: 0, 1: 1}
    )
    if to_home_x:
        m = shift(m, "gx", -1)

        def turn(r_in, m_in, r_ref, y_ref):
            for i, t in enumerate(x_home):
                r_ref[t] = m_in[i].astype(F32)
            for i, t in enumerate(y_cells):
                y_ref[i] = r_ref[t].astype(BF16)

        r, m = call(turn, [r, m], [state, msg(n_y)], aliases={0: 0})
    m = shift(m, "gy", -1 if to_home_y else 1)

    def place(r_in, s_in, m_in, r_ref, s_ref):
        for i, t in enumerate(y_cells):
            r_ref[t] = m_in[i].astype(F32)
        if with_sol:
            for i, t in enumerate(sol_cells):
                s_ref[t] = m_in[len(y_cells) + i].astype(F32)

    r, sol = call(place, [r, sol, m], [state, state], aliases={0: 0, 1: 1})
    return r, sol


def solution(mesh):
    placed = (P(None, "gx", "gy", "gz"), P("gx", "gy", "gz"), P(), P(), P())
    return jax.shard_map(
        on_device,
        mesh=mesh,
        in_specs=placed,
        out_specs=(P(None, "gx", "gy", "gz"), P(None, "gx", "gy", "gz")),
        check_vma=False,
    )
```

```python
import jax
import jax.numpy as jnp
from jax import lax
from jax.experimental import pallas as pl
from jax.experimental.pallas import tpu as pltpu
from jax.sharding import PartitionSpec as P

F32 = jnp.float32
BF16 = jnp.bfloat16
LANES = 128
VMEM_LIMIT = 28 * 1024 * 1024


class Block:
    def __init__(self, dofs, extent_x, extent_y, extent_z, rhs):
        assert extent_x % 2 == 0 and extent_y % 4 == 0 and extent_z * rhs == LANES
        self.q, self.ex, self.ey, self.ez, self.rhs = dofs, extent_x, extent_y, extent_z, rhs
        self.rows = -(-(dofs + 2) // 16) * 16
        self.sent = -(-(dofs + 2) // 8) * 8
        self.nx, self.ny = extent_x // 2, extent_y // 2
        self.tiles = extent_x * extent_y * 2
        self.own = LANES // 4
        self.half = LANES // 2
        self.faces_x = 2 * extent_y
        self.faces_y = 2 * extent_x

    def tile(self, x, y, pz):
        px, py = x % 2, y % 2
        sx, sy = (x // 2) % self.nx, (y // 2) % self.ny
        return (((px * 2 + py) * 2 + pz) * self.nx + sx) * self.ny + sy

    def span(self, parity, extent):
        return range(parity - 1, parity - 1 + extent)

    def face_x(self, x, b):
        return [self.tile(x, y, pz) for y in self.span(b, self.ey) for pz in range(2)]

    def face_y(self, y, a):
        return [self.tile(x, y, pz) for x in self.span(a, self.ex) for pz in range(2)]


def lane_iota(rows):
    return lax.broadcasted_iota(jnp.int32, (rows, LANES), 1)


def in_steps(count, page, each=4):
    def step(i, carry):
        for n in range(each):
            page(i * each + n)
        return carry

    lax.fori_loop(0, count // each, step, 0)


def weight(inside, rows):
    return jnp.broadcast_to(jnp.where(inside, 1.0, 0.0).astype(BF16), (rows, LANES))


def roll(v, by):
    by = by % LANES
    return pltpu.roll(v, by, 1) if by else v


def turned(v, by):
    return roll(v, by) if isinstance(by, int) else pltpu.roll(v, (by + LANES) % LANES, 1)


def dot(a, b):
    return jnp.dot(a, b, preferred_element_type=F32)


def call(body, ins, outs, aliases=None, scratch=(), flops=0, hbm_out=False, far_in=0, copies=0, vmem=VMEM_LIMIT):
    space = pl.BlockSpec(memory_space=pltpu.VMEM)
    far = pl.BlockSpec(memory_space=pltpu.HBM)
    if hbm_out:
        shapes = [jax.ShapeDtypeStruct(s, d) for s, d in outs]
    else:
        shapes = [pltpu.VMEM(s, d) for s, d in outs]
    return pl.pallas_call(
        body,
        in_specs=[far] * far_in + [space] * (len(ins) - far_in),
        out_specs=[far if hbm_out and copies else space] * len(outs),
        out_shape=shapes,
        scratch_shapes=[pltpu.VMEM(s, d) for s, d in scratch]
        + ([pltpu.SemaphoreType.DMA((copies,))] if copies else []),
        input_output_aliases=aliases or {},
        compiler_params=pltpu.CompilerParams(vmem_limit_bytes=vmem),
        cost_estimate=pl.CostEstimate(flops=flops, bytes_accessed=0, transcendentals=0) if flops else None,
    )(*ins)


def coef_row(bk, r_ref, t):
    return r_ref[t, bk.q : bk.q + 1, :] + r_ref[t, bk.q + 1 : bk.q + 2, :]


def shift(v, axis, distance):
    n = lax.axis_size(axis)
    return lax.ppermute(v, axis, [((i - distance) % n, i) for i in range(n)])


def shift2(v, first, d1, second, d2):
    n1, n2 = lax.axis_size(first), lax.axis_size(second)
    route = [
        (((i - d1) % n1) * n2 + (j - d2) % n2, i * n2 + j) for i in range(n1) for j in range(n2)
    ]
    return lax.ppermute(v, (first, second), route)


def pack(bk, r_ref, tiles, lanes_from, count, out_ref, parts):
    lane = lane_iota(bk.rows)
    for n in range(0, len(tiles), parts):
        total = None
        for k, t in enumerate(tiles[n : n + parts]):
            moved = roll(r_ref[t], k * count - lanes_from)
            total = moved if total is None else jnp.where(lane < k * count, total, moved)
        out_ref[n // parts] = total.astype(BF16)


def unpack(bk, msg_ref, n, lanes_to, count, parts):
    k = n % parts
    return roll(msg_ref[n // parts].astype(F32), lanes_to - k * count)


def prep_tables(bk):
    q, rows = bk.q, bk.rows

    def body(p_ref, m_ref, f_ref, o_ref, w_ref, g_ref, pick_ref):
        n = p_ref.shape[0]
        row = lax.broadcasted_iota(jnp.int32, (rows, n), 0)
        col = lax.broadcasted_iota(jnp.int32, (rows, n), 1)

        def build(o, carry):
            pick = jnp.where((col == row * 8 + o) & (row < q), 1.0, 0.0).astype(BF16)
            pick_ref[pl.ds(o * rows, rows), :] = pick
            return carry

        lax.fori_loop(0, 8, build, 0)

        def move(o, carry):
            at = pl.ds(o * rows, rows)
            left = dot(pick_ref[at, :], p_ref[...]).astype(BF16)
            o_ref[at, :] = lax.dot_general(
                left, pick_ref[...], (((1,), (1,)), ((), ())), preferred_element_type=F32
            ).astype(BF16)
            return carry

        lax.fori_loop(0, 8, move, 0)
        row = lax.broadcasted_iota(jnp.int32, (q, 7 * rows), 0)
        col = lax.broadcasted_iota(jnp.int32, (q, 7 * rows), 1)
        total = dot(m_ref[...].astype(BF16), jnp.where(col == row, 1.0, 0.0).astype(BF16))
        g_ref[...] = jnp.zeros_like(g_ref)
        w_ref[...] = jnp.zeros_like(w_ref)
        one = jnp.where(
            lax.broadcasted_iota(jnp.int32, (q, rows), 0) == lax.broadcasted_iota(jnp.int32, (q, rows), 1),
            1.0, 0.0,
        ).astype(BF16)
        for direction in range(3):
            face = f_ref[direction].astype(BF16)
            for side in range(2):
                at = rows * (1 + 2 * direction + side)
                place = jnp.where(col == row + at, 1.0, 0.0).astype(BF16)
                dims = (((1 - side,), (0,)), ((), ()))
                total = total - lax.dot_general(face, place, dims, preferred_element_type=F32)
                if direction < 2:
                    g_ref[2 * direction + side, :q, :] = lax.dot_general(
                        face, one, dims, preferred_element_type=F32
                    ).astype(BF16)
        w_ref[:q, :] = total.astype(BF16)

    return body


def prep_state(bk):
    def body(rs_ref, cc_ref, r_ref, y_ref, scr):
        rows = rs_ref.reshape(bk.q * bk.ex * bk.ey, LANES)
        src = lax.broadcasted_iota(jnp.int32, (2 * LANES, 2 * LANES), 0) % LANES
        dst = lax.broadcasted_iota(jnp.int32, (2 * LANES, 2 * LANES), 1)
        pz, lane = dst // LANES, dst % LANES - bk.own
        z = 2 * (lane // bk.rhs) + pz
        inside = (lane >= 0) & (lane < bk.half)
        split = jnp.where(inside & (src == z * bk.rhs + lane % bk.rhs), 1.0, 0.0).astype(BF16)
        zz = lax.broadcasted_iota(jnp.int32, (bk.ez, LANES), 0)
        ll = lax.broadcasted_iota(jnp.int32, (bk.ez, LANES), 1)
        spread = jnp.where(ll // bk.rhs == zz, 1.0, 0.0).astype(BF16)
        coef = cc_ref[...]
        high = coef.astype(BF16)
        low = (coef - high.astype(F32)).astype(BF16)
        high, low = dot(high, spread), dot(low, spread)
        scr[...] = jnp.zeros_like(scr)
        for x in range(bk.ex):
            for y in range(bk.ey):
                n = x * bk.ey + y
                scr[n % 4, : bk.q, :] = rows[pl.ds(n, bk.q, stride=bk.ex * bk.ey), :]
                scr[n % 4, bk.q : bk.q + 1, :] = high[n : n + 1]
                scr[n % 4, bk.q + 1 : bk.q + 2, :] = low[n : n + 1]
                raw = scr[n % 4]
                top = raw.astype(BF16)
                rest = (raw - top.astype(F32)).astype(BF16)
                out = dot(jnp.concatenate([top, rest], axis=1), split)
                r_ref[bk.tile(x, y, 0)] = out[:, :LANES]
                r_ref[bk.tile(x, y, 1)] = out[:, LANES:]
        tiles = [bk.tile(x, bk.ey - 1, pz) for x in range(bk.ex) for pz in range(2)]
        pack(bk, r_ref, tiles, bk.own, bk.half, y_ref, 2)

    return body


def halo_cells(bk):
    return [
        bk.tile(x, y, pz)
        for x in range(bk.ex - 1)
        for y in bk.span(0, bk.ey)
        for pz in range(2)
    ]


def prep_halo(bk):
    def body(r_in, y_ref, r_ref, zl_ref, zh_ref, x_ref, xl_ref, xh_ref):
        n = 0
        for x in range(bk.ex):
            for pz in range(2):
                r_ref[bk.tile(x, -1, pz)] = unpack(bk, y_ref, n, bk.own, bk.half, 2)
                n += 1
        cells = halo_cells(bk)
        pack(bk, r_ref, cells, bk.own, bk.own, zl_ref, 4)
        pack(bk, r_ref, cells, 2 * bk.own, bk.own, zh_ref, 4)
        edge = bk.face_x(bk.ex - 1, 0)
        pack(bk, r_ref, edge, bk.own, bk.half, x_ref, 2)
        pack(bk, r_ref, edge, bk.own, bk.own, xl_ref, 4)
        pack(bk, r_ref, edge, 2 * bk.own, bk.own, xh_ref, 4)

    return body


def fill_halo(bk, r_ref, zl_ref, zh_ref, x_ref, xl_ref, xh_ref):
    lane = lane_iota(bk.rows)
    below, above = lane < bk.own, lane >= 3 * bk.own

    def joined(own, low_ref, high_ref, n):
        low = unpack(bk, low_ref, n, 0, bk.own, 4)
        high = unpack(bk, high_ref, n, 3 * bk.own, bk.own, 4)
        return jnp.where(below, low, jnp.where(above, high, own))

    for n, t in enumerate(halo_cells(bk)):
        r_ref[t] = joined(r_ref[t], zl_ref, zh_ref, n)
    for n, t in enumerate(bk.face_x(-1, 0)):
        r_ref[t] = joined(unpack(bk, x_ref, n, bk.own, bk.half, 2), xl_ref, xh_ref, n)


def solve(bk, colour, r_ref, p_ref, c_ref, xl_ref, xh_ref, y_ref, xs_ref):
    a, b, g = colour
    back = bk.rhs
    n = 0
    for px in range(bk.nx):
        for py in range(0, bk.ny, 2):
            cells = []
            for half in range(2):
                for o in range(8):
                    x = a - 1 + 2 * px + o // 4
                    y = b - 1 + 2 * (py + half) + o // 2 % 2
                    pz = o % 2 if g else 1 - o % 2
                    t = bk.tile(x, y, pz)
                    scale = lax.rsqrt(coef_row(bk, r_ref, t))
                    scaled = r_ref[t] * scale
                    if g == 0 and pz == 1:
                        scaled = roll(scaled, back)
                    lanes = slice(half * LANES, (half + 1) * LANES)
                    xs_ref[n, o * bk.rows : (o + 1) * bk.rows, lanes] = scaled.astype(BF16)
                    cells.append((half, o, t, scale, g == 0 and pz == 1))
            solved = dot(p_ref[...], xs_ref[n])
            for half, o, t, scale, moved in cells:
                v = solved[o * bk.rows : (o + 1) * bk.rows, half * LANES : (half + 1) * LANES]
                if moved:
                    v = roll(v, -back)
                c_ref[t] = (v * scale).astype(BF16)
            n += 1
    for m, t in enumerate(bk.face_x(a - 1, b)):
        xl_ref[m] = c_ref[t]
    for m, t in enumerate(bk.face_x(a - 2 + bk.ex, b)):
        xh_ref[m] = c_ref[t]
    for m, t in enumerate(bk.face_y(b - 1, a) + bk.face_y(b - 2 + bk.ey, a)):
        y_ref[m] = c_ref[t]


def ghosts(bk, colour, r_ref, sol_ref, g_ref, from_below, from_above, y_ref):
    a, b, g = colour

    def add(matrix, tiles, ghost_ref, base):
        for m in range(0, len(tiles), 2):
            two = jnp.concatenate([ghost_ref[base + m], ghost_ref[base + m + 1]], axis=1)
            change = dot(g_ref[matrix], two)
            r_ref[tiles[m]] += change[:, :LANES]
            r_ref[tiles[m + 1]] += change[:, LANES:]

    add(0, bk.face_x(a - 2 + bk.ex, b), from_above, 0)
    add(1, bk.face_x(a - 1, b), from_below, 0)
    add(2, bk.face_y(b - 2 + bk.ey, a), y_ref, 0)
    add(3, bk.face_y(b - 1, a), y_ref, bk.faces_y)
    if a == 0:
        for m, t in enumerate(bk.face_x(bk.ex - 1, b)):
            sol_ref[t] += from_above[m].astype(F32)
    if b == 0:
        m = 0
        for x in bk.span(a, bk.ex):
            for pz in range(2):
                if x >= 0:
                    sol_ref[bk.tile(x, bk.ey - 1, pz)] += y_ref[m].astype(F32)
                m += 1


def own_change(bk, colour, first):
    a, b, g = colour

    def body(*refs):
        if first:
            r_in, c_ref, w_ref, r_ref, sol_ref, cm_ref, cz_ref = refs
        else:
            r_in, sol_in, c_ref, w_ref, r_ref, sol_ref, cm_ref, cz_ref = refs
        xs, ys = bk.span(a, bk.ex), bk.span(b, bk.ey)
        for x in xs:
            for y in ys:
                for pz in range(2):
                    t = bk.tile(x, y, pz)
                    c = c_ref[t].astype(F32)
                    cm_ref[t] = (c * coef_row(bk, r_ref, t)).astype(BF16)
                    cz_ref[t] = roll(c_ref[t], bk.rhs if pz else -bk.rhs)
                    if x >= 0 and y >= 0:
                        sol_ref[t] = c if first else sol_ref[t] + c
                    elif first:
                        sol_ref[t] = jnp.zeros_like(c)
        nothing = jnp.zeros((bk.rows, LANES), BF16)

        def at(x, y, pz):
            return c_ref[bk.tile(x, y, pz)] if x in xs and y in ys else nothing

        def stack(x, y, pz):
            other = bk.tile(x, y, 1 - pz)
            near, far = c_ref[other], cz_ref[other]
            return jnp.concatenate(
                [
                    cm_ref[bk.tile(x, y, pz)],
                    at(x + 1, y, pz),
                    at(x - 1, y, pz),
                    at(x, y + 1, pz),
                    at(x, y - 1, pz),
                    far if pz else near,
                    near if pz else far,
                ],
                axis=0,
            )

        for x in xs:
            for y in ys:
                both = jnp.concatenate([stack(x, y, 0), stack(x, y, 1)], axis=1)
                change = dot(w_ref[...], both)
                for pz in range(2):
                    r_ref[bk.tile(x, y, pz)] -= change[:, pz * LANES : (pz + 1) * LANES]

    return body


def leave(bk, ref):
    def body(tile_ref, out_ref):
        rows = out_ref.reshape(bk.q * bk.ex * bk.ey, LANES)
        src = lax.broadcasted_iota(jnp.int32, (2 * LANES, LANES), 0)
        dst = lax.broadcasted_iota(jnp.int32, (2 * LANES, LANES), 1)
        pz, lane = src // LANES, src % LANES - bk.own
        z = 2 * (lane // bk.rhs) + pz
        inside = (lane >= 0) & (lane < bk.half)
        join = jnp.where(inside & (dst == z * bk.rhs + lane % bk.rhs), 1.0, 0.0).astype(BF16)
        for x in range(bk.ex):
            for y in range(bk.ey):
                both = jnp.concatenate(
                    [tile_ref[bk.tile(x, y, 0)], tile_ref[bk.tile(x, y, 1)]], axis=1
                )
                top = both.astype(BF16)
                rest = (both - top.astype(F32)).astype(BF16)
                out = dot(top, join) + dot(rest, join)
                rows[pl.ds(x * bk.ey + y, bk.q, stride=bk.ex * bk.ey), :] = out[: bk.q]

    return body


class Slab:
    def __init__(self, bk, count):
        self.bk, self.count = bk, count
        self.q, self.rhs, self.rows, self.ny = bk.q, bk.rhs, bk.rows, bk.ny
        self.sent = bk.sent
        self.ey = bk.ey
        self.groups = count
        self.width = LANES // count
        self.depth = bk.ez // count
        self.halo = 2 * bk.rhs
        self.tiles = bk.tiles

    @staticmethod
    def fits(bk, count):
        depth = bk.ez // count
        return (
            bk.ez % count == 0
            and depth % 2 == 0
            and bk.nx == 2
            and (depth // 2 + 4) * bk.rhs * count == LANES
            and bk.tiles % 16 == 0
        )

    def tile(self, px, x2, y, pz):
        return (((px * 2 + y % 2) * 2 + pz) * 2 + x2) * self.ny + (y // 2) % self.ny

    def face_y(self, y):
        return [self.tile(px, x2, y, pz) for px in range(2) for x2 in range(2) for pz in range(2)]

    def edge(self, n, low_side):
        pz = n // (2 * self.ny) % 2
        index = n // (4 * self.ny) * (2 * self.ny // self.groups) + n % (2 * self.ny) // self.groups
        pairs = (2 if pz else 3) if low_side else (2 if pz else 1)
        each = {1: 8, 2: 4, 3: 2}[pairs]
        base = 0 if pz else self.tiles // (2 * self.groups) // 4
        return base + index // each, index % each * (self.width // each), pairs * self.rhs

    def pages(self, low_side):
        return 1 + max(self.edge(n, low_side)[0] for n in range(0, self.tiles, self.groups))

    def place(self, device):
        slab = device * 0
        for s, d in enumerate(self.order()):
            slab = jnp.where(device == d, s, slab)
        return slab

    def order(self):
        return [0, 1, 3, 2] if self.count == 4 else list(range(self.count))


def home_prep(bk, sb):
    def body(rs_ref, cc_ref, h_ref, up_ref, down_ref, scr, high_ref, low_ref, in_ref, cin_ref, sems):
        copies = [
            pltpu.make_async_copy(rs_ref.at[:, x], in_ref.at[x], sems.at[x]) for x in range(bk.ex)
        ]
        coefs = pltpu.make_async_copy(cc_ref, cin_ref, sems.at[bk.ex])
        coefs.start()
        for c in copies:
            c.start()
        src = lax.broadcasted_iota(jnp.int32, (LANES, 2 * LANES), 0)
        dst = lax.broadcasted_iota(jnp.int32, (LANES, 2 * LANES), 1)
        pz, lane = dst // LANES, dst % LANES - bk.own
        z = 2 * (lane // bk.rhs) + pz
        inside = (lane >= 0) & (lane < bk.half)
        split = jnp.where(inside & (src == z * bk.rhs + lane % bk.rhs), 1.0, 0.0).astype(BF16)
        zz = lax.broadcasted_iota(jnp.int32, (bk.ez, LANES), 0)
        ll = lax.broadcasted_iota(jnp.int32, (bk.ez, LANES), 1)
        spread = jnp.where(ll // bk.rhs == zz, 1.0, 0.0).astype(BF16)
        coefs.wait()
        coef = cin_ref[...]
        high = coef.astype(BF16)
        low = (coef - high.astype(F32)).astype(BF16)
        high_ref[...], low_ref[...] = dot(high, spread), dot(low, spread)
        scr[...] = jnp.zeros_like(scr)

        for x in range(bk.ex):
            copies[x].wait()
            rows = in_ref.at[x].reshape(bk.q * bk.ey, LANES)

            def column(half, carry, x=x, rows=rows):
                for i in range(bk.ey // 2):
                    y = half + 2 * i
                    n = x * bk.ey + y
                    scr[i, : bk.q, :] = rows[pl.ds(y, bk.q, stride=bk.ey), :]
                    scr[i, bk.q : bk.q + 1, :] = high_ref[pl.ds(n, 1), :]
                    scr[i, bk.q + 1 : bk.q + 2, :] = low_ref[pl.ds(n, 1), :]
                    out = dot(scr[i].astype(BF16), split)
                    h_ref[bk.tile(x, y, 0)] = out[:, :LANES].astype(BF16)
                    h_ref[bk.tile(x, y, 1)] = out[:, LANES:].astype(BF16)
                return carry

            for half in range(2):
                column(half, 0)
        lane = lane_iota(1)
        for ref, low_side in ((up_ref, False), (down_ref, True)):
            for n in range(0, bk.tiles, sb.groups):
                page, slot, width = sb.edge(n, low_side)
                start = bk.own if low_side else bk.own + bk.half - width
                total = ref[page] if slot else None
                for k in range(sb.groups):
                    at = k * sb.width + slot
                    inside = weight((lane >= at) & (lane < at + width), sb.sent)
                    v = roll(h_ref[n + k, : sb.sent], at - start) * inside
                    total = v if total is None else total + v
                ref[page] = total

    return body


def scatter(sb):
    bk, parts, rows = sb.bk, sb.groups, sb.sent

    def body(h_ref, below_ref, above_ref, *outs):
        lane = lane_iota(1)
        me = lax.axis_index("gx")
        step = bk.half // parts
        keep, slabs = [], []
        for d in range(parts):
            slab = sb.place((me + d) % parts)
            slabs.append(slab)
            group = (lane - slab * step + LANES) % LANES // sb.width
            keep.append([weight(group == (me + k) % parts, rows) for k in range(parts)])
        ends = {}
        for pz in range(2):
            for low_side in range(2):
                pairs = sb.edge(0 if not pz else 2 * sb.ny, not low_side)[2]
                if low_side:
                    inside, end = lane % sb.width < pairs, 0
                else:
                    at = (lane - step * (parts - 1) + LANES) % LANES
                    inside, end = at % sb.width >= sb.width - pairs, parts - 1
                for d in range(parts):
                    chosen = jnp.where(inside, jnp.where(slabs[d] == end, 1, 0), 0)
                    ends[pz, low_side, d] = weight(chosen == 1, rows)
        for n in range(0, sb.tiles, parts):
            totals = [None] * parts
            pz = n // (2 * sb.ny) % 2
            for k in range(parts):
                start = bk.own - (2 if pz else 1) * bk.rhs
                by = ((me + k) % parts * sb.width - start + LANES) % LANES
                v = pltpu.roll(h_ref[n + k, :rows], by, 1)
                for d in range(parts):
                    totals[d] = v * keep[d][k] if k == 0 else totals[d] + v * keep[d][k]
            page, slot, width = sb.edge(n, False)
            low = pltpu.roll(below_ref[page], (me * sb.width - slot + LANES) % LANES, 1)
            page, slot, width = sb.edge(n, True)
            by = me * sb.width + step * (parts - 1) + sb.width - width - slot
            high = pltpu.roll(above_ref[page], (by + LANES) % LANES, 1)
            for d, out in enumerate(outs):
                out[n // parts] = totals[d] + low * ends[pz, 1, d] + high * ends[pz, 0, d]

    return body


def gather_state(sb, parts_refs, r_ref):
    parts, rows = sb.groups, sb.sent
    me = lax.axis_index("gx")
    by = sb.place(me) * (sb.bk.half // parts)
    group = (lane_iota(1) - by + LANES) % LANES // sb.width
    keep = [
        [weight(group == (me - d + parts + k) % parts, rows) for d in range(parts)]
        for k in range(parts)
    ]

    def page(n):
        for k in range(parts):
            total = parts_refs[0][n] * keep[k][0]
            for d in range(1, parts):
                total = total + parts_refs[d][n] * keep[k][d]
            total = pltpu.roll(total, (2 * LANES - k * sb.width - by) % LANES, 1)
            r_ref[n * parts + k, :rows] = total.astype(F32)
            r_ref[n * parts + k, rows:] = jnp.zeros((sb.rows - rows, LANES), F32)

    in_steps(sb.tiles // parts, page)


def slab_solve(sb, colour, r_ref, p_ref, c_ref, y_ref, xs_ref, part=None):
    a, b, g = colour
    rows = sb.rows

    def column(x2, carry):
        for n, py in enumerate(range(0, sb.ny, 2)):
            if part is not None and n not in part:
                continue
            cells = []
            for half in range(2):
                for o in range(8):
                    xo, y = o // 4, b - 1 + 2 * (py + half) + o // 2 % 2
                    pz = o % 2 if g else 1 - o % 2
                    moved = -sb.rhs if g == 1 and pz == 1 else 0
                    if a or xo == 1:
                        t = sb.tile(xo if a else 0, x2, y, pz)
                    else:
                        t = sb.tile(1, 1 - x2, y, pz)
                        moved = moved + (1 - x2) * sb.width
                    scale = lax.rsqrt(coef_row(sb, r_ref, t))
                    lanes = slice(half * LANES, (half + 1) * LANES)
                    xs_ref[n, o * rows : (o + 1) * rows, lanes] = turned(
                        r_ref[t] * scale, moved
                    ).astype(BF16)
                    cells.append((half, o, t, scale, moved))
            solved = dot(p_ref[...], xs_ref[n])
            for half, o, t, scale, moved in cells:
                v = solved[o * rows : (o + 1) * rows, half * LANES : (half + 1) * LANES]
                c_ref[t] = (turned(v, -moved) * scale).astype(BF16)
        return carry

    if part is None:
        lax.fori_loop(0, 2, column, 0)
    else:
        for x2 in range(2):
            column(x2, 0)
    if y_ref is None:
        return
    for m, t in enumerate(sb.face_y(b - 1) + sb.face_y(b - 2 + sb.ey)):
        y_ref[m] = c_ref[t]


def slab_ghosts(sb, colour, r_ref, sol_ref, g_ref, y_ref):
    a, b, g = colour
    count = len(sb.face_y(0))
    for matrix, y, base in ((2, b - 2 + sb.ey, 0), (3, b - 1, count)):
        tiles = sb.face_y(y)
        for m in range(0, count, 2):
            two = jnp.concatenate([y_ref[base + m], y_ref[base + m + 1]], axis=1)
            change = dot(g_ref[matrix], two)
            r_ref[tiles[m]] += change[:, :LANES]
            r_ref[tiles[m + 1]] += change[:, LANES:]
    if b == 0:
        for m, t in enumerate(sb.face_y(sb.ey - 1)):
            sol_ref[t] += y_ref[m].astype(F32)


def slab_change(sb, colour, first, last=False):
    a, b, g = colour

    def body(*refs):
        if last:
            r_in, c_ref, w_ref, r_ref, cm_ref, cz_ref, cx_ref = refs
        elif first:
            r_in, c_ref, w_ref, r_ref, sol_ref, cm_ref, cz_ref, cx_ref = refs
        else:
            r_in, sol_in, c_ref, w_ref, r_ref, sol_ref, cm_ref, cz_ref, cx_ref = refs
        ys = sb.bk.span(b, sb.ey)
        cells = [(px, x2, y) for px in range(2) for x2 in range(2) for y in ys]
        for px, x2, y in cells:
            for pz in range(2):
                t = sb.tile(px, x2, y, pz)
                c = c_ref[t].astype(F32)
                cm_ref[t] = (c * coef_row(sb, r_ref, t)).astype(BF16)
                cz_ref[t] = roll(c_ref[t], -sb.rhs if pz else sb.rhs)
                if px == x2:
                    cx_ref[t] = roll(c_ref[t], sb.width if px else -sb.width)
                if last:
                    continue
                if y >= 0:
                    sol_ref[t] = c if first else sol_ref[t] + c
                elif first:
                    sol_ref[t] = jnp.zeros_like(c)
        nothing = jnp.zeros((sb.rows, LANES), BF16)

        def stack(px, x2, y, pz):
            beside = c_ref[sb.tile(1 - px, x2, y, pz)]
            across = (cx_ref if px == x2 else c_ref)[sb.tile(1 - px, 1 - x2, y, pz)]
            other = sb.tile(px, x2, y, 1 - pz)
            near, far = c_ref[other], cz_ref[other]
            return jnp.concatenate(
                [
                    cm_ref[sb.tile(px, x2, y, pz)],
                    across if px else beside,
                    beside if px else across,
                    c_ref[sb.tile(px, x2, y + 1, pz)] if y + 1 in ys else nothing,
                    c_ref[sb.tile(px, x2, y - 1, pz)] if y - 1 in ys else nothing,
                    near if pz else far,
                    far if pz else near,
                ],
                axis=0,
            )

        for px, x2, y in cells:
            both = jnp.concatenate([stack(px, x2, y, 0), stack(px, x2, y, 1)], axis=1)
            change = dot(w_ref[...], both)
            for pz in range(2):
                r_ref[sb.tile(px, x2, y, pz)] -= change[:, pz * LANES : (pz + 1) * LANES]

    return body


def emit_halo(sb, r_ref, up_ref, down_ref):
    rows = sb.sent
    lane = lane_iota(rows) % sb.width
    top = sb.width - 2 * sb.halo
    parts = sb.width // sb.halo

    def page(n):
        for ref, start in ((up_ref, top), (down_ref, sb.halo)):
            total = None
            for k in range(parts):
                moved = roll(r_ref[n * parts + k, :rows], k * sb.halo - start)
                total = moved if k == 0 else jnp.where(lane < k * sb.halo, total, moved)
            ref[n] = total.astype(BF16)

    in_steps(sb.tiles // parts, page)


def fill_slab_halo(sb, r_ref, below_ref, above_ref):
    rows = sb.sent
    lane = lane_iota(rows) % sb.width
    parts = sb.width // sb.halo

    def page(n):
        for k in range(parts):
            t = n * parts + k
            low = roll(below_ref[n].astype(F32), -k * sb.halo)
            high = roll(above_ref[n].astype(F32), sb.width - sb.halo - k * sb.halo)
            own = jnp.where(lane < sb.halo, low, r_ref[t, :rows])
            r_ref[t, :rows] = jnp.where(lane >= sb.width - sb.halo, high, own)

    in_steps(sb.tiles // parts, page)


def collect(sb, source, outs, extras, extra_at):
    width = sb.width - 2 * sb.halo
    parts = LANES // width
    rows = sb.sent
    lane = lane_iota(rows)
    piece = lane_iota(1) // width
    me = lax.axis_index("gx")
    slab = sb.place(me)
    offset = sb.bk.own // width
    keep = [
        [
            weight(piece == (offset + slab + k + 2 * ((me + d) % sb.groups)) % parts, rows)
            for k in range(parts)
        ]
        for d in range(len(outs))
    ]
    def page(n):
        totals = [None] * len(outs)
        for k in range(parts):
            by = (offset + slab + k) * width - sb.halo
            v = pltpu.roll(source[n * parts + k, :rows].astype(BF16), by % LANES, 1)
            for d in range(len(outs)):
                totals[d] = v * keep[d][k] if k == 0 else totals[d] + v * keep[d][k]
        for d, out in enumerate(outs):
            out[n] = totals[d]

    if outs:
        in_steps(sb.tiles // parts, page)
    per = sb.width // sb.rhs
    evens = even_tiles(sb)
    joined = []
    for m in range(sb.groups if extras else 0):
        total = None
        for k, t in enumerate(evens[m * per : (m + 1) * per]):
            v = roll(source[t, :rows].astype(BF16), k * sb.rhs - (sb.width - sb.halo - sb.rhs))
            total = v if k == 0 else jnp.where(lane % sb.width < k * sb.rhs, total, v)
        joined.append(roll(total, m * sb.width))
    for u, out in enumerate(extras):
        total = joined[0]
        for m in range(1, sb.groups):
            total = jnp.where(lane // sb.width == (u + m) % sb.groups, joined[m], total)
        out[extra_at] = total


def even_tiles(sb):
    return [t for t in range(sb.tiles) if t // (2 * sb.ny) % 2 == 0]


def deliver(sb):
    bk = sb.bk
    width = sb.width - 2 * sb.halo
    parts = LANES // width
    per = sb.width // sb.rhs

    def body(*refs):
        count = sb.groups
        both_ins = (refs[:count], refs[count : 2 * count])
        extras, outs = refs[2 * count : 3 * count], refs[3 * count : 3 * count + 2]
        buffer, sems = refs[3 * count + 2 :]
        rows_sent = sb.sent
        lane = lane_iota(1)
        piece = lane // width
        first = weight((lane >= bk.own) & (lane < bk.own + bk.rhs), rows_sent)
        later = 1 - first
        src = lax.broadcasted_iota(jnp.int32, (2 * LANES, LANES), 0)
        dst = lax.broadcasted_iota(jnp.int32, (2 * LANES, LANES), 1)
        pz, at = src // LANES, src % LANES - bk.own
        z = 2 * (at // bk.rhs) + pz
        inside = (at >= 0) & (at < bk.half)
        join = jnp.where(inside & (dst == z * bk.rhs + at % bk.rhs), 1.0, 0.0).astype(BF16)
        me = lax.axis_index("gx")
        slabs = [sb.place((me - d + sb.groups) % sb.groups) for d in range(sb.groups)]
        keep = [
            [weight(piece == (bk.own // width + s + k + 2 * me) % parts, rows_sent) for s in slabs]
            for k in range(parts)
        ]
        evens = even_tiles(sb)
        def copy_of(index, x):
            return pltpu.make_async_copy(
                buffer.at[index, x], outs[index].at[:, x], sems.at[index * bk.ex + x]
            )

        for index in range(2):
            ins = both_ins[index]
            layer = extras[0][index]
            for e in extras[1:]:
                layer = layer + e[index]

            def home(t, k, even, ins=ins, layer=layer):
                page = t // parts
                total = ins[0][page] * keep[k][0]
                for d in range(1, sb.groups):
                    total = total + ins[d][page] * keep[k][d]
                by = (3 * LANES - (k + 2 * me) * width + (bk.rhs if even else 0)) % LANES
                total = pltpu.roll(total, by, 1)
                if not even:
                    return total
                n = t // (2 * parts) * parts + k
                by = (bk.own + 3 * LANES - (me + n // per) * sb.width - n % per * sb.rhs) % LANES
                return first * pltpu.roll(layer, by, 1) + later * total

            def columns(px, carry, index=index, home=home):
                for sx in range(bk.nx):
                    x = 2 * sx + px
                    rows = buffer.at[index, x].reshape(bk.q * bk.ey, LANES)
                    for y in range(bk.ey):
                        t = bk.tile(x, y, 0)
                        k = sx * bk.ny + y // 2
                        both = jnp.concatenate(
                            [home(t, k, True), home(t + parts, k, False)], axis=1
                        )
                        out = dot(both, join)
                        rows[pl.ds(y, bk.q, stride=bk.ey), :] = out[: bk.q]
                    copy_of(index, x).start()
                return carry

            lax.fori_loop(0, 2, columns, 0)
        for index in range(2):
            for x in range(bk.ex):
                copy_of(index, x).wait()

    return body


def in_slabs(bk, sb, right_side, cell_coef, inverse, couple, weights):
    count, order = sb.count, sb.order()
    square = (sb.rows, LANES)
    state = ((sb.tiles,) + square, F32)
    coarse = ((sb.tiles,) + square, BF16)
    faces = ((2 * len(sb.face_y(0)),) + square, BF16)
    one_face = (((len(sb.face_y(0)),) + square), BF16)

    def msg(n):
        return ((n,) + square, BF16)

    def sent(n):
        return ((n, sb.sent, LANES), BF16)

    spread = ((bk.ex * bk.ey, LANES), F32)
    home, up, down = call(
        home_prep(bk, sb), [right_side, cell_coef.reshape(bk.ex * bk.ey, bk.ez)],
        [coarse, sent(sb.pages(False)), sent(sb.pages(True))],
        scratch=[
            ((bk.ey // 2,) + square, F32), spread, spread,
            ((bk.ex, bk.q, bk.ey, LANES), F32), ((bk.ex * bk.ey, bk.ez), F32),
        ],
        far_in=2, copies=bk.ex + 1, vmem=64_600_000,
    )
    below, above = shift(up, "gz", 1), shift(down, "gz", -1)
    pieces = call(scatter(sb), [home, below, above], [sent(sb.tiles // count)] * count)
    pieces = [shift(p, "gx", d) if d else p for d, p in enumerate(pieces)]

    def chain(v, step):
        n = lax.axis_size("gz")
        route = []
        for z in range(n):
            for s in range(count):
                total = (z * count + s + step) % (n * count)
                route.append((order[s] * n + z, order[total % count] * n + total // count))
        return lax.ppermute(v, ("gx", "gz"), route)

    def swap(v, step):
        return shift(v, "gy", step)

    edge = sb.face_y(-1)

    def assemble(*refs):
        r_ref, y_ref = refs[count + 1 :]
        gather_state(sb, refs[:count], r_ref)
        for m, t in enumerate(edge):
            y_ref[m] = r_ref[t].astype(BF16)

    r, moved = call(assemble, pieces + [inverse], [state, one_face])
    moved = swap(moved, 1)
    sol = halos = pending = None
    flops = 1 << 27
    solve_scratch = [((sb.ny // 2, 8 * sb.rows, 2 * LANES), BF16)]
    halo_msg = sent(sb.tiles * sb.halo // sb.width)
    refresh = (3,)

    for colour in range(8):
        par = (colour // 4, colour // 2 % 2, colour % 2)
        before = ((colour - 1) // 4, (colour - 1) // 2 % 2, (colour - 1) % 2)
        fresh = (colour - 1) in refresh
        turn = colour > 0 and par[1] != before[1]
        if turn or fresh:

            def finish(r_in, s_in, yy, gm, r_ref, s_ref, *outs, before=before, turn=turn):
                slab_ghosts(sb, before, r_ref, s_ref, gm, yy)
                if turn:
                    for m, t in enumerate(edge):
                        outs[0][m] = r_ref[t].astype(BF16)
                else:
                    emit_halo(sb, r_ref, *outs)

            outs = [one_face] if turn else [halo_msg, halo_msg]
            r, sol, *out = call(
                finish, [r, sol, pending, couple], [state, state] + outs, aliases={0: 0, 1: 1}
            )
            if turn:
                moved = swap(out[0], -1 if before[1] == 0 else 1)
            if turn and fresh:

                def turned(r_in, m_in, r_ref, u_ref, d_ref):
                    for m, t in enumerate(edge):
                        r_ref[t] = m_in[m].astype(F32)
                    emit_halo(sb, r_ref, u_ref, d_ref)

                r, *out = call(turned, [r, moved], [state, halo_msg, halo_msg], aliases={0: 0})
            if fresh:
                halos = (chain(out[0], 1), chain(out[1], -1))

                def solve_fresh(r_in, lo, hi, p, r_ref, c, fy, xs, par=par):
                    fill_slab_halo(sb, r_ref, lo, hi)
                    slab_solve(sb, par, r_ref, p, c, fy, xs)

                args = [r, *halos, inverse]
                body = solve_fresh
            else:
                args = [r, moved, inverse]
                body = None
        elif colour == 0:
            args, body = [r, moved, inverse], None
        else:

            def solve_next(r_in, s_in, yy, gm, p, r_ref, s_ref, c, fy, xs, par=par, before=before):
                slab_ghosts(sb, before, r_ref, s_ref, gm, yy)
                slab_solve(sb, par, r_ref, p, c, fy, xs)

            args, body = [r, sol, pending, couple, inverse], solve_next
        if body is None:
            pages = sb.ny // 2
            late = [0] if par[1] == 0 else [pages - 1]

            def early(r_ref, p, c, xs, par=par, late=late):
                slab_solve(sb, par, r_ref, p, c, None, xs, [n for n in range(pages) if n not in late])

            (c,) = call(early, [r, inverse], [coarse], scratch=solve_scratch, flops=flops)

            def body(r_in, m_in, p, c_in, r_ref, c, fy, xs, par=par, late=late):
                for m, t in enumerate(edge):
                    r_ref[t] = m_in[m].astype(F32)
                slab_solve(sb, par, r_ref, p, c, fy, xs, late)

            args = args + [c]

        with_sol = len(args) == 5
        split = body.__name__ == "body"
        kept = [state, state] if with_sol else [state]
        got = call(
            body, args, kept + [coarse, faces], scratch=solve_scratch, flops=flops,
            aliases={0: 0, 1: 1} if with_sol else ({0: 0, 3: 1} if split else {0: 0}),
        )
        if with_sol:
            r, sol, c, fy = got
        else:
            r, c, fy = got
        if lax.axis_size("gy") == 2:
            pending = swap(fy, 1)
        else:
            n = len(edge)
            pending = jnp.concatenate([swap(fy[:n], -1), swap(fy[n:], 1)])
        if colour == 7:

            def finished(s_in, c_ref, s_ref, *outs):

                def page(t):
                    s_ref[t] += c_ref[t].astype(F32)

                in_steps(sb.tiles, page, 16)
                collect(sb, s_ref, outs, [], 0)

            each = sent(sb.tiles * (sb.depth // 2 * sb.rhs) // LANES)
            sol, *sol_parts = call(finished, [sol, c], [state] + [each] * count, aliases={0: 0}, flops=flops)
            sol_parts = [shift(p, "gx", d) if d else p for d, p in enumerate(sol_parts)]
            (r,) = call(
                slab_change(sb, par, False, True), [r, c, weights], [state], flops=flops,
                aliases={0: 0}, scratch=[coarse, coarse, coarse],
            )
            continue
        ins = [r, c, weights] if colour == 0 else [r, sol, c, weights]
        r, sol = call(
            slab_change(sb, par, colour == 0), ins, [state, state], flops=flops,
            aliases={0: 0} if colour == 0 else {0: 0, 1: 1}, scratch=[coarse, coarse, coarse],
        )

    def last(r_in, sol_ref, yy, gm, r_ref, *outs):
        slab_ghosts(sb, (1, 1, 1), r_ref, None, gm, yy)
        collect(sb, sol_ref, [], outs[count:], 0)
        collect(sb, r_ref, outs[:count], outs[count:], 1)

    r, *parts = call(
        last, [r, sol, pending, couple], [state] + [each] * count + [sent(2)] * count, aliases={0: 0}
    )

    def next_block(v, to):
        n = lax.axis_size("gz")
        return lax.ppermute(
            v, ("gx", "gz"), [(order[-1] * n + z, to * n + (z + 1) % n) for z in range(n)]
        )

    extras = [next_block(v, u) for u, v in enumerate(parts[count:])]
    parts = [shift(p, "gx", d) if d else p for d, p in enumerate(parts[:count])]
    whole = (right_side.shape, F32)
    return tuple(
        call(
            deliver(sb), sol_parts + parts + extras, [whole, whole], hbm_out=True,
            scratch=[((2, bk.ex, bk.q, bk.ey, LANES), F32)], copies=2 * bk.ex,
        )
    )


def on_device(right_side, cell_coef, cell_matrix, face_coupling, patch_inverse):
    dofs = cell_matrix.shape[0]
    ex, ey, ez = cell_coef.shape
    bk = Block(dofs, ex, ey, ez, right_side.shape[3] // ez)
    rows, tiles = bk.rows, bk.tiles
    square = (rows, LANES)

    state = ((tiles,) + square, F32)
    coarse = ((tiles,) + square, BF16)
    face_x, face_y = ((bk.faces_x,) + square, BF16), ((2 * bk.faces_y,) + square, BF16)

    def msg(n):
        return ((n,) + square, BF16)

    inverse, weights, couple = call(
        prep_tables(bk), [patch_inverse, cell_matrix, face_coupling],
        [((8 * rows, 8 * rows), BF16), ((rows, 7 * rows), BF16), ((4, rows, rows), BF16)],
        scratch=[((8 * rows, patch_inverse.shape[0]), BF16)], flops=1 << 30,
    )
    if Slab.fits(bk, lax.axis_size("gx")):
        sb = Slab(bk, lax.axis_size("gx"))
        return in_slabs(bk, sb, right_side, cell_coef, inverse, couple, weights)

    r, ymsg = call(
        prep_state(bk), [right_side, cell_coef.reshape(ex * ey, ez)], [state, msg(ex)],
        scratch=[((4,) + square, F32)],
    )
    ymsg = shift(ymsg, "gy", 1)
    edge = 2 * ey
    inner = len(halo_cells(bk))
    r, zl, zh, xm, xl, xh = call(
        prep_halo(bk), [r, ymsg],
        [state, msg(inner // 4), msg(inner // 4), msg(edge // 2), msg(edge // 4), msg(edge // 4)],
        aliases={0: 0},
    )
    halo = (
        shift(zh, "gz", 1),
        shift(zl, "gz", -1),
        shift(xm, "gx", 1),
        shift2(xh, "gx", 1, "gz", 1),
        shift2(xl, "gx", 1, "gz", -1),
    )
    solve_scratch = [((bk.nx * bk.ny // 2, 8 * rows, 2 * LANES), BF16)]
    solve_outs = [coarse, face_x, face_x, face_y]
    flops = 1 << 27
    sol = None
    pending = None
    for colour in range(8):
        par = (colour // 4, colour // 2 % 2, colour % 2)
        if colour == 0:

            def body(r_in, zl, zh, xm, xl, xh, p, r_ref, c, fl, fh, fy, xs):
                fill_halo(bk, r_ref, zl, zh, xm, xl, xh)
                solve(bk, (0, 0, 0), r_ref, p, c, fl, fh, fy, xs)

            r, c, fl, fh, fy = call(
                body, [r, *halo, inverse], [state] + solve_outs,
                aliases={0: 0}, scratch=solve_scratch, flops=flops,
            )
        else:
            before = ((colour - 1) // 4, (colour - 1) // 2 % 2, (colour - 1) % 2)
            if par[1] == before[1]:

                def body(r_in, s_in, lo, hi, yy, gm, p, r_ref, s_ref, c, fl, fh, fy, xs, par=par, before=before):
                    ghosts(bk, before, r_ref, s_ref, gm, lo, hi, yy)
                    solve(bk, par, r_ref, p, c, fl, fh, fy, xs)

                r, sol, c, fl, fh, fy = call(
                    body, [r, sol, *pending, couple, inverse], [state, state] + solve_outs,
                    aliases={0: 0, 1: 1}, scratch=solve_scratch, flops=flops,
                )
            else:
                r, sol = move_region(bk, before, par, r, sol, pending, couple, msg, state)

                def body(r_in, p, r_ref, c, fl, fh, fy, xs, par=par):
                    solve(bk, par, r_ref, p, c, fl, fh, fy, xs)

                r, c, fl, fh, fy = call(
                    body, [r, inverse], [state] + solve_outs,
                    aliases={0: 0}, scratch=solve_scratch, flops=flops,
                )
        pending = exchange(fl, fh, fy, bk)
        if colour == 0:
            r, sol = call(
                own_change(bk, par, True), [r, c, weights], [state, state],
                aliases={0: 0}, scratch=[coarse, coarse], flops=flops,
            )
        else:
            r, sol = call(
                own_change(bk, par, False), [r, sol, c, weights], [state, state],
                aliases={0: 0, 1: 1}, scratch=[coarse, coarse], flops=flops,
            )
    whole = (right_side.shape, F32)
    (solution_out,) = call(leave(bk, None), [sol], [whole], hbm_out=True, flops=flops)

    def last(r_in, lo, hi, yy, gm, r_ref):
        ghosts(bk, (1, 1, 1), r_ref, None, gm, lo, hi, yy)

    (r,) = call(last, [r, *pending, couple], [state], aliases={0: 0})
    (residual_out,) = call(leave(bk, None), [r], [whole], hbm_out=True)
    return solution_out, residual_out


def exchange(fl, fh, fy, bk):
    below, above = shift(fh, "gx", 1), shift(fl, "gx", -1)
    if lax.axis_size("gy") == 2:
        ys = shift(fy, "gy", 1)
    else:
        n = bk.faces_y
        ys = jnp.concatenate([shift(fy[:n], "gy", -1), shift(fy[n:], "gy", 1)])
    return below, above, ys


def move_region(bk, before, par, r, sol, pending, couple, msg, state):
    to_home_y = before[1] == 0
    to_home_x = before[0] == 0 and par[0] == 1
    with_sol = before == (0, 0, 1)
    x_send = bk.face_x(-1, 1)
    x_home = bk.face_x(bk.ex - 1, 1)
    a = par[0]
    y_cells = bk.face_y(-1, a)
    sol_cells = [bk.tile(bk.ex - 1, bk.ey - 1, pz) for pz in range(2)]
    n_y = len(y_cells) + (2 if with_sol else 0)

    def finish(r_in, s_in, lo, hi, yy, gm, r_ref, s_ref, m_ref):
        ghosts(bk, before, r_ref, s_ref, gm, lo, hi, yy)
        if to_home_x:
            for m, t in enumerate(x_send):
                m_ref[m] = r_ref[t].astype(BF16)
        else:
            for m, t in enumerate(y_cells):
                m_ref[m] = r_ref[t].astype(BF16)
            if with_sol:
                for m, t in enumerate(sol_cells):
                    m_ref[len(y_cells) + m] = s_ref[t].astype(BF16)

    n_first = len(x_send) if to_home_x else n_y
    r, sol, m = call(
        finish, [r, sol, *pending, couple], [state, state, msg(n_first)], aliases={0: 0, 1: 1}
    )
    if to_home_x:
        m = shift(m, "gx", -1)

        def turn(r_in, m_in, r_ref, y_ref):
            for i, t in enumerate(x_home):
                r_ref[t] = m_in[i].astype(F32)
            for i, t in enumerate(y_cells):
                y_ref[i] = r_ref[t].astype(BF16)

        r, m = call(turn, [r, m], [state, msg(n_y)], aliases={0: 0})
    m = shift(m, "gy", -1 if to_home_y else 1)

    def place(r_in, s_in, m_in, r_ref, s_ref):
        for i, t in enumerate(y_cells):
            r_ref[t] = m_in[i].astype(F32)
        if with_sol:
            for i, t in enumerate(sol_cells):
                s_ref[t] = m_in[len(y_cells) + i].astype(F32)

    r, sol = call(place, [r, sol, m], [state, state], aliases={0: 0, 1: 1})
    return r, sol


def solution(mesh):
    placed = (P(None, "gx", "gy", "gz"), P("gx", "gy", "gz"), P(), P(), P())
    return jax.shard_map(
        on_device,
        mesh=mesh,
        in_specs=placed,
        out_specs=(P(None, "gx", "gy", "gz"), P(None, "gx", "gy", "gz")),
        check_vma=False,
    )
```

```python
import jax
import jax.numpy as jnp
from jax import lax
from jax.experimental import pallas as pl
from jax.experimental.pallas import tpu as pltpu
from jax.sharding import PartitionSpec as P

F32 = jnp.float32
BF16 = jnp.bfloat16
LANES = 128
VMEM_LIMIT = 28 * 1024 * 1024


class Block:
    def __init__(self, dofs, extent_x, extent_y, extent_z, rhs):
        assert extent_x % 2 == 0 and extent_y % 4 == 0 and extent_z * rhs == LANES
        self.q, self.ex, self.ey, self.ez, self.rhs = dofs, extent_x, extent_y, extent_z, rhs
        self.rows = -(-(dofs + 2) // 16) * 16
        self.sent = -(-(dofs + 2) // 8) * 8
        self.nx, self.ny = extent_x // 2, extent_y // 2
        self.tiles = extent_x * extent_y * 2
        self.own = LANES // 4
        self.half = LANES // 2
        self.faces_x = 2 * extent_y
        self.faces_y = 2 * extent_x

    def tile(self, x, y, pz):
        px, py = x % 2, y % 2
        sx, sy = (x // 2) % self.nx, (y // 2) % self.ny
        return (((px * 2 + py) * 2 + pz) * self.nx + sx) * self.ny + sy

    def span(self, parity, extent):
        return range(parity - 1, parity - 1 + extent)

    def face_x(self, x, b):
        return [self.tile(x, y, pz) for y in self.span(b, self.ey) for pz in range(2)]

    def face_y(self, y, a):
        return [self.tile(x, y, pz) for x in self.span(a, self.ex) for pz in range(2)]


def lane_iota(rows):
    return lax.broadcasted_iota(jnp.int32, (rows, LANES), 1)


def in_steps(count, page, each=4):
    def step(i, carry):
        for n in range(each):
            page(i * each + n)
        return carry

    lax.fori_loop(0, count // each, step, 0)


def weight(inside, rows):
    return jnp.broadcast_to(jnp.where(inside, 1.0, 0.0).astype(BF16), (rows, LANES))


def roll(v, by):
    by = by % LANES
    return pltpu.roll(v, by, 1) if by else v


def turned(v, by):
    return roll(v, by) if isinstance(by, int) else pltpu.roll(v, (by + LANES) % LANES, 1)


def dot(a, b):
    return jnp.dot(a, b, preferred_element_type=F32)


def call(body, ins, outs, aliases=None, scratch=(), flops=0, hbm_out=False, far_in=0, copies=0, vmem=VMEM_LIMIT):
    space = pl.BlockSpec(memory_space=pltpu.VMEM)
    far = pl.BlockSpec(memory_space=pltpu.HBM)
    if hbm_out:
        shapes = [jax.ShapeDtypeStruct(s, d) for s, d in outs]
    else:
        shapes = [pltpu.VMEM(s, d) for s, d in outs]
    return pl.pallas_call(
        body,
        in_specs=[far] * far_in + [space] * (len(ins) - far_in),
        out_specs=[far if hbm_out and copies else space] * len(outs),
        out_shape=shapes,
        scratch_shapes=[pltpu.VMEM(s, d) for s, d in scratch]
        + ([pltpu.SemaphoreType.DMA((copies,))] if copies else []),
        input_output_aliases=aliases or {},
        compiler_params=pltpu.CompilerParams(vmem_limit_bytes=vmem),
        cost_estimate=pl.CostEstimate(flops=flops, bytes_accessed=0, transcendentals=0) if flops else None,
    )(*ins)


def coef_row(bk, r_ref, t):
    return r_ref[t, bk.q : bk.q + 1, :] + r_ref[t, bk.q + 1 : bk.q + 2, :]


def shift(v, axis, distance):
    n = lax.axis_size(axis)
    return lax.ppermute(v, axis, [((i - distance) % n, i) for i in range(n)])


def shift2(v, first, d1, second, d2):
    n1, n2 = lax.axis_size(first), lax.axis_size(second)
    route = [
        (((i - d1) % n1) * n2 + (j - d2) % n2, i * n2 + j) for i in range(n1) for j in range(n2)
    ]
    return lax.ppermute(v, (first, second), route)


def pack(bk, r_ref, tiles, lanes_from, count, out_ref, parts):
    lane = lane_iota(bk.rows)
    for n in range(0, len(tiles), parts):
        total = None
        for k, t in enumerate(tiles[n : n + parts]):
            moved = roll(r_ref[t], k * count - lanes_from)
            total = moved if total is None else jnp.where(lane < k * count, total, moved)
        out_ref[n // parts] = total.astype(BF16)


def unpack(bk, msg_ref, n, lanes_to, count, parts):
    k = n % parts
    return roll(msg_ref[n // parts].astype(F32), lanes_to - k * count)


def prep_tables(bk):
    q, rows = bk.q, bk.rows

    def body(p_ref, m_ref, f_ref, o_ref, w_ref, g_ref, pick_ref):
        n = p_ref.shape[0]
        row = lax.broadcasted_iota(jnp.int32, (rows, n), 0)
        col = lax.broadcasted_iota(jnp.int32, (rows, n), 1)

        def build(o, carry):
            pick = jnp.where((col == row * 8 + o) & (row < q), 1.0, 0.0).astype(BF16)
            pick_ref[pl.ds(o * rows, rows), :] = pick
            return carry

        lax.fori_loop(0, 8, build, 0)

        def move(o, carry):
            at = pl.ds(o * rows, rows)
            left = dot(pick_ref[at, :], p_ref[...]).astype(BF16)
            o_ref[at, :] = lax.dot_general(
                left, pick_ref[...], (((1,), (1,)), ((), ())), preferred_element_type=F32
            ).astype(BF16)
            return carry

        lax.fori_loop(0, 8, move, 0)
        row = lax.broadcasted_iota(jnp.int32, (q, 7 * rows), 0)
        col = lax.broadcasted_iota(jnp.int32, (q, 7 * rows), 1)
        total = dot(m_ref[...].astype(BF16), jnp.where(col == row, 1.0, 0.0).astype(BF16))
        g_ref[...] = jnp.zeros_like(g_ref)
        w_ref[...] = jnp.zeros_like(w_ref)
        one = jnp.where(
            lax.broadcasted_iota(jnp.int32, (q, rows), 0) == lax.broadcasted_iota(jnp.int32, (q, rows), 1),
            1.0, 0.0,
        ).astype(BF16)
        for direction in range(3):
            face = f_ref[direction].astype(BF16)
            for side in range(2):
                at = rows * (1 + 2 * direction + side)
                place = jnp.where(col == row + at, 1.0, 0.0).astype(BF16)
                dims = (((1 - side,), (0,)), ((), ()))
                total = total - lax.dot_general(face, place, dims, preferred_element_type=F32)
                if direction < 2:
                    g_ref[2 * direction + side, :q, :] = lax.dot_general(
                        face, one, dims, preferred_element_type=F32
                    ).astype(BF16)
        w_ref[:q, :] = total.astype(BF16)

    return body


def prep_state(bk):
    def body(rs_ref, cc_ref, r_ref, y_ref, scr):
        rows = rs_ref.reshape(bk.q * bk.ex * bk.ey, LANES)
        src = lax.broadcasted_iota(jnp.int32, (2 * LANES, 2 * LANES), 0) % LANES
        dst = lax.broadcasted_iota(jnp.int32, (2 * LANES, 2 * LANES), 1)
        pz, lane = dst // LANES, dst % LANES - bk.own
        z = 2 * (lane // bk.rhs) + pz
        inside = (lane >= 0) & (lane < bk.half)
        split = jnp.where(inside & (src == z * bk.rhs + lane % bk.rhs), 1.0, 0.0).astype(BF16)
        zz = lax.broadcasted_iota(jnp.int32, (bk.ez, LANES), 0)
        ll = lax.broadcasted_iota(jnp.int32, (bk.ez, LANES), 1)
        spread = jnp.where(ll // bk.rhs == zz, 1.0, 0.0).astype(BF16)
        coef = cc_ref[...]
        high = coef.astype(BF16)
        low = (coef - high.astype(F32)).astype(BF16)
        high, low = dot(high, spread), dot(low, spread)
        scr[...] = jnp.zeros_like(scr)
        for x in range(bk.ex):
            for y in range(bk.ey):
                n = x * bk.ey + y
                scr[n % 4, : bk.q, :] = rows[pl.ds(n, bk.q, stride=bk.ex * bk.ey), :]
                scr[n % 4, bk.q : bk.q + 1, :] = high[n : n + 1]
                scr[n % 4, bk.q + 1 : bk.q + 2, :] = low[n : n + 1]
                raw = scr[n % 4]
                top = raw.astype(BF16)
                rest = (raw - top.astype(F32)).astype(BF16)
                out = dot(jnp.concatenate([top, rest], axis=1), split)
                r_ref[bk.tile(x, y, 0)] = out[:, :LANES]
                r_ref[bk.tile(x, y, 1)] = out[:, LANES:]
        tiles = [bk.tile(x, bk.ey - 1, pz) for x in range(bk.ex) for pz in range(2)]
        pack(bk, r_ref, tiles, bk.own, bk.half, y_ref, 2)

    return body


def halo_cells(bk):
    return [
        bk.tile(x, y, pz)
        for x in range(bk.ex - 1)
        for y in bk.span(0, bk.ey)
        for pz in range(2)
    ]


def prep_halo(bk):
    def body(r_in, y_ref, r_ref, zl_ref, zh_ref, x_ref, xl_ref, xh_ref):
        n = 0
        for x in range(bk.ex):
            for pz in range(2):
                r_ref[bk.tile(x, -1, pz)] = unpack(bk, y_ref, n, bk.own, bk.half, 2)
                n += 1
        cells = halo_cells(bk)
        pack(bk, r_ref, cells, bk.own, bk.own, zl_ref, 4)
        pack(bk, r_ref, cells, 2 * bk.own, bk.own, zh_ref, 4)
        edge = bk.face_x(bk.ex - 1, 0)
        pack(bk, r_ref, edge, bk.own, bk.half, x_ref, 2)
        pack(bk, r_ref, edge, bk.own, bk.own, xl_ref, 4)
        pack(bk, r_ref, edge, 2 * bk.own, bk.own, xh_ref, 4)

    return body


def fill_halo(bk, r_ref, zl_ref, zh_ref, x_ref, xl_ref, xh_ref):
    lane = lane_iota(bk.rows)
    below, above = lane < bk.own, lane >= 3 * bk.own

    def joined(own, low_ref, high_ref, n):
        low = unpack(bk, low_ref, n, 0, bk.own, 4)
        high = unpack(bk, high_ref, n, 3 * bk.own, bk.own, 4)
        return jnp.where(below, low, jnp.where(above, high, own))

    for n, t in enumerate(halo_cells(bk)):
        r_ref[t] = joined(r_ref[t], zl_ref, zh_ref, n)
    for n, t in enumerate(bk.face_x(-1, 0)):
        r_ref[t] = joined(unpack(bk, x_ref, n, bk.own, bk.half, 2), xl_ref, xh_ref, n)


def solve(bk, colour, r_ref, p_ref, c_ref, xl_ref, xh_ref, y_ref, xs_ref):
    a, b, g = colour
    back = bk.rhs
    n = 0
    for px in range(bk.nx):
        for py in range(0, bk.ny, 2):
            cells = []
            for half in range(2):
                for o in range(8):
                    x = a - 1 + 2 * px + o // 4
                    y = b - 1 + 2 * (py + half) + o // 2 % 2
                    pz = o % 2 if g else 1 - o % 2
                    t = bk.tile(x, y, pz)
                    scale = lax.rsqrt(coef_row(bk, r_ref, t))
                    scaled = r_ref[t] * scale
                    if g == 0 and pz == 1:
                        scaled = roll(scaled, back)
                    lanes = slice(half * LANES, (half + 1) * LANES)
                    xs_ref[n, o * bk.rows : (o + 1) * bk.rows, lanes] = scaled.astype(BF16)
                    cells.append((half, o, t, scale, g == 0 and pz == 1))
            solved = dot(p_ref[...], xs_ref[n])
            for half, o, t, scale, moved in cells:
                v = solved[o * bk.rows : (o + 1) * bk.rows, half * LANES : (half + 1) * LANES]
                if moved:
                    v = roll(v, -back)
                c_ref[t] = (v * scale).astype(BF16)
            n += 1
    for m, t in enumerate(bk.face_x(a - 1, b)):
        xl_ref[m] = c_ref[t]
    for m, t in enumerate(bk.face_x(a - 2 + bk.ex, b)):
        xh_ref[m] = c_ref[t]
    for m, t in enumerate(bk.face_y(b - 1, a) + bk.face_y(b - 2 + bk.ey, a)):
        y_ref[m] = c_ref[t]


def ghosts(bk, colour, r_ref, sol_ref, g_ref, from_below, from_above, y_ref):
    a, b, g = colour

    def add(matrix, tiles, ghost_ref, base):
        for m in range(0, len(tiles), 2):
            two = jnp.concatenate([ghost_ref[base + m], ghost_ref[base + m + 1]], axis=1)
            change = dot(g_ref[matrix], two)
            r_ref[tiles[m]] += change[:, :LANES]
            r_ref[tiles[m + 1]] += change[:, LANES:]

    add(0, bk.face_x(a - 2 + bk.ex, b), from_above, 0)
    add(1, bk.face_x(a - 1, b), from_below, 0)
    add(2, bk.face_y(b - 2 + bk.ey, a), y_ref, 0)
    add(3, bk.face_y(b - 1, a), y_ref, bk.faces_y)
    if a == 0:
        for m, t in enumerate(bk.face_x(bk.ex - 1, b)):
            sol_ref[t] += from_above[m].astype(F32)
    if b == 0:
        m = 0
        for x in bk.span(a, bk.ex):
            for pz in range(2):
                if x >= 0:
                    sol_ref[bk.tile(x, bk.ey - 1, pz)] += y_ref[m].astype(F32)
                m += 1


def own_change(bk, colour, first):
    a, b, g = colour

    def body(*refs):
        if first:
            r_in, c_ref, w_ref, r_ref, sol_ref, cm_ref, cz_ref = refs
        else:
            r_in, sol_in, c_ref, w_ref, r_ref, sol_ref, cm_ref, cz_ref = refs
        xs, ys = bk.span(a, bk.ex), bk.span(b, bk.ey)
        for x in xs:
            for y in ys:
                for pz in range(2):
                    t = bk.tile(x, y, pz)
                    c = c_ref[t].astype(F32)
                    cm_ref[t] = (c * coef_row(bk, r_ref, t)).astype(BF16)
                    cz_ref[t] = roll(c_ref[t], bk.rhs if pz else -bk.rhs)
                    if x >= 0 and y >= 0:
                        sol_ref[t] = c if first else sol_ref[t] + c
                    elif first:
                        sol_ref[t] = jnp.zeros_like(c)
        nothing = jnp.zeros((bk.rows, LANES), BF16)

        def at(x, y, pz):
            return c_ref[bk.tile(x, y, pz)] if x in xs and y in ys else nothing

        def stack(x, y, pz):
            other = bk.tile(x, y, 1 - pz)
            near, far = c_ref[other], cz_ref[other]
            return jnp.concatenate(
                [
                    cm_ref[bk.tile(x, y, pz)],
                    at(x + 1, y, pz),
                    at(x - 1, y, pz),
                    at(x, y + 1, pz),
                    at(x, y - 1, pz),
                    far if pz else near,
                    near if pz else far,
                ],
                axis=0,
            )

        for x in xs:
            for y in ys:
                both = jnp.concatenate([stack(x, y, 0), stack(x, y, 1)], axis=1)
                change = dot(w_ref[...], both)
                for pz in range(2):
                    r_ref[bk.tile(x, y, pz)] -= change[:, pz * LANES : (pz + 1) * LANES]

    return body


def leave(bk, ref):
    def body(tile_ref, out_ref):
        rows = out_ref.reshape(bk.q * bk.ex * bk.ey, LANES)
        src = lax.broadcasted_iota(jnp.int32, (2 * LANES, LANES), 0)
        dst = lax.broadcasted_iota(jnp.int32, (2 * LANES, LANES), 1)
        pz, lane = src // LANES, src % LANES - bk.own
        z = 2 * (lane // bk.rhs) + pz
        inside = (lane >= 0) & (lane < bk.half)
        join = jnp.where(inside & (dst == z * bk.rhs + lane % bk.rhs), 1.0, 0.0).astype(BF16)
        for x in range(bk.ex):
            for y in range(bk.ey):
                both = jnp.concatenate(
                    [tile_ref[bk.tile(x, y, 0)], tile_ref[bk.tile(x, y, 1)]], axis=1
                )
                top = both.astype(BF16)
                rest = (both - top.astype(F32)).astype(BF16)
                out = dot(top, join) + dot(rest, join)
                rows[pl.ds(x * bk.ey + y, bk.q, stride=bk.ex * bk.ey), :] = out[: bk.q]

    return body


class Slab:
    def __init__(self, bk, count):
        self.bk, self.count = bk, count
        self.q, self.rhs, self.rows, self.ny = bk.q, bk.rhs, bk.rows, bk.ny
        self.sent = bk.sent
        self.ey = bk.ey
        self.groups = count
        self.width = LANES // count
        self.depth = bk.ez // count
        self.halo = 2 * bk.rhs
        self.tiles = bk.tiles

    @staticmethod
    def fits(bk, count):
        depth = bk.ez // count
        return (
            bk.ez % count == 0
            and depth % 2 == 0
            and bk.nx == 2
            and (depth // 2 + 4) * bk.rhs * count == LANES
            and bk.tiles % 16 == 0
        )

    def tile(self, px, x2, y, pz):
        return (((px * 2 + y % 2) * 2 + pz) * 2 + x2) * self.ny + (y // 2) % self.ny

    def face_y(self, y):
        return [self.tile(px, x2, y, pz) for px in range(2) for x2 in range(2) for pz in range(2)]

    def edge(self, n, low_side):
        pz = n // (2 * self.ny) % 2
        index = n // (4 * self.ny) * (2 * self.ny // self.groups) + n % (2 * self.ny) // self.groups
        pairs = (2 if pz else 3) if low_side else (2 if pz else 1)
        each = {1: 8, 2: 4, 3: 2}[pairs]
        base = 0 if pz else self.tiles // (2 * self.groups) // 4
        return base + index // each, index % each * (self.width // each), pairs * self.rhs

    def pages(self, low_side):
        return 1 + max(self.edge(n, low_side)[0] for n in range(0, self.tiles, self.groups))

    def place(self, device):
        slab = device * 0
        for s, d in enumerate(self.order()):
            slab = jnp.where(device == d, s, slab)
        return slab

    def order(self):
        return [0, 1, 3, 2] if self.count == 4 else list(range(self.count))


def home_prep(bk, sb):
    def body(rs_ref, cc_ref, h_ref, up_ref, down_ref, scr, high_ref, low_ref, in_ref, cin_ref, sems):
        copies = [
            pltpu.make_async_copy(rs_ref.at[:, x], in_ref.at[x], sems.at[x]) for x in range(bk.ex)
        ]
        coefs = pltpu.make_async_copy(cc_ref, cin_ref, sems.at[bk.ex])
        coefs.start()
        for c in copies:
            c.start()
        src = lax.broadcasted_iota(jnp.int32, (LANES, 2 * LANES), 0)
        dst = lax.broadcasted_iota(jnp.int32, (LANES, 2 * LANES), 1)
        pz, lane = dst // LANES, dst % LANES - bk.own
        z = 2 * (lane // bk.rhs) + pz
        inside = (lane >= 0) & (lane < bk.half)
        split = jnp.where(inside & (src == z * bk.rhs + lane % bk.rhs), 1.0, 0.0).astype(BF16)
        zz = lax.broadcasted_iota(jnp.int32, (bk.ez, LANES), 0)
        ll = lax.broadcasted_iota(jnp.int32, (bk.ez, LANES), 1)
        spread = jnp.where(ll // bk.rhs == zz, 1.0, 0.0).astype(BF16)
        coefs.wait()
        coef = cin_ref[...]
        high = coef.astype(BF16)
        low = (coef - high.astype(F32)).astype(BF16)
        high_ref[...], low_ref[...] = dot(high, spread), dot(low, spread)
        scr[...] = jnp.zeros_like(scr)

        for x in range(bk.ex):
            copies[x].wait()
            rows = in_ref.at[x].reshape(bk.q * bk.ey, LANES)

            def column(half, carry, x=x, rows=rows):
                for i in range(bk.ey // 2):
                    y = half + 2 * i
                    n = x * bk.ey + y
                    scr[i, : bk.q, :] = rows[pl.ds(y, bk.q, stride=bk.ey), :]
                    scr[i, bk.q : bk.q + 1, :] = high_ref[pl.ds(n, 1), :]
                    scr[i, bk.q + 1 : bk.q + 2, :] = low_ref[pl.ds(n, 1), :]
                    out = dot(scr[i].astype(BF16), split)
                    h_ref[bk.tile(x, y, 0)] = out[:, :LANES].astype(BF16)
                    h_ref[bk.tile(x, y, 1)] = out[:, LANES:].astype(BF16)
                return carry

            for half in range(2):
                column(half, 0)
        lane = lane_iota(1)
        for ref, low_side in ((up_ref, False), (down_ref, True)):
            for n in range(0, bk.tiles, sb.groups):
                page, slot, width = sb.edge(n, low_side)
                start = bk.own if low_side else bk.own + bk.half - width
                total = ref[page] if slot else None
                for k in range(sb.groups):
                    at = k * sb.width + slot
                    inside = weight((lane >= at) & (lane < at + width), sb.sent)
                    v = roll(h_ref[n + k, : sb.sent], at - start) * inside
                    total = v if total is None else total + v
                ref[page] = total

    return body


def scatter(sb):
    bk, parts, rows = sb.bk, sb.groups, sb.sent

    def body(h_ref, below_ref, above_ref, *outs):
        lane = lane_iota(1)
        me = lax.axis_index("gx")
        step = bk.half // parts
        keep, slabs = [], []
        for d in range(parts):
            slab = sb.place((me + d) % parts)
            slabs.append(slab)
            group = (lane - slab * step + LANES) % LANES // sb.width
            keep.append([weight(group == (me + k) % parts, rows) for k in range(parts)])
        ends = {}
        for pz in range(2):
            for low_side in range(2):
                pairs = sb.edge(0 if not pz else 2 * sb.ny, not low_side)[2]
                if low_side:
                    inside, end = lane % sb.width < pairs, 0
                else:
                    at = (lane - step * (parts - 1) + LANES) % LANES
                    inside, end = at % sb.width >= sb.width - pairs, parts - 1
                for d in range(parts):
                    chosen = jnp.where(inside, jnp.where(slabs[d] == end, 1, 0), 0)
                    ends[pz, low_side, d] = weight(chosen == 1, rows)
        for n in range(0, sb.tiles, parts):
            totals = [None] * parts
            pz = n // (2 * sb.ny) % 2
            for k in range(parts):
                start = bk.own - (2 if pz else 1) * bk.rhs
                by = ((me + k) % parts * sb.width - start + LANES) % LANES
                v = pltpu.roll(h_ref[n + k, :rows], by, 1)
                for d in range(parts):
                    totals[d] = v * keep[d][k] if k == 0 else totals[d] + v * keep[d][k]
            page, slot, width = sb.edge(n, False)
            low = pltpu.roll(below_ref[page], (me * sb.width - slot + LANES) % LANES, 1)
            page, slot, width = sb.edge(n, True)
            by = me * sb.width + step * (parts - 1) + sb.width - width - slot
            high = pltpu.roll(above_ref[page], (by + LANES) % LANES, 1)
            for d, out in enumerate(outs):
                out[n // parts] = totals[d] + low * ends[pz, 1, d] + high * ends[pz, 0, d]

    return body


def gather_state(sb, parts_refs, r_ref):
    parts, rows = sb.groups, sb.sent
    me = lax.axis_index("gx")
    by = sb.place(me) * (sb.bk.half // parts)
    group = (lane_iota(1) - by + LANES) % LANES // sb.width
    keep = [
        [weight(group == (me - d + parts + k) % parts, rows) for d in range(parts)]
        for k in range(parts)
    ]

    def page(n):
        for k in range(parts):
            total = parts_refs[0][n] * keep[k][0]
            for d in range(1, parts):
                total = total + parts_refs[d][n] * keep[k][d]
            total = pltpu.roll(total, (2 * LANES - k * sb.width - by) % LANES, 1)
            r_ref[n * parts + k, :rows] = total.astype(F32)
            r_ref[n * parts + k, rows:] = jnp.zeros((sb.rows - rows, LANES), F32)

    in_steps(sb.tiles // parts, page)


def slab_solve(sb, colour, r_ref, p_ref, c_ref, y_ref, xs_ref, part=None):
    a, b, g = colour
    rows = sb.rows

    def column(x2, carry):
        for n, py in enumerate(range(0, sb.ny, 2)):
            if part is not None and n not in part:
                continue
            cells = []
            for half in range(2):
                for o in range(8):
                    xo, y = o // 4, b - 1 + 2 * (py + half) + o // 2 % 2
                    pz = o % 2 if g else 1 - o % 2
                    moved = -sb.rhs if g == 1 and pz == 1 else 0
                    if a or xo == 1:
                        t = sb.tile(xo if a else 0, x2, y, pz)
                    else:
                        t = sb.tile(1, 1 - x2, y, pz)
                        moved = moved + (1 - x2) * sb.width
                    scale = lax.rsqrt(coef_row(sb, r_ref, t))
                    lanes = slice(half * LANES, (half + 1) * LANES)
                    xs_ref[n, o * rows : (o + 1) * rows, lanes] = turned(
                        r_ref[t] * scale, moved
                    ).astype(BF16)
                    cells.append((half, o, t, scale, moved))
            solved = dot(p_ref[...], xs_ref[n])
            for half, o, t, scale, moved in cells:
                v = solved[o * rows : (o + 1) * rows, half * LANES : (half + 1) * LANES]
                c_ref[t] = (turned(v, -moved) * scale).astype(BF16)
        return carry

    if part is None:
        lax.fori_loop(0, 2, column, 0)
    else:
        for x2 in range(2):
            column(x2, 0)
    if y_ref is None:
        return
    for m, t in enumerate(sb.face_y(b - 1) + sb.face_y(b - 2 + sb.ey)):
        y_ref[m] = c_ref[t]


def slab_ghosts(sb, colour, r_ref, sol_ref, g_ref, y_ref):
    a, b, g = colour
    count = len(sb.face_y(0))
    for matrix, y, base in ((2, b - 2 + sb.ey, 0), (3, b - 1, count)):
        tiles = sb.face_y(y)
        for m in range(0, count, 2):
            two = jnp.concatenate([y_ref[base + m], y_ref[base + m + 1]], axis=1)
            change = dot(g_ref[matrix], two)
            r_ref[tiles[m]] += change[:, :LANES]
            r_ref[tiles[m + 1]] += change[:, LANES:]
    if b == 0:
        for m, t in enumerate(sb.face_y(sb.ey - 1)):
            sol_ref[t] += y_ref[m].astype(F32)


def slab_change(sb, colour, first, last=False):
    a, b, g = colour

    def body(*refs):
        if last:
            r_in, c_ref, w_ref, r_ref, cm_ref, cz_ref, cx_ref = refs
        elif first:
            r_in, c_ref, w_ref, r_ref, sol_ref, cm_ref, cz_ref, cx_ref = refs
        else:
            r_in, sol_in, c_ref, w_ref, r_ref, sol_ref, cm_ref, cz_ref, cx_ref = refs
        ys = sb.bk.span(b, sb.ey)
        cells = [(px, x2, y) for px in range(2) for x2 in range(2) for y in ys]
        for px, x2, y in cells:
            for pz in range(2):
                t = sb.tile(px, x2, y, pz)
                c = c_ref[t].astype(F32)
                cm_ref[t] = (c * coef_row(sb, r_ref, t)).astype(BF16)
                cz_ref[t] = roll(c_ref[t], -sb.rhs if pz else sb.rhs)
                if px == x2:
                    cx_ref[t] = roll(c_ref[t], sb.width if px else -sb.width)
                if last:
                    continue
                if y >= 0:
                    sol_ref[t] = c if first else sol_ref[t] + c
                elif first:
                    sol_ref[t] = jnp.zeros_like(c)
        nothing = jnp.zeros((sb.rows, LANES), BF16)

        def stack(px, x2, y, pz):
            beside = c_ref[sb.tile(1 - px, x2, y, pz)]
            across = (cx_ref if px == x2 else c_ref)[sb.tile(1 - px, 1 - x2, y, pz)]
            other = sb.tile(px, x2, y, 1 - pz)
            near, far = c_ref[other], cz_ref[other]
            return jnp.concatenate(
                [
                    cm_ref[sb.tile(px, x2, y, pz)],
                    across if px else beside,
                    beside if px else across,
                    c_ref[sb.tile(px, x2, y + 1, pz)] if y + 1 in ys else nothing,
                    c_ref[sb.tile(px, x2, y - 1, pz)] if y - 1 in ys else nothing,
                    near if pz else far,
                    far if pz else near,
                ],
                axis=0,
            )

        for px, x2, y in cells:
            both = jnp.concatenate([stack(px, x2, y, 0), stack(px, x2, y, 1)], axis=1)
            change = dot(w_ref[...], both)
            for pz in range(2):
                r_ref[sb.tile(px, x2, y, pz)] -= change[:, pz * LANES : (pz + 1) * LANES]

    return body


def emit_halo(sb, r_ref, up_ref, down_ref):
    rows = sb.sent
    lane = lane_iota(rows) % sb.width
    top = sb.width - 2 * sb.halo
    parts = sb.width // sb.halo

    def page(n):
        for ref, start in ((up_ref, top), (down_ref, sb.halo)):
            total = None
            for k in range(parts):
                moved = roll(r_ref[n * parts + k, :rows], k * sb.halo - start)
                total = moved if k == 0 else jnp.where(lane < k * sb.halo, total, moved)
            ref[n] = total.astype(BF16)

    in_steps(sb.tiles // parts, page)


def fill_slab_halo(sb, r_ref, below_ref, above_ref):
    rows = sb.sent
    lane = lane_iota(rows) % sb.width
    parts = sb.width // sb.halo

    def page(n):
        for k in range(parts):
            t = n * parts + k
            low = roll(below_ref[n].astype(F32), -k * sb.halo)
            high = roll(above_ref[n].astype(F32), sb.width - sb.halo - k * sb.halo)
            own = jnp.where(lane < sb.halo, low, r_ref[t, :rows])
            r_ref[t, :rows] = jnp.where(lane >= sb.width - sb.halo, high, own)

    in_steps(sb.tiles // parts, page)


def collect(sb, source, outs, extras, extra_at):
    width = sb.width - 2 * sb.halo
    parts = LANES // width
    rows = sb.sent
    lane = lane_iota(rows)
    piece = lane_iota(1) // width
    me = lax.axis_index("gx")
    slab = sb.place(me)
    offset = sb.bk.own // width
    keep = [
        [
            weight(piece == (offset + slab + k + 2 * ((me + d) % sb.groups)) % parts, rows)
            for k in range(parts)
        ]
        for d in range(len(outs))
    ]
    def page(n):
        totals = [None] * len(outs)
        for k in range(parts):
            by = (offset + slab + k) * width - sb.halo
            v = pltpu.roll(source[n * parts + k, :rows].astype(BF16), by % LANES, 1)
            for d in range(len(outs)):
                totals[d] = v * keep[d][k] if k == 0 else totals[d] + v * keep[d][k]
        for d, out in enumerate(outs):
            out[n] = totals[d]

    if outs:
        in_steps(sb.tiles // parts, page)
    per = sb.width // sb.rhs
    evens = even_tiles(sb)
    joined = []
    for m in range(sb.groups if extras else 0):
        total = None
        for k, t in enumerate(evens[m * per : (m + 1) * per]):
            v = roll(source[t, :rows].astype(BF16), k * sb.rhs - (sb.width - sb.halo - sb.rhs))
            total = v if k == 0 else jnp.where(lane % sb.width < k * sb.rhs, total, v)
        joined.append(roll(total, m * sb.width))
    for u, out in enumerate(extras):
        total = joined[0]
        for m in range(1, sb.groups):
            total = jnp.where(lane // sb.width == (u + m) % sb.groups, joined[m], total)
        out[extra_at] = total


def even_tiles(sb):
    return [t for t in range(sb.tiles) if t // (2 * sb.ny) % 2 == 0]


def deliver(sb):
    bk = sb.bk
    width = sb.width - 2 * sb.halo
    parts = LANES // width
    per = sb.width // sb.rhs

    def body(*refs):
        count = sb.groups
        both_ins = (refs[:count], refs[count : 2 * count])
        extras, outs = refs[2 * count : 3 * count], refs[3 * count : 3 * count + 2]
        buffer, sems = refs[3 * count + 2 :]
        rows_sent = sb.sent
        lane = lane_iota(1)
        piece = lane // width
        first = weight((lane >= bk.own) & (lane < bk.own + bk.rhs), rows_sent)
        later = 1 - first
        src = lax.broadcasted_iota(jnp.int32, (2 * LANES, LANES), 0)
        dst = lax.broadcasted_iota(jnp.int32, (2 * LANES, LANES), 1)
        pz, at = src // LANES, src % LANES - bk.own
        z = 2 * (at // bk.rhs) + pz
        inside = (at >= 0) & (at < bk.half)
        join = jnp.where(inside & (dst == z * bk.rhs + at % bk.rhs), 1.0, 0.0).astype(BF16)
        me = lax.axis_index("gx")
        slabs = [sb.place((me - d + sb.groups) % sb.groups) for d in range(sb.groups)]
        keep = [
            [weight(piece == (bk.own // width + s + k + 2 * me) % parts, rows_sent) for s in slabs]
            for k in range(parts)
        ]
        evens = even_tiles(sb)
        def copy_of(index, x):
            return pltpu.make_async_copy(
                buffer.at[index, x], outs[index].at[:, x], sems.at[index * bk.ex + x]
            )

        for index in range(2):
            ins = both_ins[index]
            layer = extras[0][index]
            for e in extras[1:]:
                layer = layer + e[index]

            def home(t, k, even, ins=ins, layer=layer):
                page = t // parts
                total = ins[0][page] * keep[k][0]
                for d in range(1, sb.groups):
                    total = total + ins[d][page] * keep[k][d]
                by = (3 * LANES - (k + 2 * me) * width + (bk.rhs if even else 0)) % LANES
                total = pltpu.roll(total, by, 1)
                if not even:
                    return total
                n = t // (2 * parts) * parts + k
                by = (bk.own + 3 * LANES - (me + n // per) * sb.width - n % per * sb.rhs) % LANES
                return first * pltpu.roll(layer, by, 1) + later * total

            def columns(px, carry, index=index, home=home):
                for sx in range(bk.nx):
                    x = 2 * sx + px
                    rows = buffer.at[index, x].reshape(bk.q * bk.ey, LANES)
                    for y in range(bk.ey):
                        t = bk.tile(x, y, 0)
                        k = sx * bk.ny + y // 2
                        both = jnp.concatenate(
                            [home(t, k, True), home(t + parts, k, False)], axis=1
                        )
                        out = dot(both, join)
                        rows[pl.ds(y, bk.q, stride=bk.ey), :] = out[: bk.q]
                    copy_of(index, x).start()
                return carry

            lax.fori_loop(0, 2, columns, 0)
        for index in range(2):
            for x in range(bk.ex):
                copy_of(index, x).wait()

    return body


def in_slabs(bk, sb, right_side, cell_coef, inverse, couple, weights):
    count, order = sb.count, sb.order()
    square = (sb.rows, LANES)
    state = ((sb.tiles,) + square, F32)
    coarse = ((sb.tiles,) + square, BF16)
    faces = ((2 * len(sb.face_y(0)),) + square, BF16)
    one_face = (((len(sb.face_y(0)),) + square), BF16)

    def msg(n):
        return ((n,) + square, BF16)

    def sent(n):
        return ((n, sb.sent, LANES), BF16)

    spread = ((bk.ex * bk.ey, LANES), F32)
    home, up, down = call(
        home_prep(bk, sb), [right_side, cell_coef.reshape(bk.ex * bk.ey, bk.ez)],
        [coarse, sent(sb.pages(False)), sent(sb.pages(True))],
        scratch=[
            ((bk.ey // 2,) + square, F32), spread, spread,
            ((bk.ex, bk.q, bk.ey, LANES), F32), ((bk.ex * bk.ey, bk.ez), F32),
        ],
        far_in=2, copies=bk.ex + 1, vmem=64_600_000,
    )
    below, above = shift(up, "gz", 1), shift(down, "gz", -1)
    pieces = call(scatter(sb), [home, below, above], [sent(sb.tiles // count)] * count)
    pieces = [shift(p, "gx", d) if d else p for d, p in enumerate(pieces)]

    def chain(v, step):
        n = lax.axis_size("gz")
        route = []
        for z in range(n):
            for s in range(count):
                total = (z * count + s + step) % (n * count)
                route.append((order[s] * n + z, order[total % count] * n + total // count))
        return lax.ppermute(v, ("gx", "gz"), route)

    def swap(v, step):
        return shift(v, "gy", step)

    edge = sb.face_y(-1)

    def assemble(*refs):
        r_ref, y_ref = refs[count + 1 :]
        gather_state(sb, refs[:count], r_ref)
        for m, t in enumerate(edge):
            y_ref[m] = r_ref[t].astype(BF16)

    r, moved = call(assemble, pieces + [inverse], [state, one_face])
    moved = swap(moved, 1)
    sol = halos = pending = None
    flops = 1 << 27
    solve_scratch = [((sb.ny // 2, 8 * sb.rows, 2 * LANES), BF16)]
    halo_msg = sent(sb.tiles * sb.halo // sb.width)
    refresh = (3,)

    for colour in range(8):
        par = (colour // 4, colour // 2 % 2, colour % 2)
        before = ((colour - 1) // 4, (colour - 1) // 2 % 2, (colour - 1) % 2)
        fresh = (colour - 1) in refresh
        turn = colour > 0 and par[1] != before[1]
        assert turn or not fresh
        if turn:

            def finish(r_in, s_in, yy, gm, r_ref, s_ref, *outs, before=before, fresh=fresh):
                slab_ghosts(sb, before, r_ref, s_ref, gm, yy)
                if not fresh:
                    for m, t in enumerate(edge):
                        outs[0][m] = r_ref[t].astype(BF16)
                else:
                    emit_halo(sb, r_ref, *outs)

            outs = [halo_msg, halo_msg] if fresh else [one_face]
            r, sol, *out = call(
                finish, [r, sol, pending, couple], [state, state] + outs, aliases={0: 0, 1: 1}
            )
            if fresh:
                halos = [chain(out[0], 1), chain(out[1], -1)]

                def fill(r_in, lo, hi, r_ref, y_ref):
                    fill_slab_halo(sb, r_ref, lo, hi)
                    for m, t in enumerate(edge):
                        y_ref[m] = r_ref[t].astype(BF16)

                r, *out = call(fill, [r, *halos], [state, one_face], aliases={0: 0})
            moved = swap(out[0], -1 if before[1] == 0 else 1)
            args, body = [r, moved, inverse], None
        elif colour == 0:
            args, body = [r, moved, inverse], None
        else:

            def solve_next(r_in, s_in, yy, gm, p, r_ref, s_ref, c, fy, xs, par=par, before=before):
                slab_ghosts(sb, before, r_ref, s_ref, gm, yy)
                slab_solve(sb, par, r_ref, p, c, fy, xs)

            args, body = [r, sol, pending, couple, inverse], solve_next
        if body is None:
            pages = sb.ny // 2
            late = [0] if par[1] == 0 else [pages - 1]

            def early(r_ref, p, c, xs, par=par, late=late):
                slab_solve(sb, par, r_ref, p, c, None, xs, [n for n in range(pages) if n not in late])

            (c,) = call(early, [r, inverse], [coarse], scratch=solve_scratch, flops=flops)

            def body(r_in, m_in, p, c_in, r_ref, c, fy, xs, par=par, late=late):
                for m, t in enumerate(edge):
                    r_ref[t] = m_in[m].astype(F32)
                slab_solve(sb, par, r_ref, p, c, fy, xs, late)

            args = args + [c]

        with_sol = len(args) == 5
        split = body.__name__ == "body"
        kept = [state, state] if with_sol else [state]
        got = call(
            body, args, kept + [coarse, faces], scratch=solve_scratch, flops=flops,
            aliases={0: 0, 1: 1} if with_sol else ({0: 0, 3: 1} if split else {0: 0}),
        )
        if with_sol:
            r, sol, c, fy = got
        else:
            r, c, fy = got
        if lax.axis_size("gy") == 2:
            pending = swap(fy, 1)
        else:
            n = len(edge)
            pending = jnp.concatenate([swap(fy[:n], -1), swap(fy[n:], 1)])
        if colour == 7:

            def finished(s_in, c_ref, s_ref, *outs):

                def page(t):
                    s_ref[t] += c_ref[t].astype(F32)

                in_steps(sb.tiles, page, 16)
                collect(sb, s_ref, outs, [], 0)

            each = sent(sb.tiles * (sb.depth // 2 * sb.rhs) // LANES)
            sol, *sol_parts = call(finished, [sol, c], [state] + [each] * count, aliases={0: 0}, flops=flops)
            sol_parts = [shift(p, "gx", d) if d else p for d, p in enumerate(sol_parts)]
            (r,) = call(
                slab_change(sb, par, False, True), [r, c, weights], [state], flops=flops,
                aliases={0: 0}, scratch=[coarse, coarse, coarse],
            )
            continue
        ins = [r, c, weights] if colour == 0 else [r, sol, c, weights]
        r, sol = call(
            slab_change(sb, par, colour == 0), ins, [state, state], flops=flops,
            aliases={0: 0} if colour == 0 else {0: 0, 1: 1}, scratch=[coarse, coarse, coarse],
        )

    def last(r_in, sol_ref, yy, gm, r_ref, *outs):
        slab_ghosts(sb, (1, 1, 1), r_ref, None, gm, yy)
        collect(sb, sol_ref, [], outs[count:], 0)
        collect(sb, r_ref, outs[:count], outs[count:], 1)

    r, *parts = call(
        last, [r, sol, pending, couple], [state] + [each] * count + [sent(2)] * count, aliases={0: 0}
    )

    def next_block(v, to):
        n = lax.axis_size("gz")
        return lax.ppermute(
            v, ("gx", "gz"), [(order[-1] * n + z, to * n + (z + 1) % n) for z in range(n)]
        )

    extras = [next_block(v, u) for u, v in enumerate(parts[count:])]
    parts = [shift(p, "gx", d) if d else p for d, p in enumerate(parts[:count])]
    whole = (right_side.shape, F32)
    return tuple(
        call(
            deliver(sb), sol_parts + parts + extras, [whole, whole], hbm_out=True,
            scratch=[((2, bk.ex, bk.q, bk.ey, LANES), F32)], copies=2 * bk.ex,
        )
    )


def on_device(right_side, cell_coef, cell_matrix, face_coupling, patch_inverse):
    dofs = cell_matrix.shape[0]
    ex, ey, ez = cell_coef.shape
    bk = Block(dofs, ex, ey, ez, right_side.shape[3] // ez)
    rows, tiles = bk.rows, bk.tiles
    square = (rows, LANES)

    state = ((tiles,) + square, F32)
    coarse = ((tiles,) + square, BF16)
    face_x, face_y = ((bk.faces_x,) + square, BF16), ((2 * bk.faces_y,) + square, BF16)

    def msg(n):
        return ((n,) + square, BF16)

    inverse, weights, couple = call(
        prep_tables(bk), [patch_inverse, cell_matrix, face_coupling],
        [((8 * rows, 8 * rows), BF16), ((rows, 7 * rows), BF16), ((4, rows, rows), BF16)],
        scratch=[((8 * rows, patch_inverse.shape[0]), BF16)], flops=1 << 30,
    )
    if Slab.fits(bk, lax.axis_size("gx")):
        sb = Slab(bk, lax.axis_size("gx"))
        return in_slabs(bk, sb, right_side, cell_coef, inverse, couple, weights)

    r, ymsg = call(
        prep_state(bk), [right_side, cell_coef.reshape(ex * ey, ez)], [state, msg(ex)],
        scratch=[((4,) + square, F32)],
    )
    ymsg = shift(ymsg, "gy", 1)
    edge = 2 * ey
    inner = len(halo_cells(bk))
    r, zl, zh, xm, xl, xh = call(
        prep_halo(bk), [r, ymsg],
        [state, msg(inner // 4), msg(inner // 4), msg(edge // 2), msg(edge // 4), msg(edge // 4)],
        aliases={0: 0},
    )
    halo = (
        shift(zh, "gz", 1),
        shift(zl, "gz", -1),
        shift(xm, "gx", 1),
        shift2(xh, "gx", 1, "gz", 1),
        shift2(xl, "gx", 1, "gz", -1),
    )
    solve_scratch = [((bk.nx * bk.ny // 2, 8 * rows, 2 * LANES), BF16)]
    solve_outs = [coarse, face_x, face_x, face_y]
    flops = 1 << 27
    sol = None
    pending = None
    for colour in range(8):
        par = (colour // 4, colour // 2 % 2, colour % 2)
        if colour == 0:

            def body(r_in, zl, zh, xm, xl, xh, p, r_ref, c, fl, fh, fy, xs):
                fill_halo(bk, r_ref, zl, zh, xm, xl, xh)
                solve(bk, (0, 0, 0), r_ref, p, c, fl, fh, fy, xs)

            r, c, fl, fh, fy = call(
                body, [r, *halo, inverse], [state] + solve_outs,
                aliases={0: 0}, scratch=solve_scratch, flops=flops,
            )
        else:
            before = ((colour - 1) // 4, (colour - 1) // 2 % 2, (colour - 1) % 2)
            if par[1] == before[1]:

                def body(r_in, s_in, lo, hi, yy, gm, p, r_ref, s_ref, c, fl, fh, fy, xs, par=par, before=before):
                    ghosts(bk, before, r_ref, s_ref, gm, lo, hi, yy)
                    solve(bk, par, r_ref, p, c, fl, fh, fy, xs)

                r, sol, c, fl, fh, fy = call(
                    body, [r, sol, *pending, couple, inverse], [state, state] + solve_outs,
                    aliases={0: 0, 1: 1}, scratch=solve_scratch, flops=flops,
                )
            else:
                r, sol = move_region(bk, before, par, r, sol, pending, couple, msg, state)

                def body(r_in, p, r_ref, c, fl, fh, fy, xs, par=par):
                    solve(bk, par, r_ref, p, c, fl, fh, fy, xs)

                r, c, fl, fh, fy = call(
                    body, [r, inverse], [state] + solve_outs,
                    aliases={0: 0}, scratch=solve_scratch, flops=flops,
                )
        pending = exchange(fl, fh, fy, bk)
        if colour == 0:
            r, sol = call(
                own_change(bk, par, True), [r, c, weights], [state, state],
                aliases={0: 0}, scratch=[coarse, coarse], flops=flops,
            )
        else:
            r, sol = call(
                own_change(bk, par, False), [r, sol, c, weights], [state, state],
                aliases={0: 0, 1: 1}, scratch=[coarse, coarse], flops=flops,
            )
    whole = (right_side.shape, F32)
    (solution_out,) = call(leave(bk, None), [sol], [whole], hbm_out=True, flops=flops)

    def last(r_in, lo, hi, yy, gm, r_ref):
        ghosts(bk, (1, 1, 1), r_ref, None, gm, lo, hi, yy)

    (r,) = call(last, [r, *pending, couple], [state], aliases={0: 0})
    (residual_out,) = call(leave(bk, None), [r], [whole], hbm_out=True)
    return solution_out, residual_out


def exchange(fl, fh, fy, bk):
    below, above = shift(fh, "gx", 1), shift(fl, "gx", -1)
    if lax.axis_size("gy") == 2:
        ys = shift(fy, "gy", 1)
    else:
        n = bk.faces_y
        ys = jnp.concatenate([shift(fy[:n], "gy", -1), shift(fy[n:], "gy", 1)])
    return below, above, ys


def move_region(bk, before, par, r, sol, pending, couple, msg, state):
    to_home_y = before[1] == 0
    to_home_x = before[0] == 0 and par[0] == 1
    with_sol = before == (0, 0, 1)
    x_send = bk.face_x(-1, 1)
    x_home = bk.face_x(bk.ex - 1, 1)
    a = par[0]
    y_cells = bk.face_y(-1, a)
    sol_cells = [bk.tile(bk.ex - 1, bk.ey - 1, pz) for pz in range(2)]
    n_y = len(y_cells) + (2 if with_sol else 0)

    def finish(r_in, s_in, lo, hi, yy, gm, r_ref, s_ref, m_ref):
        ghosts(bk, before, r_ref, s_ref, gm, lo, hi, yy)
        if to_home_x:
            for m, t in enumerate(x_send):
                m_ref[m] = r_ref[t].astype(BF16)
        else:
            for m, t in enumerate(y_cells):
                m_ref[m] = r_ref[t].astype(BF16)
            if with_sol:
                for m, t in enumerate(sol_cells):
                    m_ref[len(y_cells) + m] = s_ref[t].astype(BF16)

    n_first = len(x_send) if to_home_x else n_y
    r, sol, m = call(
        finish, [r, sol, *pending, couple], [state, state, msg(n_first)], aliases={0: 0, 1: 1}
    )
    if to_home_x:
        m = shift(m, "gx", -1)

        def turn(r_in, m_in, r_ref, y_ref):
            for i, t in enumerate(x_home):
                r_ref[t] = m_in[i].astype(F32)
            for i, t in enumerate(y_cells):
                y_ref[i] = r_ref[t].astype(BF16)

        r, m = call(turn, [r, m], [state, msg(n_y)], aliases={0: 0})
    m = shift(m, "gy", -1 if to_home_y else 1)

    def place(r_in, s_in, m_in, r_ref, s_ref):
        for i, t in enumerate(y_cells):
            r_ref[t] = m_in[i].astype(F32)
        if with_sol:
            for i, t in enumerate(sol_cells):
                s_ref[t] = m_in[len(y_cells) + i].astype(F32)

    r, sol = call(place, [r, sol, m], [state, state], aliases={0: 0, 1: 1})
    return r, sol


def solution(mesh):
    placed = (P(None, "gx", "gy", "gz"), P("gx", "gy", "gz"), P(), P(), P())
    return jax.shard_map(
        on_device,
        mesh=mesh,
        in_specs=placed,
        out_specs=(P(None, "gx", "gy", "gz"), P(None, "gx", "gy", "gz")),
        check_vma=False,
    )
```
